32 devices in a mesh: data: 1 (over z), feat: 4 (over y), graph: 8 (over x, core).
Axes of the slice: x: 4, y: 4, z: 1, core: 2. Of those that a mesh axis runs over, the one named last changes fastest.
The devices are a block of a 4x4x8 slice.
Arguments:
- X: bfloat16 [16384, 300], P(('data', 'graph'), 'feat')
- dst_local: int32 [327680], P(('data', 'graph'))
- src_slot: int32 [327680], P(('data', 'graph'))
- valid: int32 [327680], P(('data', 'graph'))
- w: float32 [327680], P(('data', 'graph'))
- send_idx: int32 [64, 256], P(('data', 'graph'))
- send_valid: int32 [64, 256], P(('data', 'graph'))
- hub_ids: int32 [128], P('data')
- W1: bfloat16 [300, 512], P('feat')
- W2: bfloat16 [512, 512], P('feat')
- b1: float32 [512], P('feat')
- b2: float32 [512], P('feat')
Outputs:
- output: float32 [16384, 512], P(('data', 'graph'), 'feat')
All inputs are finite; a program needn't handle non-finite values.
Results may differ from the reference program's by a relative error of at most 0.001.
Values are sent between devices in bfloat16 or wider.
A program may use at most 768 MiB of HBM per device.

```python
import jax
import jax.numpy as jnp
from jax import lax

GRAPH = 8
VERT_DEV = 2048
DEG = 20
SEND_ROWS = 256
F_IN = 300
F_HID = 512

HUB_DEV = VERT_DEV // 128
HUB_COUNT = GRAPH * HUB_DEV
EDGE_DEV = VERT_DEV * DEG
ACC_ROWS = VERT_DEV + HUB_COUNT


def draw_graph(key):
    sub_keys = jax.random.split(key, 12)
    nonhub = VERT_DEV - HUB_DEV
    dev_ids = jnp.arange(GRAPH)
    row_perm = jax.vmap(lambda sub_key: jax.random.permutation(sub_key, VERT_DEV))(jax.random.split(sub_keys[0], GRAPH))
    hub_ids = (dev_ids[:, None] * VERT_DEV + row_perm[:, :HUB_DEV]).reshape(HUB_COUNT)
    edge_count = jax.random.randint(sub_keys[1], (GRAPH,), EDGE_DEV // 4, EDGE_DEV + 1)
    full_dev = jax.random.randint(sub_keys[2], (), 0, GRAPH)
    edge_count = jnp.where(dev_ids == full_dev, EDGE_DEV, edge_count)
    valid = (jnp.arange(EDGE_DEV)[None, :] < edge_count[:, None]).astype(jnp.int32)
    send_count = jax.random.randint(sub_keys[3], (GRAPH, GRAPH), max(1, SEND_ROWS // 4), SEND_ROWS + 1)
    full_pair = jax.random.randint(sub_keys[4], (), 0, GRAPH)
    is_full = (dev_ids[:, None] == full_pair) & (dev_ids[None, :] == (full_pair + 1) % GRAPH)
    send_count = jnp.where(is_full, SEND_ROWS, send_count)
    send_count = jnp.where(dev_ids[:, None] == dev_ids[None, :], 0, send_count)
    send_valid = (jnp.arange(SEND_ROWS)[None, None, :] < send_count[:, :, None]).astype(jnp.int32)
    send_rank = jax.random.randint(sub_keys[5], (GRAPH, GRAPH, SEND_ROWS), 0, nonhub)
    send_idx = row_perm[dev_ids[:, None, None], HUB_DEV + send_rank]
    src_kind = jax.random.randint(sub_keys[6], (GRAPH, EDGE_DEV), 0, 100)
    local_src = jax.random.randint(sub_keys[7], (GRAPH, EDGE_DEV), 0, VERT_DEV)
    peer_dev = (dev_ids[:, None] + 1 + jax.random.randint(sub_keys[8], (GRAPH, EDGE_DEV), 0, GRAPH - 1)) % GRAPH
    peer_count = send_count[peer_dev, dev_ids[:, None]]
    halo_pos = jax.random.randint(sub_keys[9], (GRAPH, EDGE_DEV), 0, peer_count)
    halo_src = VERT_DEV + peer_dev * SEND_ROWS + halo_pos
    hub_src = VERT_DEV + GRAPH * SEND_ROWS + jax.random.randint(sub_keys[10], (GRAPH, EDGE_DEV), 0, HUB_COUNT)
    src_slot = jnp.where(src_kind < 50, local_src, jnp.where(src_kind < 85, halo_src, hub_src))
    dst_keys = jax.random.split(sub_keys[11], 3)
    dst_kind = jax.random.randint(dst_keys[0], (GRAPH, EDGE_DEV), 0, 100)
    skew_draw = jax.random.randint(dst_keys[1], (GRAPH, EDGE_DEV), 0, 32768)
    dst_rank = (((skew_draw * skew_draw) >> 15) * nonhub) >> 15
    local_dst = row_perm[dev_ids[:, None], HUB_DEV + dst_rank]
    hub_dst = VERT_DEV + jax.random.randint(dst_keys[2], (GRAPH, EDGE_DEV), 0, HUB_COUNT)
    dst_local = jnp.where(dst_kind < 10, hub_dst, local_dst)
    flat_dst = (dev_ids[:, None] * ACC_ROWS + dst_local).reshape(-1)
    in_deg = jax.ops.segment_sum(valid.reshape(-1), flat_dst, num_segments=GRAPH * ACC_ROWS).reshape(GRAPH, ACC_ROWS)
    hub_deg = jnp.sum(in_deg[:, VERT_DEV:], axis=0)
    all_deg = jnp.concatenate([in_deg[:, :VERT_DEV], jnp.broadcast_to(hub_deg[None, :], (GRAPH, HUB_COUNT))], axis=1)
    dst_deg = jnp.take_along_axis(all_deg, dst_local, axis=1)
    return dst_local, src_slot, valid, dst_deg, send_idx, send_valid, hub_ids


def setup_inputs(seed: int = 0, part: int = 0) -> dict:
    base_key = jax.random.key(seed)
    part_key = jax.random.fold_in(base_key, part)
    dst_local, src_slot, valid, dst_deg, send_idx, send_valid, hub_ids = draw_graph(jax.random.fold_in(part_key, 1))
    key_x, key_u = jax.random.split(jax.random.fold_in(part_key, 2), 2)
    key_w1, key_w2, key_b1, key_b2 = jax.random.split(jax.random.key(seed + 1), 4)
    feats = jax.random.normal(key_x, (GRAPH * VERT_DEV, F_IN), jnp.float32)
    edge_scale = jax.random.uniform(key_u, (GRAPH, EDGE_DEV), jnp.float32, 0.5, 1.5)
    edge_weight = edge_scale * lax.rsqrt(jnp.maximum(dst_deg, 1).astype(jnp.float32))
    w_first = jax.random.normal(key_w1, (F_IN, F_HID), jnp.float32) * (F_IN ** -0.5)
    w_second = jax.random.normal(key_w2, (F_HID, F_HID), jnp.float32) * (F_HID ** -0.5)
    return {
        "X": feats.astype(jnp.bfloat16),
        "dst_local": dst_local.reshape(-1),
        "src_slot": src_slot.reshape(-1),
        "valid": valid.reshape(-1),
        "w": edge_weight.reshape(-1),
        "send_idx": send_idx.reshape(GRAPH * GRAPH, SEND_ROWS),
        "send_valid": send_valid.reshape(GRAPH * GRAPH, SEND_ROWS),
        "hub_ids": hub_ids,
        "W1": w_first.astype(jnp.bfloat16),
        "W2": w_second.astype(jnp.bfloat16),
        "b1": 0.5 * jax.random.normal(key_b1, (F_HID,), jnp.float32),
        "b2": 0.5 * jax.random.normal(key_b2, (F_HID,), jnp.float32),
    }


def reference(X, dst_local, src_slot, valid, w, send_idx, send_valid, hub_ids, W1, W2, b1, b2):
    dst_dev = dst_local.reshape(GRAPH, EDGE_DEV)
    src_dev = src_slot.reshape(GRAPH, EDGE_DEV)
    coef_dev = (w * valid.astype(jnp.float32)).reshape(GRAPH, EDGE_DEV)
    send_grid = send_idx.reshape(GRAPH, GRAPH, SEND_ROWS)
    keep_grid = send_valid.reshape(GRAPH, GRAPH, SEND_ROWS) > 0
    sender_ids = jnp.arange(GRAPH)[:, None]

    def gcn_layer(layer_in, weight, bias_vec):
        z_rows = jnp.dot(layer_in, weight, preferred_element_type=jnp.float32).astype(jnp.bfloat16)
        feat_width = weight.shape[1]
        z_grid = z_rows.reshape(GRAPH, VERT_DEV, feat_width)
        hub_feat = z_rows[hub_ids]

        def device_sum(dev_args):
            dev_index, dst_edges, src_edges, coef_edges = dev_args
            halo_rows = z_grid[sender_ids, send_grid[:, dev_index, :]]
            halo_rows = jnp.where(keep_grid[:, dev_index, :, None], halo_rows, jnp.zeros_like(halo_rows))
            slot_table = jnp.concatenate([z_grid[dev_index], halo_rows.reshape(GRAPH * SEND_ROWS, feat_width), hub_feat], axis=0)
            messages = slot_table[src_edges].astype(jnp.float32) * coef_edges[:, None]
            return jax.ops.segment_sum(messages, dst_edges, num_segments=ACC_ROWS)

        partial_sum = lax.map(device_sum, (jnp.arange(GRAPH), dst_dev, src_dev, coef_dev))
        hub_total = jnp.sum(partial_sum[:, VERT_DEV:], axis=0)
        own_rows = partial_sum[:, :VERT_DEV].reshape(GRAPH * VERT_DEV, feat_width).at[hub_ids].add(hub_total)
        return own_rows + bias_vec

    hidden = jnp.maximum(gcn_layer(X, W1, b1), 0.0).astype(jnp.bfloat16)
    return gcn_layer(hidden, W2, b2)
```

```python
import functools

import jax
import jax.numpy as jnp
from jax import lax
from jax.experimental import pallas as pl
from jax.experimental.pallas import tpu as pltpu
from jax.sharding import PartitionSpec as P

DB, SB, KW = 128, 256, 256
BF16_MAX = 3.3895313892515355e38


def bf16_parts(x):
    hi = jnp.clip(x, -BF16_MAX, BF16_MAX).astype(jnp.bfloat16)
    rest = x - hi.astype(jnp.float32)
    mid = rest.astype(jnp.bfloat16)
    low = (rest - mid.astype(jnp.float32)).astype(jnp.bfloat16)
    return hi, mid, low


def build_kernel(nsb, starts_ref, edges_ref, a_ref):
    db = pl.program_id(0)
    dbase = (db * DB).astype(jnp.float32)
    iota_d = lax.broadcasted_iota(jnp.int32, (DB, KW), 0).astype(jnp.bfloat16)
    iota_s = lax.broadcasted_iota(jnp.int32, (SB, KW), 0).astype(jnp.bfloat16)

    def window(sb, start):
        base = pl.multiple_of((start // 128) * 128, 128)
        shift = start - base
        raw = edges_ref[:, pl.ds(base, KW + 128)]
        rows = pltpu.roll(raw, KW + 128 - shift, 1)[:, :KW]
        dst = (rows[0:1] - dbase).astype(jnp.bfloat16)
        src = (rows[1:2] - jnp.float32(SB) * sb).astype(jnp.bfloat16)
        hi, mid, low = bf16_parts(rows[2:3])
        hit = iota_d == dst
        zero = jnp.zeros((), jnp.bfloat16)
        d3 = jnp.concatenate([jnp.where(hit, part, zero) for part in (hi, mid, low)], axis=0)
        sel = jnp.where(iota_s == src, jnp.ones((), jnp.bfloat16), zero)
        out = lax.dot_general(d3, sel, (((1,), (1,)), ((), ())), preferred_element_type=jnp.float32)
        return out[:DB] + (out[DB:2 * DB] + out[2 * DB:])

    for sb in range(nsb):
        start = starts_ref[db * nsb + sb]
        a_ref[:, sb * SB:(sb + 1) * SB] = window(jnp.float32(sb), start)
    for sb in range(nsb):
        start = starts_ref[db * nsb + sb]
        end = starts_ref[db * nsb + sb + 1]

        def more(i, carry):
            a_ref[:, sb * SB:(sb + 1) * SB] += window(jnp.float32(sb), start + i * KW)
            return carry

        lax.fori_loop(1, (end - start + KW - 1) // KW, more, 0)


def build_adjacency(starts, edges, ndb, nsb):
    return pl.pallas_call(
        functools.partial(build_kernel, nsb),
        out_shape=jax.ShapeDtypeStruct((ndb * DB, nsb * SB), jnp.float32),
        grid_spec=pltpu.PrefetchScalarGridSpec(
            num_scalar_prefetch=1,
            grid=(ndb,),
            in_specs=[pl.BlockSpec(edges.shape, lambda i, s: (0, 0))],
            out_specs=pl.BlockSpec((DB, nsb * SB), lambda i, s: (i, 0)),
        ),
        name="build",
    )(starts, edges)


def apply_kernel(a_ref, t_ref, o_ref):
    parts = bf16_parts(a_ref[...])
    rows = a_ref.shape[0]
    out = jnp.dot(jnp.concatenate(parts, axis=0), t_ref[...], preferred_element_type=jnp.float32)
    o_ref[...] = out[:rows] + (out[rows:2 * rows] + out[2 * rows:])


def apply_adjacency(adj, table):
    rows, cols = adj.shape
    width = table.shape[1]
    return pl.pallas_call(
        apply_kernel,
        out_shape=jax.ShapeDtypeStruct((rows, width), jnp.float32),
        grid=(rows // DB,),
        in_specs=[pl.BlockSpec((DB, cols), lambda i: (i, 0)), pl.BlockSpec(table.shape, lambda i: (0, 0))],
        out_specs=pl.BlockSpec((DB, width), lambda i: (i, 0)),
        name="apply",
    )(adj, table)


def solution(mesh):
    rows_axes = ("data", "graph")
    nfeat = mesh.shape["feat"]
    ngraph = mesh.shape["graph"]

    def device_program(x_loc, dst_loc, src_loc, valid_loc, w_loc, send_loc, keep_loc, hub_ids, w_first, w_second, b_first, b_second):
        vert = x_loc.shape[0]
        nhub = hub_ids.shape[0]
        per = nhub // ngraph
        nsend = send_loc.shape[1]
        me = lax.axis_index("graph")
        ndb = (vert + nhub) // DB
        table_rows = vert + ngraph * nsend + nhub
        nsb = -(-table_rows // SB)

        owner = hub_ids // vert
        ks = jnp.arange(nhub)
        before = (owner[None, :] == owner[:, None]) & (ks[None, :] < ks[:, None])
        pos = owner * per + jnp.sum(before.astype(jnp.int32), axis=1)
        at_pos = pos[None, :] == ks[:, None]
        hub_by_pos = jnp.sum(jnp.where(at_pos, hub_ids[None, :], 0), axis=1)
        k_by_pos = jnp.sum(jnp.where(at_pos, ks[None, :], 0), axis=1)
        my_hubs = lax.dynamic_slice(hub_by_pos, (me * per,), (per,)) - me * vert

        live = valid_loc > 0
        key = ((dst_loc // DB) << 20) | ((src_loc // SB) << 15) | ((dst_loc % DB) << 8) | (src_loc % SB)
        key = jnp.where(live, key, 1 << 26)
        coef = w_loc * valid_loc.astype(jnp.float32)
        bound_db = jnp.arange(ndb * nsb + 1) // nsb
        bound = (bound_db << 20) | ((jnp.arange(ndb * nsb + 1) % nsb) << 15)
        starts = jnp.sum((key[None, :] < bound[:, None]).astype(jnp.int32), axis=1)
        skey, sw = lax.sort((key, coef), num_keys=1, is_stable=False)
        sdst = (skey >> 20) * DB + ((skey >> 8) & (DB - 1))
        ssrc = ((skey >> 15) & 31) * SB + (skey & (SB - 1))
        edges = jnp.stack([sdst.astype(jnp.float32), ssrc.astype(jnp.float32), sw])
        edges = jnp.pad(edges, ((0, 5), (0, 2 * KW)), constant_values=-1.0)
        adj = build_adjacency(starts, edges, ndb, nsb)

        w_all1 = lax.all_gather(w_first, "feat", axis=0, tiled=True)
        w_all2 = lax.all_gather(w_second, "feat", axis=0, tiled=True)
        zero_bf16 = jnp.zeros((), jnp.bfloat16)
        send_rows = jnp.concatenate([send_loc, jnp.broadcast_to(my_hubs[None, :], (ngraph, per))], axis=1)
        send_keep = jnp.concatenate([keep_loc > 0, jnp.ones((ngraph, per), bool)], axis=1)[:, :, None]
        hub_sel = (pos[:, None] == ks[None, :]).astype(jnp.bfloat16)

        def gcn_layer(layer_in, w_all, bias):
            width = layer_in.shape[1]
            part = vert // nfeat
            mine = lax.all_to_all(layer_in.reshape(nfeat, part, width), "feat", 0, 0, tiled=True)
            full = jnp.concatenate([mine[f] for f in range(nfeat)], axis=1)
            z_rows = jnp.dot(full, w_all, preferred_element_type=jnp.float32).astype(jnp.bfloat16)
            cols = z_rows.shape[1] // nfeat
            z_send = jnp.stack([z_rows[:, f * cols:(f + 1) * cols] for f in range(nfeat)])
            z_loc = lax.all_to_all(z_send, "feat", 0, 0, tiled=True).reshape(vert, cols)
            buf = jnp.where(send_keep, z_loc[send_rows], zero_bf16)
            got = lax.all_to_all(buf, "graph", 0, 0, tiled=True)
            hub_feat = jnp.dot(hub_sel, got[:, nsend:].reshape(nhub, cols), preferred_element_type=jnp.float32).astype(jnp.bfloat16)
            pad = jnp.zeros((nsb * SB - table_rows, cols), jnp.bfloat16)
            table = jnp.concatenate([z_loc, got[:, :nsend].reshape(-1, cols), hub_feat, pad], axis=0)
            sums = apply_adjacency(adj, table)
            hub_part = sums[vert:][k_by_pos].reshape(ngraph, per, cols)
            hub_all = lax.all_to_all(hub_part, "graph", 0, 0, tiled=True)
            hub_total = jnp.sum(hub_all, axis=0)
            return sums[:vert].at[my_hubs].add(hub_total, unique_indices=True) + bias

        hidden = jnp.maximum(gcn_layer(x_loc, w_all1, b_first), 0.0).astype(jnp.bfloat16)
        return gcn_layer(hidden, w_all2, b_second)

    edge_spec = P(rows_axes)
    send_spec = P(rows_axes, None)
    in_specs = (P(rows_axes, "feat"), edge_spec, edge_spec, edge_spec, edge_spec, send_spec, send_spec, P("data"), P("feat", None), P("feat", None), P("feat"), P("feat"))
    return jax.shard_map(device_program, mesh=mesh, in_specs=in_specs, out_specs=P(rows_axes, "feat"), check_vma=False)
```

```python
import functools

import jax
import jax.numpy as jnp
from jax import lax
from jax.experimental import pallas as pl
from jax.experimental.pallas import tpu as pltpu
from jax.sharding import PartitionSpec as P

DB, SB, KW = 128, 256, 256
MESH = pl.DeviceIdType.MESH
F32, BF16 = jnp.float32, jnp.bfloat16


def bf16_parts(x):
    hi = x.astype(BF16)
    rest = x - hi.astype(F32)
    mid = rest.astype(BF16)
    low = (rest - mid.astype(F32)).astype(BF16)
    return hi, mid, low


def build_kernel(nsb, starts_ref, edges_ref, rowid_ref, colid_ref, a_ref):
    db = pl.program_id(0)
    dbase = (db * DB).astype(F32)
    row_id = rowid_ref[0]
    iota_s = lax.broadcasted_iota(jnp.int32, (SB, KW), 0).astype(BF16)
    zero = jnp.zeros((), BF16)

    def window(sb, start):
        base = pl.multiple_of((start // 128) * 128, 128)
        shift = start - base
        raw = edges_ref[:, pl.ds(base, KW + 128)]
        rows = pltpu.roll(raw, KW + 128 - shift, 1)[:, :KW]
        dst = (rows[0:1] - dbase).astype(BF16)
        src = (rows[1:2] - F32(SB * sb)).astype(BF16)
        hit = row_id == dst
        d3 = jnp.concatenate([jnp.where(hit, part, zero) for part in bf16_parts(rows[2:3])], axis=0)
        col_id = colid_ref[...] if sb == nsb - 1 else iota_s
        sel = jnp.where(col_id == src, jnp.ones((), BF16), zero)
        out = lax.dot_general(d3, sel, (((1,), (1,)), ((), ())), preferred_element_type=F32)
        return out[:DB] + (out[DB:2 * DB] + out[2 * DB:])

    for sb in range(nsb):
        a_ref[:, sb * SB:(sb + 1) * SB] = window(sb, starts_ref[db * nsb + sb])
    for sb in range(nsb):
        start = starts_ref[db * nsb + sb]
        end = starts_ref[db * nsb + sb + 1]

        def more(i, carry):
            a_ref[:, sb * SB:(sb + 1) * SB] += window(sb, start + i * KW)
            return carry

        lax.fori_loop(1, (end - start + KW - 1) // KW, more, 0)


def build_adjacency(starts, edges, rowid, colid, ndb, nsb):
    return pl.pallas_call(
        functools.partial(build_kernel, nsb),
        out_shape=jax.ShapeDtypeStruct((ndb * DB, nsb * SB), F32),
        grid_spec=pltpu.PrefetchScalarGridSpec(
            num_scalar_prefetch=1,
            grid=(ndb,),
            in_specs=[
                pl.BlockSpec(edges.shape, lambda i, s: (0, 0)),
                pl.BlockSpec((1, DB, KW), lambda i, s: (i // (ndb - 1), 0, 0)),
                pl.BlockSpec(colid.shape, lambda i, s: (0, 0)),
            ],
            out_specs=pl.BlockSpec((DB, nsb * SB), lambda i, s: (i, 0)),
        ),
        name="build",
    )(starts, edges, rowid, colid)


def layers_kernel(dims, x_ref, w1_ref, w2_ref, idx_ref, myhub_ref, b1_ref, b2_ref, inv_ref, a_hbm, o_ref,
                  a_v, xin, w1in, w2in, tab1, tab2, zout, hsend, hin, halo, hubsend, hubrecv,
                  a_sem, xs, xr, w1s, w1r, w2s, w2r, z1s, z1r, z2s, z2r, hs, hr, ps, pr, us, ur, ns, nr):
    nfeat, ngraph, vert, nsend, per = dims
    part, rows_send = vert // nfeat, nsend + per
    nchunk = part // DB
    f, g = lax.axis_index("feat"), lax.axis_index("graph")
    halo_base, hub_base = vert, vert + ngraph * nsend
    nblock = vert // DB

    def fpeer(r):
        return lax.rem(f + r, nfeat)

    def gpeer(r):
        return lax.rem(g + r, ngraph)

    def frdma(src, dst, send, recv, r):
        return pltpu.make_async_remote_copy(src, dst, send, recv, device_id={"feat": fpeer(r)}, device_id_type=MESH)

    def grdma(src, dst, send, recv, r):
        return pltpu.make_async_remote_copy(src, dst, send, recv, device_id={"graph": gpeer(r)}, device_id_type=MESH)

    a_copies = [pltpu.make_async_copy(a_hbm.at[pl.ds(i * DB, DB)], a_v.at[pl.ds(i * DB, DB)], a_sem.at[i]) for i in range(a_hbm.shape[0] // DB)]
    for copy in a_copies:
        copy.start()

    barrier = pltpu.get_barrier_semaphore()
    for r in range(1, nfeat):
        pl.semaphore_signal(barrier, inc=1, device_id={"feat": fpeer(r)}, device_id_type=MESH)
    for r in range(1, ngraph):
        pl.semaphore_signal(barrier, inc=1, device_id={"graph": gpeer(r)}, device_id_type=MESH)
    pl.semaphore_wait(barrier, nfeat + ngraph - 2)

    def quarter(q):
        return pl.ds(pl.multiple_of(q * part, part), part)

    x_copies = [frdma(x_ref.at[quarter(fpeer(r))], xin.at[f], xs.at[r - 1], xr.at[r - 1], r) for r in range(1, nfeat)]
    w1_copies = [frdma(w1_ref, w1in.at[f], w1s.at[r - 1], w1r.at[r - 1], r) for r in range(1, nfeat)]
    w2_copies = [frdma(w2_ref, w2in.at[f], w2s.at[r - 1], w2r.at[r - 1], r) for r in range(1, nfeat)]
    for copy in w1_copies + x_copies + w2_copies:
        copy.start()
    xin[f] = x_ref[quarter(f)]
    w1in[f] = w1_ref[...]
    w2in[f] = w2_ref[...]
    pad_rows = a_v.shape[1] - hub_base - ngraph * per
    for tab in (tab1, tab2):
        tab[pl.ds(pl.multiple_of(halo_base + g * nsend, nsend), nsend)] = jnp.zeros((nsend, tab.shape[1]), BF16)
        tab[hub_base + ngraph * per:] = jnp.zeros((pad_rows, tab.shape[1]), BF16)

    for copy in w1_copies + x_copies:
        copy.wait_recv()
    cols = tab1.shape[1]
    z = None
    for s in range(nfeat):
        term = jnp.dot(xin[s], w1in[s], preferred_element_type=F32)
        z = term if z is None else z + term
    z = z.astype(BF16)
    for q in range(nfeat):
        zout[q] = z[:, q * cols:(q + 1) * cols]
    z1_copies = [frdma(zout.at[fpeer(r)], tab1.at[quarter(f)], z1s.at[r - 1], z1r.at[r - 1], r) for r in range(1, nfeat)]
    for copy in z1_copies:
        copy.start()
    tab1[quarter(f)] = zout[f]
    for copy in z1_copies:
        copy.wait_recv()

    lane = lax.broadcasted_iota(jnp.int32, (1, DB), 1)

    def select_rows(tab, idx):
        pieces = [jnp.where(idx == lane + DB * j, F32(1), F32(0)).astype(BF16) for j in range(vert // DB)]
        return jnp.dot(jnp.concatenate(pieces, axis=1), tab[:vert], preferred_element_type=F32).astype(BF16)

    def halo_copies(tab, layer, r):
        p = gpeer(r)
        return (
            grdma(halo.at[layer, p, pl.ds(0, nsend)], tab.at[pl.ds(pl.multiple_of(halo_base + g * nsend, nsend), nsend)],
                  hs.at[layer, r - 1], hr.at[layer, r - 1], r),
            grdma(halo.at[layer, p, pl.ds(nsend, per)], tab.at[pl.ds(pl.multiple_of(hub_base + g * per, per), per)],
                  ps.at[layer, r - 1], pr.at[layer, r - 1], r),
        )

    def exchange_halo(tab, layer):
        def one(r, carry):
            p = gpeer(r)
            halo[layer, p] = select_rows(tab, idx_ref[p])
            for copy in halo_copies(tab, layer, r):
                copy.start()
            return carry

        lax.fori_loop(1, ngraph, one, 0)
        tab[pl.ds(pl.multiple_of(hub_base + g * per, per), per)] = select_rows(tab, idx_ref[g, nsend:])

        def arrive(r, carry):
            for copy in halo_copies(tab, layer, r):
                copy.wait_recv()
            return carry

        lax.fori_loop(1, ngraph, arrive, 0)

    inv = inv_ref[...]

    def block(tab, rb):
        a = a_v[pl.ds(pl.multiple_of(rb * DB, DB), DB), :]
        out = jnp.dot(jnp.concatenate(bf16_parts(a), axis=0), tab[...], preferred_element_type=F32)
        return (out[:DB] + (out[DB:2 * DB] + out[2 * DB:])) * inv

    def hub_copy(layer, r):
        p = gpeer(r)
        return grdma(hubsend.at[layer, pl.ds(pl.multiple_of(p * per, per), per)], hubrecv.at[layer, g], us.at[layer, r - 1], ur.at[layer, r - 1], r)

    def exchange_hubs(tab, layer):
        hubsend[layer] = block(tab, nblock)
        for r in range(1, ngraph):
            hub_copy(layer, r).start()
        hubrecv[layer, g] = hubsend[layer, pl.ds(pl.multiple_of(g * per, per), per)]

    def hub_totals(layer):
        for r in range(1, ngraph):
            hub_copy(layer, r).wait_recv()
        total = hubrecv[layer, 0]
        for p in range(1, ngraph):
            total = total + hubrecv[layer, p]
        fill = jnp.zeros((DB - 3 * per, total.shape[1]), BF16)
        return jnp.concatenate([*bf16_parts(total), fill], axis=0)

    def with_hubs(layer, totals, y, rb):
        rows = lax.broadcasted_iota(jnp.int32, (DB, DB), 0) + rb * DB
        sel = jnp.where(rows == myhub_ref[...], F32(1), F32(0)).astype(BF16)
        return y + jnp.dot(sel, totals, preferred_element_type=F32)

    exchange_halo(tab1, 0)
    for copy in a_copies:
        copy.wait()
    exchange_hubs(tab1, 0)
    totals1 = hub_totals(0)
    for copy in w2_copies:
        copy.wait_recv()

    def chunk(i):
        return pl.ds(pl.multiple_of(i * DB, DB), DB)

    def h_copy(i, r):
        return frdma(hsend.at[fpeer(r), chunk(i)], hin.at[f, chunk(i)], ns.at[i, r - 1], nr.at[i, r - 1], r)

    def z2_copy(i, r):
        return frdma(zout.at[fpeer(r), chunk(i)], tab2.at[pl.ds(pl.multiple_of(f * part + i * DB, DB), DB)], z2s.at[i, r - 1], z2r.at[i, r - 1], r)

    for copy in z1_copies:
        copy.wait_send()

    def z2_chunk(i):
        for r in range(1, nfeat):
            h_copy(i, r).wait_recv()
        acc = None
        for s in range(nfeat):
            term = jnp.dot(hin[s, chunk(i)], w2in[s], preferred_element_type=F32)
            acc = term if acc is None else acc + term
        acc = acc.astype(BF16)
        for q in range(nfeat):
            zout[q, chunk(i)] = acc[:, q * cols:(q + 1) * cols]
        for r in range(1, nfeat):
            z2_copy(i, r).start()
        tab2[pl.ds(pl.multiple_of(f * part + i * DB, DB), DB)] = zout[f, chunk(i)]

    bias1 = b1_ref[...]

    def rows1(t, carry):
        i, rr = t // nfeat, lax.rem(t, nfeat)
        q = fpeer(rr + 1)
        rb = q * nchunk + i
        h = jnp.maximum(with_hubs(0, totals1, block(tab1, rb), rb) + bias1, 0.0).astype(BF16)

        @pl.when(rr < nfeat - 1)
        def _():
            hsend[q, chunk(i)] = h
            h_copy(i, rr + 1).start()

        @pl.when(rr == nfeat - 1)
        def _():
            hin[f, chunk(i)] = h

        @pl.when((rr == nfeat - 2) & (i > 0))
        def _():
            z2_chunk(i - 1)

        return carry

    lax.fori_loop(0, nblock, rows1, 0)
    z2_chunk(nchunk - 1)
    for i in range(nchunk):
        for r in range(1, nfeat):
            z2_copy(i, r).wait_recv()

    exchange_halo(tab2, 1)
    exchange_hubs(tab2, 1)
    totals2 = hub_totals(1)
    bias2 = b2_ref[...]

    def rows2(rb, carry):
        o_ref[chunk(rb), :] = with_hubs(1, totals2, block(tab2, rb), rb) + bias2
        return carry

    lax.fori_loop(0, nblock, rows2, 0)

    for copy in x_copies + w1_copies + w2_copies:
        copy.wait_send()
    for i in range(nchunk):
        for r in range(1, nfeat):
            h_copy(i, r).wait_send()
            z2_copy(i, r).wait_send()
    for layer, tab in enumerate((tab1, tab2)):
        for r in range(1, ngraph):
            for copy in halo_copies(tab, layer, r):
                copy.wait_send()
            hub_copy(layer, r).wait_send()


def run_layers(nfeat, ngraph, nsend, per, x, w1, w2, idx, myhub, b1, b2, inv, adj):
    vert = x.shape[0]
    part, cols = vert // nfeat, b1.shape[1]
    nchunk, nblk = part // DB, adj.shape[0] // DB
    vm = lambda shape, dt: pltpu.VMEM(shape, dt)
    dma = lambda *shape: pltpu.SemaphoreType.DMA(shape)
    vspec = pl.BlockSpec(memory_space=pltpu.VMEM)
    fr, gr = nfeat - 1, ngraph - 1
    return pl.pallas_call(
        functools.partial(layers_kernel, (nfeat, ngraph, vert, nsend, per)),
        out_shape=jax.ShapeDtypeStruct((vert, cols), F32),
        in_specs=[vspec] * 8 + [pl.BlockSpec(memory_space=pl.ANY)],
        out_specs=vspec,
        scratch_shapes=[
            vm(adj.shape, F32), vm((nfeat, part, x.shape[1]), BF16), vm((nfeat, *w1.shape), BF16), vm((nfeat, *w2.shape), BF16),
            vm((adj.shape[1], cols), BF16), vm((adj.shape[1], cols), BF16), vm((nfeat, part, cols), BF16), vm((nfeat, part, cols), BF16),
            vm((nfeat, part, cols), BF16), vm((2, ngraph, nsend + per, cols), BF16), vm((2, ngraph * per, cols), F32), vm((2, ngraph, per, cols), F32),
            dma(nblk), dma(fr), dma(fr), dma(fr), dma(fr), dma(fr), dma(fr), dma(fr), dma(fr), dma(nchunk, fr), dma(nchunk, fr),
            dma(2, gr), dma(2, gr), dma(2, gr), dma(2, gr), dma(2, gr), dma(2, gr), dma(nchunk, fr), dma(nchunk, fr),
        ],
        compiler_params=pltpu.CompilerParams(collective_id=0, has_side_effects=True, vmem_limit_bytes=62 * 2**20),
        name="layers",
    )(x, w1, w2, idx, myhub, b1, b2, inv, adj)


def solution(mesh):
    rows_axes = ("data", "graph")
    nfeat = mesh.shape["feat"]
    ngraph = mesh.shape["graph"]

    def device_program(x_loc, dst_loc, src_loc, valid_loc, w_loc, send_loc, keep_loc, hub_ids, w_first, w_second, b_first, b_second):
        vert = x_loc.shape[0]
        nhub = hub_ids.shape[0]
        per = nhub // ngraph
        nsend = send_loc.shape[1]
        cols = b_first.shape[0]
        me = lax.axis_index("graph")
        ndb = (vert + nhub) // DB
        table_rows = vert + ngraph * nsend + nhub
        nsb = -(-table_rows // SB)

        owner = hub_ids // vert
        ks = jnp.arange(nhub)
        before = (owner[None, :] == owner[:, None]) & (ks[None, :] < ks[:, None])
        pos = owner * per + jnp.sum(before.astype(jnp.int32), axis=1)
        at_pos = pos[None, :] == ks[:, None]
        hub_by_pos = jnp.sum(jnp.where(at_pos, hub_ids[None, :], 0), axis=1)
        k_by_pos = jnp.sum(jnp.where(at_pos, ks[None, :], 0), axis=1)
        my_hubs = lax.dynamic_slice(hub_by_pos, (me * per,), (per,)) - me * vert

        key = ((dst_loc // DB) << 20) | ((src_loc // SB) << 15) | ((dst_loc % DB) << 8) | (src_loc % SB)
        key = jnp.where(valid_loc > 0, key, 1 << 26)
        coef = w_loc * valid_loc.astype(F32)
        large = jnp.max(coef) > 1e30
        coef = coef * jnp.where(large, F32(2.0**-40), F32(1))
        inv = jnp.where(large, F32(2.0**40), F32(1))
        nb = jnp.arange(ndb * nsb + 1)
        bound = ((nb // nsb) << 20) | ((nb % nsb) << 15)
        starts = jnp.sum((key[None, :] < bound[:, None]).astype(jnp.int32), axis=1)
        skey, sw = lax.sort((key, coef), num_keys=1, is_stable=False)
        sdst = (skey >> 20) * DB + ((skey >> 8) & (DB - 1))
        ssrc = ((skey >> 15) & 31) * SB + (skey & (SB - 1))
        edges = jnp.stack([sdst.astype(F32), ssrc.astype(F32), sw])
        edges = jnp.pad(edges, ((0, 5), (0, 2 * KW)), constant_values=-1.0)
        rowid = jnp.stack([jnp.arange(DB), k_by_pos]).astype(BF16)
        rowid = jnp.broadcast_to(rowid[:, :, None], (2, DB, KW))
        colid = jnp.pad(k_by_pos, (0, SB - nhub), constant_values=300).astype(BF16)
        colid = jnp.broadcast_to(colid[:, None], (SB, KW))
        adj = build_adjacency(starts, edges, rowid, colid, ndb, nsb)

        idx = jnp.where(keep_loc > 0, send_loc, -1)
        idx = jnp.concatenate([idx, jnp.broadcast_to(my_hubs[None, :], (ngraph, per))], axis=1)
        idx = jnp.broadcast_to(idx[:, :, None], (*idx.shape, DB))
        myhub = jnp.pad(jnp.concatenate([my_hubs] * 3), (0, DB - 3 * per), constant_values=-1)[None, :]
        inv = jnp.full((1, cols), inv)
        return run_layers(nfeat, ngraph, nsend, per, x_loc, w_first, w_second, idx, myhub, b_first[None, :], b_second[None, :], inv, adj)

    edge_spec = P(rows_axes)
    send_spec = P(rows_axes, None)
    in_specs = (P(rows_axes, "feat"), edge_spec, edge_spec, edge_spec, edge_spec, send_spec, send_spec, P("data"), P("feat", None), P("feat", None), P("feat"), P("feat"))
    return jax.shard_map(device_program, mesh=mesh, in_specs=in_specs, out_specs=P(rows_axes, "feat"), check_vma=False)
```

```python
import functools

import jax
import jax.numpy as jnp
from jax import lax
from jax.experimental import pallas as pl
from jax.experimental.pallas import tpu as pltpu
from jax.sharding import PartitionSpec as P

DB, SB, KW = 128, 256, 256
LAG = 4
MESH = pl.DeviceIdType.MESH
F32, BF16 = jnp.float32, jnp.bfloat16


def bf16_parts(x):
    hi = x.astype(BF16)
    rest = x - hi.astype(F32)
    mid = rest.astype(BF16)
    low = (rest - mid.astype(F32)).astype(BF16)
    return hi, mid, low


def build_kernel(nsb, starts_ref, edges_ref, rowid_ref, colid_ref, a_ref):
    db = pl.program_id(0)
    dbase = (db * DB).astype(F32)
    row_id = rowid_ref[0]
    iota_s = lax.broadcasted_iota(jnp.int32, (SB, KW), 0).astype(BF16)
    zero = jnp.zeros((), BF16)

    def window(sb, start):
        base = pl.multiple_of((start // 128) * 128, 128)
        shift = start - base
        raw = edges_ref[:, pl.ds(base, KW + 128)]
        rows = pltpu.roll(raw, KW + 128 - shift, 1)[:, :KW]
        dst = (rows[0:1] - dbase).astype(BF16)
        src = (rows[1:2] - F32(SB * sb)).astype(BF16)
        hit = row_id == dst
        d3 = jnp.concatenate([jnp.where(hit, part, zero) for part in bf16_parts(rows[2:3])], axis=0)
        col_id = colid_ref[...] if sb == nsb - 1 else iota_s
        sel = jnp.where(col_id == src, jnp.ones((), BF16), zero)
        out = lax.dot_general(d3, sel, (((1,), (1,)), ((), ())), preferred_element_type=F32)
        return out[:DB] + (out[DB:2 * DB] + out[2 * DB:])

    for sb in range(nsb):
        a_ref[:, sb * SB:(sb + 1) * SB] = window(sb, starts_ref[db * nsb + sb])
    for sb in range(nsb):
        start = starts_ref[db * nsb + sb]
        end = starts_ref[db * nsb + sb + 1]

        def more(i, carry):
            a_ref[:, sb * SB:(sb + 1) * SB] += window(sb, start + i * KW)
            return carry

        lax.fori_loop(1, (end - start + KW - 1) // KW, more, 0)


def build_adjacency(starts, edges, rowid, colid, ndb, nsb):
    return pl.pallas_call(
        functools.partial(build_kernel, nsb),
        out_shape=jax.ShapeDtypeStruct((ndb * DB, nsb * SB), F32),
        grid_spec=pltpu.PrefetchScalarGridSpec(
            num_scalar_prefetch=1,
            grid=(ndb,),
            in_specs=[
                pl.BlockSpec(edges.shape, lambda i, s: (0, 0)),
                pl.BlockSpec((1, DB, KW), lambda i, s: (i // (ndb - 1), 0, 0)),
                pl.BlockSpec(colid.shape, lambda i, s: (0, 0)),
            ],
            out_specs=pl.BlockSpec((DB, nsb * SB), lambda i, s: (i, 0)),
        ),
        name="build",
    )(starts, edges, rowid, colid)


def layers_kernel(dims, x_ref, w1_ref, w2_ref, idx_ref, myhub_ref, b1_ref, b2_ref, inv_ref, a_hbm, o_ref,
                  a_v, acc, tot, xin, w1in, w2in, tab1, tab2, zout, hsend, hin, halo, hubsend, hubrecv,
                  a_sem, xs, xr, w1s, w1r, w2s, w2r, z1s, z1r, z2s, z2r, hs, hr, ps, pr, us, ur, ns, nr):
    nfeat, ngraph, vert, nsend, per = dims
    part, rows_send = vert // nfeat, nsend + per
    nchunk = part // DB
    f, g = lax.axis_index("feat"), lax.axis_index("graph")
    halo_base, hub_base = vert, vert + ngraph * nsend
    nblock = vert // DB

    def fpeer(r):
        return lax.rem(f + r, nfeat)

    def gpeer(r):
        return lax.rem(g + r, ngraph)

    def frdma(src, dst, send, recv, r):
        return pltpu.make_async_remote_copy(src, dst, send, recv, device_id={"feat": fpeer(r)}, device_id_type=MESH)

    def grdma(src, dst, send, recv, r):
        return pltpu.make_async_remote_copy(src, dst, send, recv, device_id={"graph": gpeer(r)}, device_id_type=MESH)

    for i in range(a_hbm.shape[0] // DB):
        pltpu.make_async_copy(a_hbm.at[pl.ds(i * DB, DB)], a_v.at[pl.ds(i * DB, DB)], a_sem.at[i]).start()

    barrier = pltpu.get_barrier_semaphore()
    for r in range(1, nfeat):
        pl.semaphore_signal(barrier, inc=1, device_id={"feat": fpeer(r)}, device_id_type=MESH)
    for r in range(1, ngraph):
        pl.semaphore_signal(barrier, inc=1, device_id={"graph": gpeer(r)}, device_id_type=MESH)
    pl.semaphore_wait(barrier, nfeat + ngraph - 2)

    def quarter(q):
        return pl.ds(pl.multiple_of(q * part, part), part)

    x_copies = [frdma(x_ref.at[quarter(fpeer(r))], xin.at[f], xs.at[r - 1], xr.at[r - 1], r) for r in range(1, nfeat)]
    w1_copies = [frdma(w1_ref, w1in.at[f], w1s.at[r - 1], w1r.at[r - 1], r) for r in range(1, nfeat)]
    w2_copies = [frdma(w2_ref, w2in.at[f], w2s.at[r - 1], w2r.at[r - 1], r) for r in range(1, nfeat)]
    for copy in w1_copies + x_copies + w2_copies:
        copy.start()
    xin[f] = x_ref[quarter(f)]
    w1in[f] = w1_ref[...]
    w2in[f] = w2_ref[...]
    pad_rows = a_v.shape[1] - hub_base - ngraph * per
    for tab in (tab1, tab2):
        tab[pl.ds(pl.multiple_of(halo_base + g * nsend, nsend), nsend)] = jnp.zeros((nsend, tab.shape[1]), BF16)
        tab[hub_base + ngraph * per:] = jnp.zeros((pad_rows, tab.shape[1]), BF16)

    for copy in w1_copies + x_copies:
        copy.wait_recv()
    cols = tab1.shape[1]
    z = None
    for s in range(nfeat):
        term = jnp.dot(xin[s], w1in[s], preferred_element_type=F32)
        z = term if z is None else z + term
    z = z.astype(BF16)
    for q in range(nfeat):
        zout[q] = z[:, q * cols:(q + 1) * cols]
    z1_copies = [frdma(zout.at[fpeer(r)], tab1.at[quarter(f)], z1s.at[r - 1], z1r.at[r - 1], r) for r in range(1, nfeat)]
    for copy in z1_copies:
        copy.start()
    tab1[quarter(f)] = zout[f]
    for copy in z1_copies:
        copy.wait_recv()

    lane = lax.broadcasted_iota(jnp.int32, (1, DB), 1)

    def select_rows(tab, idx):
        pieces = [jnp.where(idx == lane + DB * j, F32(1), F32(0)).astype(BF16) for j in range(vert // DB)]
        return jnp.dot(jnp.concatenate(pieces, axis=1), tab[:vert], preferred_element_type=F32).astype(BF16)

    def halo_copies(tab, layer, r):
        p = gpeer(r)
        return (
            grdma(halo.at[layer, p, pl.ds(0, nsend)], tab.at[pl.ds(pl.multiple_of(halo_base + g * nsend, nsend), nsend)],
                  hs.at[layer, r - 1], hr.at[layer, r - 1], r),
            grdma(halo.at[layer, p, pl.ds(nsend, per)], tab.at[pl.ds(pl.multiple_of(hub_base + g * per, per), per)],
                  ps.at[layer, r - 1], pr.at[layer, r - 1], r),
        )

    def start_halo(tab, layer):
        def one(r, carry):
            p = gpeer(r)
            halo[layer, p] = select_rows(tab, idx_ref[p])
            for copy in halo_copies(tab, layer, r):
                copy.start()
            return carry

        lax.fori_loop(1, ngraph, one, 0)
        tab[pl.ds(pl.multiple_of(hub_base + g * per, per), per)] = select_rows(tab, idx_ref[g, nsend:])

    def wait_halo(tab, layer):
        def arrive(r, carry):
            for copy in halo_copies(tab, layer, r):
                copy.wait_recv()
            return carry

        lax.fori_loop(1, ngraph, arrive, 0)

    inv = inv_ref[...]

    def chunk(i):
        return pl.ds(pl.multiple_of(i * DB, DB), DB)

    def product(a, tab):
        out = jnp.dot(jnp.concatenate(bf16_parts(a), axis=0), tab, preferred_element_type=F32)
        return out[:DB] + (out[DB:2 * DB] + out[2 * DB:])

    def a_copy(rb):
        return pltpu.make_async_copy(a_hbm.at[chunk(rb)], a_v.at[chunk(rb)], a_sem.at[rb])

    def own_part(tab, layer):
        def one(rb, carry):
            if layer == 0:
                a_copy(rb).wait()
            acc[chunk(rb)] = product(a_v[chunk(rb), :vert], tab[:vert])
            return carry

        lax.fori_loop(0, nblock + 1, one, 0)

    def far_part(tab, rb):
        return (acc[chunk(rb)] + product(a_v[chunk(rb), vert:], tab[vert:])) * inv

    def hub_copy(layer, r):
        p = gpeer(r)
        return grdma(hubsend.at[layer, pl.ds(pl.multiple_of(p * per, per), per)], hubrecv.at[layer, g], us.at[layer, r - 1], ur.at[layer, r - 1], r)

    def exchange_hubs(tab, layer):
        hubsend[layer] = far_part(tab, nblock)
        for r in range(1, ngraph):
            hub_copy(layer, r).start()
        hubrecv[layer, g] = hubsend[layer, pl.ds(pl.multiple_of(g * per, per), per)]

    def hub_totals(layer):
        for r in range(1, ngraph):
            hub_copy(layer, r).wait_recv()
        total = hubrecv[layer, 0]
        for p in range(1, ngraph):
            total = total + hubrecv[layer, p]
        fill = jnp.zeros((DB - 3 * per, total.shape[1]), BF16)
        tot[layer] = jnp.concatenate([*bf16_parts(total), fill], axis=0)

    def with_hubs(layer, rb):
        rows = lax.broadcasted_iota(jnp.int32, (DB, DB), 0) + rb * DB
        sel = jnp.where(rows == myhub_ref[...], F32(1), F32(0)).astype(BF16)
        return acc[chunk(rb)] + jnp.dot(sel, tot[layer], preferred_element_type=F32)

    start_halo(tab1, 0)
    own_part(tab1, 0)
    wait_halo(tab1, 0)
    exchange_hubs(tab1, 0)
    for copy in w2_copies:
        copy.wait_recv()

    def h_copy(i, r):
        return frdma(hsend.at[fpeer(r), chunk(i)], hin.at[f, chunk(i)], ns.at[i, r - 1], nr.at[i, r - 1], r)

    def z2_copy(i, r):
        return frdma(zout.at[fpeer(r), chunk(i)], tab2.at[pl.ds(pl.multiple_of(f * part + i * DB, DB), DB)], z2s.at[i, r - 1], z2r.at[i, r - 1], r)

    for copy in z1_copies:
        copy.wait_send()

    def z2_chunk(i):
        for r in range(1, nfeat):
            h_copy(i, r).wait_recv()
        acc = None
        for s in range(nfeat):
            term = jnp.dot(hin[s, chunk(i)], w2in[s], preferred_element_type=F32)
            acc = term if acc is None else acc + term
        acc = acc.astype(BF16)
        for q in range(nfeat):
            zout[q, chunk(i)] = acc[:, q * cols:(q + 1) * cols]
        for r in range(1, nfeat):
            z2_copy(i, r).start()
        tab2[pl.ds(pl.multiple_of(f * part + i * DB, DB), DB)] = zout[f, chunk(i)]

    bias1 = b1_ref[...]

    def place(t):
        i, rr = t // nfeat, lax.rem(t, nfeat)
        q = fpeer(rr + 1)
        return i, rr, q, q * nchunk + i

    def rows1(t, carry):
        @pl.when(t < nblock)
        def _():
            rb = place(t)[3]
            acc[chunk(rb)] = far_part(tab1, rb)

        @pl.when(t == LAG)
        def _():
            hub_totals(0)

        @pl.when(t >= LAG)
        def _():
            i, rr, q, rb = place(t - LAG)
            h = jnp.maximum(with_hubs(0, rb) + bias1, 0.0).astype(BF16)

            @pl.when(rr < nfeat - 1)
            def _():
                hsend[q, chunk(i)] = h
                h_copy(i, rr + 1).start()

            @pl.when(rr == nfeat - 1)
            def _():
                hin[f, chunk(i)] = h

            @pl.when((rr == nfeat - 2) & (i > 0))
            def _():
                z2_chunk(i - 1)

        return carry

    lax.fori_loop(0, nblock + LAG, rows1, 0)
    z2_chunk(nchunk - 1)
    for i in range(nchunk):
        for r in range(1, nfeat):
            z2_copy(i, r).wait_recv()

    start_halo(tab2, 1)
    own_part(tab2, 1)
    wait_halo(tab2, 1)
    exchange_hubs(tab2, 1)
    bias2 = b2_ref[...]

    def rows2(t, carry):
        @pl.when(t < nblock)
        def _():
            acc[chunk(t)] = far_part(tab2, t)

        @pl.when(t == LAG)
        def _():
            hub_totals(1)

        @pl.when(t >= LAG)
        def _():
            o_ref[chunk(t - LAG), :] = with_hubs(1, t - LAG) + bias2

        return carry

    lax.fori_loop(0, nblock + LAG, rows2, 0)

    for copy in x_copies + w1_copies + w2_copies:
        copy.wait_send()
    for i in range(nchunk):
        for r in range(1, nfeat):
            h_copy(i, r).wait_send()
            z2_copy(i, r).wait_send()
    for layer, tab in enumerate((tab1, tab2)):
        for r in range(1, ngraph):
            for copy in halo_copies(tab, layer, r):
                copy.wait_send()
            hub_copy(layer, r).wait_send()


def run_layers(nfeat, ngraph, nsend, per, x, w1, w2, idx, myhub, b1, b2, inv, adj):
    vert = x.shape[0]
    part, cols = vert // nfeat, b1.shape[1]
    nchunk, nblk = part // DB, adj.shape[0] // DB
    vm = lambda shape, dt: pltpu.VMEM(shape, dt)
    dma = lambda *shape: pltpu.SemaphoreType.DMA(shape)
    vspec = pl.BlockSpec(memory_space=pltpu.VMEM)
    fr, gr = nfeat - 1, ngraph - 1
    return pl.pallas_call(
        functools.partial(layers_kernel, (nfeat, ngraph, vert, nsend, per)),
        out_shape=jax.ShapeDtypeStruct((vert, cols), F32),
        in_specs=[vspec] * 8 + [pl.BlockSpec(memory_space=pl.ANY)],
        out_specs=vspec,
        scratch_shapes=[
            vm(adj.shape, F32), vm((adj.shape[0], cols), F32), vm((2, DB, cols), BF16), vm((nfeat, part, x.shape[1]), BF16), vm((nfeat, *w1.shape), BF16), vm((nfeat, *w2.shape), BF16),
            vm((adj.shape[1], cols), BF16), vm((adj.shape[1], cols), BF16), vm((nfeat, part, cols), BF16), vm((nfeat, part, cols), BF16),
            vm((nfeat, part, cols), BF16), vm((2, ngraph, nsend + per, cols), BF16), vm((2, ngraph * per, cols), F32), vm((2, ngraph, per, cols), F32),
            dma(nblk), dma(fr), dma(fr), dma(fr), dma(fr), dma(fr), dma(fr), dma(fr), dma(fr), dma(nchunk, fr), dma(nchunk, fr),
            dma(2, gr), dma(2, gr), dma(2, gr), dma(2, gr), dma(2, gr), dma(2, gr), dma(nchunk, fr), dma(nchunk, fr),
        ],
        compiler_params=pltpu.CompilerParams(collective_id=0, has_side_effects=True, vmem_limit_bytes=62 * 2**20),
        name="layers",
    )(x, w1, w2, idx, myhub, b1, b2, inv, adj)


def solution(mesh):
    rows_axes = ("data", "graph")
    nfeat = mesh.shape["feat"]
    ngraph = mesh.shape["graph"]

    def device_program(x_loc, dst_loc, src_loc, valid_loc, w_loc, send_loc, keep_loc, hub_ids, w_first, w_second, b_first, b_second):
        vert = x_loc.shape[0]
        nhub = hub_ids.shape[0]
        per = nhub // ngraph
        nsend = send_loc.shape[1]
        cols = b_first.shape[0]
        me = lax.axis_index("graph")
        ndb = (vert + nhub) // DB
        table_rows = vert + ngraph * nsend + nhub
        nsb = -(-table_rows // SB)

        owner = hub_ids // vert
        ks = jnp.arange(nhub)
        before = (owner[None, :] == owner[:, None]) & (ks[None, :] < ks[:, None])
        pos = owner * per + jnp.sum(before.astype(jnp.int32), axis=1)
        at_pos = pos[None, :] == ks[:, None]
        hub_by_pos = jnp.sum(jnp.where(at_pos, hub_ids[None, :], 0), axis=1)
        k_by_pos = jnp.sum(jnp.where(at_pos, ks[None, :], 0), axis=1)
        my_hubs = lax.dynamic_slice(hub_by_pos, (me * per,), (per,)) - me * vert

        key = ((dst_loc // DB) << 20) | ((src_loc // SB) << 15) | ((dst_loc % DB) << 8) | (src_loc % SB)
        key = jnp.where(valid_loc > 0, key, 1 << 26)
        coef = w_loc * valid_loc.astype(F32)
        large = jnp.max(coef) > 1e30
        coef = coef * jnp.where(large, F32(2.0**-40), F32(1))
        inv = jnp.where(large, F32(2.0**40), F32(1))
        nb = jnp.arange(ndb * nsb + 1)
        bound = ((nb // nsb) << 20) | ((nb % nsb) << 15)
        starts = jnp.sum((key[None, :] < bound[:, None]).astype(jnp.int32), axis=1)
        skey, sw = lax.sort((key, coef), num_keys=1, is_stable=False)
        sdst = (skey >> 20) * DB + ((skey >> 8) & (DB - 1))
        ssrc = ((skey >> 15) & 31) * SB + (skey & (SB - 1))
        edges = jnp.stack([sdst.astype(F32), ssrc.astype(F32), sw])
        edges = jnp.pad(edges, ((0, 5), (0, 2 * KW)), constant_values=-1.0)
        rowid = jnp.stack([jnp.arange(DB), k_by_pos]).astype(BF16)
        rowid = jnp.broadcast_to(rowid[:, :, None], (2, DB, KW))
        colid = jnp.pad(k_by_pos, (0, SB - nhub), constant_values=300).astype(BF16)
        colid = jnp.broadcast_to(colid[:, None], (SB, KW))
        adj = build_adjacency(starts, edges, rowid, colid, ndb, nsb)

        idx = jnp.where(keep_loc > 0, send_loc, -1)
        idx = jnp.concatenate([idx, jnp.broadcast_to(my_hubs[None, :], (ngraph, per))], axis=1)
        idx = jnp.broadcast_to(idx[:, :, None], (*idx.shape, DB))
        myhub = jnp.pad(jnp.concatenate([my_hubs] * 3), (0, DB - 3 * per), constant_values=-1)[None, :]
        inv = jnp.full((1, cols), inv)
        return run_layers(nfeat, ngraph, nsend, per, x_loc, w_first, w_second, idx, myhub, b_first[None, :], b_second[None, :], inv, adj)

    edge_spec = P(rows_axes)
    send_spec = P(rows_axes, None)
    in_specs = (P(rows_axes, "feat"), edge_spec, edge_spec, edge_spec, edge_spec, send_spec, send_spec, P("data"), P("feat", None), P("feat", None), P("feat"), P("feat"))
    return jax.shard_map(device_program, mesh=mesh, in_specs=in_specs, out_specs=P(rows_axes, "feat"), check_vma=False)
```

```python
import functools

import jax
import jax.numpy as jnp
from jax import lax
from jax.experimental import pallas as pl
from jax.experimental.pallas import tpu as pltpu
from jax.sharding import PartitionSpec as P

DB, SB, KW = 128, 256, 256
LAG = 4
MESH = pl.DeviceIdType.MESH
F32, BF16 = jnp.float32, jnp.bfloat16


def bf16_parts(x):
    hi = x.astype(BF16)
    rest = x - hi.astype(F32)
    mid = rest.astype(BF16)
    low = (rest - mid.astype(F32)).astype(BF16)
    return hi, mid, low


def build_kernel(ndb, nsb, starts_ref, edges_ref, hubcol_ref, a_ref):
    db = pl.program_id(0)
    dbase = (db * DB).astype(F32)
    hub_col = hubcol_ref[...]
    row_id = jnp.where(db == ndb - 1, hub_col, lax.broadcasted_iota(jnp.int32, (DB, 128), 0).astype(F32)).astype(BF16)
    row_id = jnp.concatenate([row_id] * (KW // 128), axis=1)
    iota_s = lax.broadcasted_iota(jnp.int32, (SB, KW), 0).astype(BF16)
    last_id = jnp.concatenate([hub_col, jnp.full((SB - DB, 128), 300.0, F32)], axis=0).astype(BF16)
    last_id = jnp.concatenate([last_id] * (KW // 128), axis=1)
    zero = jnp.zeros((), BF16)

    def window(sb, start):
        chunk = start // 128
        shift = start - chunk * 128
        raw = edges_ref[pl.ds(pl.multiple_of(chunk * 8, 8), 8 * (KW // 128 + 1)), :]
        raw = jnp.concatenate([raw[8 * i:8 * i + 8] for i in range(KW // 128 + 1)], axis=1)
        rows = pltpu.roll(raw, KW + 128 - shift, 1)[:, :KW]
        dst = (rows[0:1] - dbase).astype(BF16)
        src = (rows[1:2] - F32(SB * sb)).astype(BF16)
        hit = row_id == dst
        d3 = jnp.concatenate([jnp.where(hit, part, zero) for part in bf16_parts(rows[2:3])], axis=0)
        col_id = last_id if sb == nsb - 1 else iota_s
        sel = jnp.where(col_id == src, jnp.ones((), BF16), zero)
        out = lax.dot_general(d3, sel, (((1,), (1,)), ((), ())), preferred_element_type=F32)
        return out[:DB] + (out[DB:2 * DB] + out[2 * DB:])

    for sb in range(nsb):
        a_ref[:, sb * SB:(sb + 1) * SB] = window(sb, starts_ref[0, db * nsb + sb])
    for sb in range(nsb):
        start = starts_ref[0, db * nsb + sb]
        end = starts_ref[0, db * nsb + sb + 1]

        def more(i, carry):
            a_ref[:, sb * SB:(sb + 1) * SB] += window(sb, start + i * KW)
            return carry

        lax.fori_loop(1, (end - start + KW - 1) // KW, more, 0)


def build_adjacency(starts, edges, hub_col, ndb, nsb):
    return pl.pallas_call(
        functools.partial(build_kernel, ndb, nsb),
        out_shape=jax.ShapeDtypeStruct((ndb * DB, nsb * SB), F32),
        grid_spec=pltpu.PrefetchScalarGridSpec(
            num_scalar_prefetch=1,
            grid=(ndb,),
            in_specs=[pl.BlockSpec(edges.shape, lambda i, s: (0, 0)), pl.BlockSpec(hub_col.shape, lambda i, s: (0, 0))],
            out_specs=pl.BlockSpec((DB, nsb * SB), lambda i, s: (i, 0)),
        ),
        name="build",
    )(starts, edges, hub_col)


def iota2(axis):
    return lax.broadcasted_iota(jnp.int32, (8, 128), axis)


def sort_levels(kref, wref, first, last):
    sub, lane = iota2(0), iota2(1)

    def bit(b):
        return ((sub >> (b - 6)) & 1) == 1 if b < 9 else ((lane >> (b - 9)) & 1) == 1

    def within(level):
        steps = []
        for j in range(level - 1, 5, -1):
            high = bit(j)
            if level < 16:
                want_max = high != bit(level)
            else:
                want_max = high
            steps.append((j, high, want_max))

        def body(it, carry):
            pairs = [(kref[it * 16 + u], wref[it * 16 + u]) for u in range(16)]
            for j, high, want_max in steps:
                axis, m, size = (0, 1 << (j - 6), 8) if j < 9 else (1, 1 << (j - 9), 128)
                new = []
                index = (lane if axis else sub) ^ m
                for key, w in pairs:
                    if 2 * m == size:
                        pk, pw = pltpu.roll(key, m, axis), pltpu.roll(w, m, axis)
                    else:
                        pk = jnp.take_along_axis(key, index, axis=axis)
                        pw = jnp.take_along_axis(w, index, axis=axis)
                    nk = jnp.where(want_max, jnp.maximum(key, pk), jnp.minimum(key, pk))
                    new.append((nk, jnp.where(nk == key, w, pw)))
                pairs = new
            for u, (key, w) in enumerate(pairs):
                kref[it * 16 + u] = key
                wref[it * 16 + u] = w
            return carry

        lax.fori_loop(0, 4, body, 0)

    def across(level, top, low):
        base = 3 if low >= 3 else 0

        def body(it, carry):
            where_v = [(it + 8 * u) if base == 3 else (it * 8 + u) for u in range(8)]
            ks, ws = [kref[v] for v in where_v], [wref[v] for v in where_v]
            for j in range(top, low - 1, -1):
                m = 1 << (j - base)
                for u in range(8):
                    if u & m:
                        continue
                    a, b = u, u | m
                    down = None
                    if level < 6 and base <= level < base + 3:
                        flip = bool(u >> (level - base) & 1)
                        swap = (ks[a] < ks[b]) if flip else (ks[a] > ks[b])
                    elif level < 6:
                        down = jnp.full((8, 128), (it >> (level - 3 + base)) & 1, jnp.int32) == 1
                        swap = (ks[a] > ks[b]) != down
                    elif level < 16:
                        swap = (ks[a] > ks[b]) != bit(level)
                    else:
                        swap = ks[a] > ks[b]
                    ks[a], ks[b] = jnp.where(swap, ks[b], ks[a]), jnp.where(swap, ks[a], ks[b])
                    ws[a], ws[b] = jnp.where(swap, ws[b], ws[a]), jnp.where(swap, ws[a], ws[b])
            for u, v in enumerate(where_v):
                kref[v] = ks[u]
                wref[v] = ws[u]
            return carry

        lax.fori_loop(0, 8, body, 0)

    for level in range(first, last + 1):
        if level > 6:
            within(level)
        if level > 3:
            across(level, min(level - 1, 5), 3)
        across(level, min(level - 1, 2), 0)


def pre_kernel(dims, dst_ref, src_ref, valid_ref, w_ref, x_ref, w1_ref, w2_ref,
               edges_ref, starts_ref, tab_ref, w2all_ref, inv_ref,
               kref, wref, xin, w1in, w2in, tab, zout, xs, xr, w1s, w1r, w2s, w2r, zs, zr):
    nfeat, ngraph, ndb, nsb = dims
    vert = x_ref.shape[0]
    part = vert // nfeat
    f = lax.axis_index("feat")

    def fpeer(r):
        return lax.rem(f + r, nfeat)

    def frdma(src, dst, send, recv, r):
        return pltpu.make_async_remote_copy(src, dst, send, recv, device_id={"feat": fpeer(r)}, device_id_type=MESH)

    def quarter(q):
        return pl.ds(pl.multiple_of(q * part, part), part)

    barrier = pltpu.get_barrier_semaphore()
    for r in range(1, nfeat):
        pl.semaphore_signal(barrier, inc=1, device_id={"feat": fpeer(r)}, device_id_type=MESH)
    pl.semaphore_wait(barrier, nfeat - 1)
    peers = range(1, nfeat)
    x_copies = [frdma(x_ref.at[quarter(fpeer(r))], xin.at[f], xs.at[r - 1], xr.at[r - 1], r) for r in peers]
    w1_copies = [frdma(w1_ref, w1in.at[f], w1s.at[r - 1], w1r.at[r - 1], r) for r in peers]
    w2_copies = [frdma(w2_ref, w2in.at[f], w2s.at[r - 1], w2r.at[r - 1], r) for r in peers]
    z_copies = [frdma(zout.at[fpeer(r)], tab.at[quarter(f)], zs.at[r - 1], zr.at[r - 1], r) for r in peers]
    for copy in w1_copies + x_copies:
        copy.start()
    xin[f] = x_ref[quarter(f)]
    w1in[f] = w1_ref[...]
    w2in[f] = w2_ref[...]

    dst, src = dst_ref[...], src_ref[...]
    key = (((dst // DB) * nsb + src // SB) << 15) | ((dst % DB) << 8) | (src % SB)
    nbucket = ndb * nsb
    key = jnp.where(valid_ref[...] > 0, key, nbucket << 15).astype(F32)
    coef = w_ref[...] * valid_ref[...].astype(F32)
    large = jnp.max(coef, keepdims=True) > 1e30
    coef = coef * jnp.where(large, F32(2.0**-40), F32(1))
    inv_ref[...] = jnp.broadcast_to(jnp.where(large, F32(2.0**40), F32(1)), inv_ref.shape)
    used = dst.shape[0] // 8
    kref[:used] = key.reshape(used, 8, 128)
    wref[:used] = coef.reshape(used, 8, 128)
    kref[used:] = jnp.full((64 - used, 8, 128), nbucket << 15, F32)
    wref[used:] = jnp.zeros((64 - used, 8, 128), F32)
    sort_levels(kref, wref, 1, 11)

    for copy in w1_copies + x_copies:
        copy.wait_recv()
    cols = tab.shape[1]
    z = None
    for s in range(nfeat):
        term = jnp.dot(xin[s], w1in[s], preferred_element_type=F32)
        z = term if z is None else z + term
    z = z.astype(BF16)
    for q in range(nfeat):
        zout[q] = z[:, q * cols:(q + 1) * cols]
    for copy in z_copies + w2_copies:
        copy.start()
    tab[quarter(f)] = zout[f]
    sort_levels(kref, wref, 12, 16)

    nb = starts_ref.shape[1]
    bound = (lax.broadcasted_iota(jnp.int32, (nb, 1), 0) << 15).astype(F32)
    last = kref[63, 7:8, :]
    lane = lax.broadcasted_iota(jnp.int32, (1, 128), 1)
    before = jnp.where(lane == 0, F32(-1), pltpu.roll(last, 1, 1))
    full = last < bound
    row_sel = jnp.where((before < bound) & jnp.logical_not(full), F32(1), F32(0)).astype(BF16)
    keys = kref[...].reshape(512, 128)
    picked = None
    for piece in bf16_parts(keys):
        term = lax.dot_general(row_sel, piece, (((1,), (1,)), ((), ())), preferred_element_type=F32)
        picked = term if picked is None else picked + term
    inside = jnp.where(picked < bound, F32(1), F32(0)).astype(BF16)
    count = lax.dot_general(jnp.ones((8, 512), BF16), inside, (((1,), (1,)), ((), ())), preferred_element_type=F32)
    rows = lax.dot_general(jnp.ones((8, 128), BF16), jnp.where(full, F32(1), F32(0)).astype(BF16), (((1,), (1,)), ((), ())), preferred_element_type=F32)
    starts_ref[...] = (count + 512.0 * rows).astype(jnp.int32)

    nl = edges_ref.shape[0] // 32
    for k in range(4):
        kk = jnp.concatenate([kref[:, 2 * k, :], kref[:, 2 * k + 1, :]], axis=0)
        ww = jnp.concatenate([wref[:, 2 * k, :], wref[:, 2 * k + 1, :]], axis=0)
        ki = kk.astype(jnp.int32)
        bucket = ki >> 15
        block = jnp.floor((bucket.astype(F32) + 0.5) * F32(1.0 / nsb))
        edge_dst = block * DB + ((ki >> 8) & (DB - 1)).astype(F32)
        edge_src = (bucket.astype(F32) - block * nsb) * SB + (ki & (SB - 1)).astype(F32)
        for field, val in enumerate((edge_dst, edge_src, ww)):
            edges_ref[pl.ds(k * 8 + field, nl, stride=32), :] = val.T[:nl]

    for copy in z_copies + w2_copies:
        copy.wait_recv()
    tab_ref[...] = tab[...]
    w2all_ref[...] = w2in[...]
    for copy in x_copies + w1_copies + w2_copies + z_copies:
        copy.wait_send()


def run_pre(nfeat, ngraph, ndb, nsb, dst, src, valid, w, x, w1, w2):
    vert, part = x.shape[0], x.shape[0] // nfeat
    cols = w1.shape[1] // nfeat
    nrows = dst.shape[0]
    vm = lambda shape, dt: pltpu.VMEM(shape, dt)
    dma = pltpu.SemaphoreType.DMA((nfeat - 1,))
    vspec = pl.BlockSpec(memory_space=pltpu.VMEM)
    shape = jax.ShapeDtypeStruct
    return pl.pallas_call(
        functools.partial(pre_kernel, (nfeat, ngraph, ndb, nsb)),
        out_shape=[shape(((nrows + 4) * 8, 128), F32), shape((8, 384), jnp.int32), shape((vert, cols), BF16), shape((nfeat, *w2.shape), BF16), shape((1, cols), F32)],
        in_specs=[vspec] * 7,
        out_specs=[vspec] * 5,
        scratch_shapes=[
            vm((64, 8, 128), F32), vm((64, 8, 128), F32), vm((nfeat, part, x.shape[1]), BF16), vm((nfeat, *w1.shape), BF16), vm((nfeat, *w2.shape), BF16),
            vm((vert, cols), BF16), vm((nfeat, part, cols), BF16), dma, dma, dma, dma, dma, dma, dma, dma,
        ],
        compiler_params=pltpu.CompilerParams(collective_id=0, has_side_effects=True, vmem_limit_bytes=40 * 2**20),
        name="pre",
    )(dst, src, valid, w, x, w1, w2)


def layers_kernel(dims, tabown_ref, w2in, idx_ref, myhub_ref, b1_ref, b2_ref, inv_ref, a_hbm, o_ref,
                  a_v, acc, tot, tab1, tab2, zout, hsend, hin, halo, hubsend, hubrecv,
                  a_sem, z2s, z2r, hs, hr, ps, pr, us, ur, ns, nr):
    nfeat, ngraph, vert, nsend, per = dims
    part, rows_send = vert // nfeat, nsend + per
    nchunk = part // DB
    f, g = lax.axis_index("feat"), lax.axis_index("graph")
    halo_base, hub_base = vert, vert + ngraph * nsend
    nblock = vert // DB

    def fpeer(r):
        return lax.rem(f + r, nfeat)

    def gpeer(r):
        return lax.rem(g + r, ngraph)

    def frdma(src, dst, send, recv, r):
        return pltpu.make_async_remote_copy(src, dst, send, recv, device_id={"feat": fpeer(r)}, device_id_type=MESH)

    def grdma(src, dst, send, recv, r):
        return pltpu.make_async_remote_copy(src, dst, send, recv, device_id={"graph": gpeer(r)}, device_id_type=MESH)

    for i in range(a_hbm.shape[0] // DB):
        pltpu.make_async_copy(a_hbm.at[pl.ds(i * DB, DB)], a_v.at[pl.ds(i * DB, DB)], a_sem.at[i]).start()

    barrier = pltpu.get_barrier_semaphore()
    for r in range(1, nfeat):
        pl.semaphore_signal(barrier, inc=1, device_id={"feat": fpeer(r)}, device_id_type=MESH)
    for r in range(1, ngraph):
        pl.semaphore_signal(barrier, inc=1, device_id={"graph": gpeer(r)}, device_id_type=MESH)
    pl.semaphore_wait(barrier, nfeat + ngraph - 2)

    pad_rows = a_v.shape[1] - hub_base - ngraph * per
    for tab in (tab1, tab2):
        tab[pl.ds(pl.multiple_of(halo_base + g * nsend, nsend), nsend)] = jnp.zeros((nsend, tab.shape[1]), BF16)
        tab[hub_base + ngraph * per:] = jnp.zeros((pad_rows, tab.shape[1]), BF16)

    cols = tab1.shape[1]
    tab1[:vert] = tabown_ref[...]

    lane = lax.broadcasted_iota(jnp.int32, (1, DB), 1)

    def select_rows(tab, idx):
        pieces = [jnp.where(idx == lane + DB * j, F32(1), F32(0)).astype(BF16) for j in range(vert // DB)]
        return jnp.dot(jnp.concatenate(pieces, axis=1), tab[:vert], preferred_element_type=F32).astype(BF16)

    def halo_copies(tab, layer, r):
        p = gpeer(r)
        return (
            grdma(halo.at[layer, p, pl.ds(0, nsend)], tab.at[pl.ds(pl.multiple_of(halo_base + g * nsend, nsend), nsend)],
                  hs.at[layer, r - 1], hr.at[layer, r - 1], r),
            grdma(halo.at[layer, p, pl.ds(nsend, per)], tab.at[pl.ds(pl.multiple_of(hub_base + g * per, per), per)],
                  ps.at[layer, r - 1], pr.at[layer, r - 1], r),
        )

    def start_halo(tab, layer):
        def one(r, carry):
            p = gpeer(r)
            halo[layer, p] = select_rows(tab, idx_ref[p])
            for copy in halo_copies(tab, layer, r):
                copy.start()
            return carry

        lax.fori_loop(1, ngraph, one, 0)
        tab[pl.ds(pl.multiple_of(hub_base + g * per, per), per)] = select_rows(tab, idx_ref[g, nsend:])

    def wait_halo(tab, layer):
        def arrive(r, carry):
            for copy in halo_copies(tab, layer, r):
                copy.wait_recv()
            return carry

        lax.fori_loop(1, ngraph, arrive, 0)

    inv = inv_ref[...]

    def chunk(i):
        return pl.ds(pl.multiple_of(i * DB, DB), DB)

    def product(a, tab):
        out = jnp.dot(jnp.concatenate(bf16_parts(a), axis=0), tab, preferred_element_type=F32)
        return out[:DB] + (out[DB:2 * DB] + out[2 * DB:])

    def a_copy(rb):
        return pltpu.make_async_copy(a_hbm.at[chunk(rb)], a_v.at[chunk(rb)], a_sem.at[rb])

    def own_part(tab, layer):
        def one(rb, carry):
            if layer == 0:
                a_copy(rb).wait()
            acc[chunk(rb)] = product(a_v[chunk(rb), :vert], tab[:vert])
            return carry

        lax.fori_loop(0, nblock + 1, one, 0)

    def far_part(tab, rb):
        return (acc[chunk(rb)] + product(a_v[chunk(rb), vert:], tab[vert:])) * inv

    def hub_copy(layer, r):
        p = gpeer(r)
        return grdma(hubsend.at[layer, pl.ds(pl.multiple_of(p * per, per), per)], hubrecv.at[layer, g], us.at[layer, r - 1], ur.at[layer, r - 1], r)

    def exchange_hubs(tab, layer):
        hubsend[layer] = far_part(tab, nblock)
        for r in range(1, ngraph):
            hub_copy(layer, r).start()
        hubrecv[layer, g] = hubsend[layer, pl.ds(pl.multiple_of(g * per, per), per)]

    def hub_totals(layer):
        for r in range(1, ngraph):
            hub_copy(layer, r).wait_recv()
        total = hubrecv[layer, 0]
        for p in range(1, ngraph):
            total = total + hubrecv[layer, p]
        fill = jnp.zeros((DB - 3 * per, total.shape[1]), BF16)
        tot[layer] = jnp.concatenate([*bf16_parts(total), fill], axis=0)

    def with_hubs(layer, rb):
        rows = lax.broadcasted_iota(jnp.int32, (DB, DB), 0) + rb * DB
        sel = jnp.where(rows == myhub_ref[...], F32(1), F32(0)).astype(BF16)
        return acc[chunk(rb)] + jnp.dot(sel, tot[layer], preferred_element_type=F32)

    start_halo(tab1, 0)
    own_part(tab1, 0)
    wait_halo(tab1, 0)
    exchange_hubs(tab1, 0)
    def h_copy(i, r):
        return frdma(hsend.at[fpeer(r), chunk(i)], hin.at[f, chunk(i)], ns.at[i, r - 1], nr.at[i, r - 1], r)

    def z2_copy(i, r):
        return frdma(zout.at[fpeer(r), chunk(i)], tab2.at[pl.ds(pl.multiple_of(f * part + i * DB, DB), DB)], z2s.at[i, r - 1], z2r.at[i, r - 1], r)

    def z2_chunk(i):
        for r in range(1, nfeat):
            h_copy(i, r).wait_recv()
        acc = None
        for s in range(nfeat):
            term = jnp.dot(hin[s, chunk(i)], w2in[s], preferred_element_type=F32)
            acc = term if acc is None else acc + term
        acc = acc.astype(BF16)
        for q in range(nfeat):
            zout[q, chunk(i)] = acc[:, q * cols:(q + 1) * cols]
        for r in range(1, nfeat):
            z2_copy(i, r).start()
        tab2[pl.ds(pl.multiple_of(f * part + i * DB, DB), DB)] = zout[f, chunk(i)]

    bias1 = b1_ref[...]

    def place(t):
        i, rr = t // nfeat, lax.rem(t, nfeat)
        q = fpeer(rr + 1)
        return i, rr, q, q * nchunk + i

    def rows1(t, carry):
        @pl.when(t < nblock)
        def _():
            rb = place(t)[3]
            acc[chunk(rb)] = far_part(tab1, rb)

        @pl.when(t == LAG)
        def _():
            hub_totals(0)

        @pl.when(t >= LAG)
        def _():
            i, rr, q, rb = place(t - LAG)
            h = jnp.maximum(with_hubs(0, rb) + bias1, 0.0).astype(BF16)

            @pl.when(rr < nfeat - 1)
            def _():
                hsend[q, chunk(i)] = h
                h_copy(i, rr + 1).start()

            @pl.when(rr == nfeat - 1)
            def _():
                hin[f, chunk(i)] = h

            @pl.when((rr == nfeat - 2) & (i > 0))
            def _():
                z2_chunk(i - 1)

        return carry

    lax.fori_loop(0, nblock + LAG, rows1, 0)
    z2_chunk(nchunk - 1)
    for i in range(nchunk):
        for r in range(1, nfeat):
            z2_copy(i, r).wait_recv()

    start_halo(tab2, 1)
    own_part(tab2, 1)
    wait_halo(tab2, 1)
    exchange_hubs(tab2, 1)
    bias2 = b2_ref[...]

    def rows2(t, carry):
        @pl.when(t < nblock)
        def _():
            acc[chunk(t)] = far_part(tab2, t)

        @pl.when(t == LAG)
        def _():
            hub_totals(1)

        @pl.when(t >= LAG)
        def _():
            o_ref[chunk(t - LAG), :] = with_hubs(1, t - LAG) + bias2

        return carry

    lax.fori_loop(0, nblock + LAG, rows2, 0)

    for i in range(nchunk):
        for r in range(1, nfeat):
            h_copy(i, r).wait_send()
            z2_copy(i, r).wait_send()
    for layer, tab in enumerate((tab1, tab2)):
        for r in range(1, ngraph):
            for copy in halo_copies(tab, layer, r):
                copy.wait_send()
            hub_copy(layer, r).wait_send()


def run_layers(nfeat, ngraph, nsend, per, tab_own, w2, idx, myhub, b1, b2, inv, adj):
    vert = tab_own.shape[0]
    part, cols = vert // nfeat, b1.shape[1]
    nchunk, nblk = part // DB, adj.shape[0] // DB
    vm = lambda shape, dt: pltpu.VMEM(shape, dt)
    dma = lambda *shape: pltpu.SemaphoreType.DMA(shape)
    vspec = pl.BlockSpec(memory_space=pltpu.VMEM)
    fr, gr = nfeat - 1, ngraph - 1
    return pl.pallas_call(
        functools.partial(layers_kernel, (nfeat, ngraph, vert, nsend, per)),
        out_shape=jax.ShapeDtypeStruct((vert, cols), F32),
        in_specs=[vspec] * 7 + [pl.BlockSpec(memory_space=pl.ANY)],
        out_specs=vspec,
        scratch_shapes=[
            vm(adj.shape, F32), vm((adj.shape[0], cols), F32), vm((2, DB, cols), BF16),
            vm((adj.shape[1], cols), BF16), vm((adj.shape[1], cols), BF16), vm((nfeat, part, cols), BF16), vm((nfeat, part, cols), BF16),
            vm((nfeat, part, cols), BF16), vm((2, ngraph, nsend + per, cols), BF16), vm((2, ngraph * per, cols), F32), vm((2, ngraph, per, cols), F32),
            dma(nblk), dma(nchunk, fr), dma(nchunk, fr),
            dma(2, gr), dma(2, gr), dma(2, gr), dma(2, gr), dma(2, gr), dma(2, gr), dma(nchunk, fr), dma(nchunk, fr),
        ],
        compiler_params=pltpu.CompilerParams(collective_id=1, has_side_effects=True, vmem_limit_bytes=62 * 2**20),
        name="layers",
    )(tab_own, w2, idx, myhub, b1, b2, inv, adj)


def solution(mesh):
    rows_axes = ("data", "graph")
    nfeat = mesh.shape["feat"]
    ngraph = mesh.shape["graph"]

    def device_program(x_loc, dst_loc, src_loc, valid_loc, w_loc, send_loc, keep_loc, hub_ids, w_first, w_second, b_first, b_second):
        vert = x_loc.shape[0]
        nhub = hub_ids.shape[0]
        per = nhub // ngraph
        nsend = send_loc.shape[1]
        me = lax.axis_index("graph")
        ndb = (vert + nhub) // DB
        table_rows = vert + ngraph * nsend + nhub
        nsb = -(-table_rows // SB)

        owner = hub_ids // vert
        ks = jnp.arange(nhub)
        before = (owner[None, :] == owner[:, None]) & (ks[None, :] < ks[:, None])
        pos = owner * per + jnp.sum(before.astype(jnp.int32), axis=1)
        at_pos = pos[None, :] == ks[:, None]
        hub_by_pos = jnp.sum(jnp.where(at_pos, hub_ids[None, :], 0), axis=1)
        k_by_pos = jnp.sum(jnp.where(at_pos, ks[None, :], 0), axis=1)
        my_hubs = lax.dynamic_slice(hub_by_pos, (me * per,), (per,)) - me * vert

        grid = lambda v: v.reshape(-1, 128)
        edges, starts, tab_own, w2_all, inv = run_pre(nfeat, ngraph, ndb, nsb, grid(dst_loc), grid(src_loc), grid(valid_loc), grid(w_loc), x_loc, w_first, w_second)
        hub_col = jnp.broadcast_to(k_by_pos.astype(F32)[:, None], (DB, 128))
        adj = build_adjacency(starts, edges, hub_col, ndb, nsb)

        idx = jnp.where(keep_loc > 0, send_loc, -1)
        idx = jnp.concatenate([idx, jnp.broadcast_to(my_hubs[None, :], (ngraph, per))], axis=1)
        idx = jnp.broadcast_to(idx[:, :, None], (*idx.shape, DB))
        myhub = jnp.pad(jnp.concatenate([my_hubs] * 3), (0, DB - 3 * per), constant_values=-1)[None, :]
        return run_layers(nfeat, ngraph, nsend, per, tab_own, w2_all, idx, myhub, b_first[None, :], b_second[None, :], inv, adj)

    edge_spec = P(rows_axes)
    send_spec = P(rows_axes, None)
    in_specs = (P(rows_axes, "feat"), edge_spec, edge_spec, edge_spec, edge_spec, send_spec, send_spec, P("data"), P("feat", None), P("feat", None), P("feat"), P("feat"))
    return jax.shard_map(device_program, mesh=mesh, in_specs=in_specs, out_specs=P(rows_axes, "feat"), check_vma=False)
```

```python
import functools

import jax
import jax.numpy as jnp
from jax import lax
from jax.experimental import pallas as pl
from jax.experimental.pallas import tpu as pltpu
from jax.sharding import PartitionSpec as P

DB, SB, KW = 128, 256, 256
MESH = pl.DeviceIdType.MESH
F32, BF16 = jnp.float32, jnp.bfloat16


def bf16_parts(x):
    hi = x.astype(BF16)
    rest = x - hi.astype(F32)
    mid = rest.astype(BF16)
    low = (rest - mid.astype(F32)).astype(BF16)
    return hi, mid, low


def build_kernel(ndb, nsb, ncol, starts_ref, edges_ref, hubcol_ref, a_ref):
    db = pl.program_id(0)
    dbase = (db * DB).astype(F32)
    hub_col = hubcol_ref[...]
    row_id = jnp.where(db == ndb - 1, hub_col, lax.broadcasted_iota(jnp.int32, (DB, 128), 0).astype(F32)).astype(BF16)
    iota_s = lax.broadcasted_iota(jnp.int32, (SB, 128), 0).astype(BF16)
    zero = jnp.zeros((), BF16)

    def window(sb, start, slots):
        width = min(SB, ncol - sb * SB)
        chunk = start // 128
        shift = start - chunk * 128
        raw = edges_ref[pl.ds(pl.multiple_of(chunk * 8, 8), 8 * (slots // 128 + 1)), :]
        raw = jnp.concatenate([raw[8 * i:8 * i + 8] for i in range(slots // 128 + 1)], axis=1)
        rows = pltpu.roll(raw, slots + 128 - shift, 1)[:, :slots]
        dst = (rows[0:1] - dbase).astype(BF16)
        src = (rows[1:2] - F32(SB * sb)).astype(BF16)
        tiled = lambda v: jnp.concatenate([v] * (slots // 128), axis=1)
        hit = tiled(row_id) == dst
        d3 = jnp.concatenate([jnp.where(hit, part, zero) for part in bf16_parts(rows[2:3])], axis=0)
        col_id = hub_col.astype(BF16) if sb == nsb - 1 else iota_s
        sel = jnp.where(tiled(col_id) == src, jnp.ones((), BF16), zero)
        out = lax.dot_general(d3, sel, (((1,), (1,)), ((), ())), preferred_element_type=F32)
        return out[:DB] + (out[DB:2 * DB] + out[2 * DB:]), slice(sb * SB, sb * SB + width)

    slots = [KW] * (nsb - 1) + [2 * KW]
    over = None
    for sb in range(nsb):
        start = starts_ref[0, db * nsb + sb]
        more = starts_ref[0, db * nsb + sb + 1] - start - slots[sb]
        over = more if over is None else jnp.maximum(over, more)
        block, where = window(sb, start, slots[sb])
        a_ref[:, where] = block

    @pl.when(over > 0)
    def _():
        for sb in range(nsb):
            start = starts_ref[0, db * nsb + sb] + slots[sb]
            end = starts_ref[0, db * nsb + sb + 1]

            def step(i, carry):
                block, where = window(sb, start + i * KW, KW)
                a_ref[:, where] += block
                return carry

            lax.fori_loop(0, (jnp.maximum(end - start, 0) + KW - 1) // KW, step, 0)


def build_adjacency(starts, edges, hub_col, ndb, nsb, ncol):
    return pl.pallas_call(
        functools.partial(build_kernel, ndb, nsb, ncol),
        out_shape=jax.ShapeDtypeStruct((ndb * DB, ncol), F32),
        grid_spec=pltpu.PrefetchScalarGridSpec(
            num_scalar_prefetch=1,
            grid=(ndb,),
            in_specs=[pl.BlockSpec(edges.shape, lambda i, s: (0, 0)), pl.BlockSpec(hub_col.shape, lambda i, s: (0, 0))],
            out_specs=pl.BlockSpec((DB, ncol), lambda i, s: (i, 0)),
        ),
        name="build",
    )(starts, edges, hub_col)


def iota2(axis):
    return lax.broadcasted_iota(jnp.int32, (8, 128), axis)


def sort_levels(kref, wref, first, last):
    sub, lane = iota2(0), iota2(1)

    def bit(b):
        return ((sub >> (b - 6)) & 1) == 1 if b < 9 else ((lane >> (b - 9)) & 1) == 1

    def within(level):
        steps = []
        for j in range(level - 1, 5, -1):
            high = bit(j)
            if level < 16:
                want_max = high != bit(level)
            else:
                want_max = high
            steps.append((j, high, want_max))

        def body(it, carry):
            pairs = [(kref[it * 16 + u], wref[it * 16 + u]) for u in range(16)]
            for j, high, want_max in steps:
                axis, m, size = (0, 1 << (j - 6), 8) if j < 9 else (1, 1 << (j - 9), 128)
                new = []
                index = (lane if axis else sub) ^ m
                for key, w in pairs:
                    if 2 * m == size:
                        pk, pw = pltpu.roll(key, m, axis), pltpu.roll(w, m, axis)
                    else:
                        pk = jnp.take_along_axis(key, index, axis=axis)
                        pw = jnp.take_along_axis(w, index, axis=axis)
                    nk = jnp.where(want_max, jnp.maximum(key, pk), jnp.minimum(key, pk))
                    new.append((nk, jnp.where(nk == key, w, pw)))
                pairs = new
            for u, (key, w) in enumerate(pairs):
                kref[it * 16 + u] = key
                wref[it * 16 + u] = w
            return carry

        lax.fori_loop(0, 4, body, 0)

    def across(level, top, low):
        base = 3 if low >= 3 else 0

        def body(it, carry):
            where_v = [(it + 8 * u) if base == 3 else (it * 8 + u) for u in range(8)]
            ks, ws = [kref[v] for v in where_v], [wref[v] for v in where_v]
            for j in range(top, low - 1, -1):
                m = 1 << (j - base)
                for u in range(8):
                    if u & m:
                        continue
                    a, b = u, u | m
                    down = None
                    if level < 6 and base <= level < base + 3:
                        flip = bool(u >> (level - base) & 1)
                        swap = (ks[a] < ks[b]) if flip else (ks[a] > ks[b])
                    elif level < 6:
                        down = jnp.full((8, 128), (it >> (level - 3 + base)) & 1, jnp.int32) == 1
                        swap = (ks[a] > ks[b]) != down
                    elif level < 16:
                        swap = (ks[a] > ks[b]) != bit(level)
                    else:
                        swap = ks[a] > ks[b]
                    ks[a], ks[b] = jnp.where(swap, ks[b], ks[a]), jnp.where(swap, ks[a], ks[b])
                    ws[a], ws[b] = jnp.where(swap, ws[b], ws[a]), jnp.where(swap, ws[a], ws[b])
            for u, v in enumerate(where_v):
                kref[v] = ks[u]
                wref[v] = ws[u]
            return carry

        lax.fori_loop(0, 8, body, 0)

    for level in range(first, last + 1):
        if level > 6:
            within(level)
        if level > 3:
            across(level, min(level - 1, 5), 3)
        across(level, min(level - 1, 2), 0)


def pre_kernel(dims, dst_ref, src_ref, valid_ref, w_ref, x_ref, w1_ref, hub_ref, send_ref, keep_ref,
               edges_ref, starts_ref, tab_ref, inv_ref, hubcol_ref, myhub_ref, idx_ref,
               kref, wref, xin, w1in, tab, zout, xs, xr, w1s, w1r, zs, zr):
    nfeat, ngraph, ndb, nsb = dims
    vert = x_ref.shape[0]
    part = vert // nfeat
    f = lax.axis_index("feat")

    def fpeer(r):
        return lax.rem(f + r, nfeat)

    def frdma(src, dst, send, recv, r):
        return pltpu.make_async_remote_copy(src, dst, send, recv, device_id={"feat": fpeer(r)}, device_id_type=MESH)

    def quarter(q):
        return pl.ds(pl.multiple_of(q * part, part), part)

    barrier = pltpu.get_barrier_semaphore()
    for r in range(1, nfeat):
        pl.semaphore_signal(barrier, inc=1, device_id={"feat": fpeer(r)}, device_id_type=MESH)
    pl.semaphore_wait(barrier, nfeat - 1)
    peers = range(1, nfeat)
    x_copies = [frdma(x_ref.at[quarter(fpeer(r))], xin.at[f], xs.at[r - 1], xr.at[r - 1], r) for r in peers]
    w1_copies = [frdma(w1_ref, w1in.at[f], w1s.at[r - 1], w1r.at[r - 1], r) for r in peers]
    z_copies = [frdma(zout.at[fpeer(r)], tab.at[quarter(f)], zs.at[r - 1], zr.at[r - 1], r) for r in peers]
    for copy in w1_copies + x_copies:
        copy.start()
    xin[f] = x_ref[quarter(f)]
    w1in[f] = w1_ref[...]

    dst, src = dst_ref[...], src_ref[...]
    key = (((dst // DB) * nsb + src // SB) << 15) | ((dst % DB) << 8) | (src % SB)
    nbucket = ndb * nsb
    key = jnp.where(valid_ref[...] > 0, key, nbucket << 15).astype(F32)
    coef = w_ref[...] * valid_ref[...].astype(F32)
    large = jnp.max(coef, keepdims=True) > 1e30
    coef = coef * jnp.where(large, F32(2.0**-40), F32(1))
    inv_ref[...] = jnp.broadcast_to(jnp.where(large, F32(2.0**40), F32(1)), inv_ref.shape)
    used = dst.shape[0] // 8
    kref[:used] = key.reshape(used, 8, 128)
    wref[:used] = coef.reshape(used, 8, 128)
    kref[used:] = jnp.full((64 - used, 8, 128), nbucket << 15, F32)
    wref[used:] = jnp.zeros((64 - used, 8, 128), F32)
    sort_levels(kref, wref, 1, 12)

    g, per = lax.axis_index("graph"), DB // ngraph
    lane_id = lax.broadcasted_iota(jnp.int32, (DB, DB), 1).astype(F32)
    row_id = lax.broadcasted_iota(jnp.int32, (DB, DB), 0).astype(F32)
    down = lambda row: jnp.broadcast_to(row, (DB, DB)).T
    ids = hub_ref[...].astype(F32)
    owner = (hub_ref[...] // vert).astype(F32)
    owner_down = down(owner)
    earlier = (owner == owner_down) & (lane_id < row_id)
    pos_down = owner_down * per + jnp.sum(jnp.where(earlier, F32(1), F32(0)), axis=1, keepdims=True)
    pos = pos_down.T
    base = (g * per).astype(F32)
    first = (g * vert).astype(F32)
    hubcol_ref[...] = jnp.broadcast_to(jnp.sum(jnp.where(pos == row_id, lane_id, F32(0)), axis=1, keepdims=True), (DB, DB))
    lane_row = lax.broadcasted_iota(jnp.int32, (1, DB), 1)
    target = (lane_row % per).astype(F32) + base
    mine = jnp.sum(jnp.where(pos_down == target, down(ids), F32(0)), axis=0, keepdims=True) - first
    myhub_ref[...] = jnp.where(lane_row < 3 * per, mine, F32(-1)).astype(jnp.int32)
    mine_down = jnp.sum(jnp.where(pos == row_id + base, ids, F32(0)), axis=1, keepdims=True) - first
    mine_down = jnp.broadcast_to(mine_down, (DB, DB))[:per].astype(jnp.int32)
    rows = jnp.where(keep_ref[...] > 0, send_ref[...], -1).astype(F32)
    nsend = rows.shape[1]
    for p in range(ngraph):
        for h in range(nsend // DB):
            idx_ref[p, h * DB:(h + 1) * DB] = down(rows[p:p + 1, h * DB:(h + 1) * DB]).astype(jnp.int32)
        idx_ref[p, nsend:] = mine_down

    for copy in w1_copies + x_copies:
        copy.wait_recv()
    cols = tab.shape[1]
    z = None
    for s in range(nfeat):
        term = jnp.dot(xin[s], w1in[s], preferred_element_type=F32)
        z = term if z is None else z + term
    z = z.astype(BF16)
    for q in range(nfeat):
        zout[q] = z[:, q * cols:(q + 1) * cols]
    for copy in z_copies:
        copy.start()
    tab[quarter(f)] = zout[f]
    sort_levels(kref, wref, 13, 16)

    nb = starts_ref.shape[1]
    bound = (lax.broadcasted_iota(jnp.int32, (nb, 1), 0) << 15).astype(F32)
    last = kref[63, 7:8, :]
    lane = lax.broadcasted_iota(jnp.int32, (1, 128), 1)
    before = jnp.where(lane == 0, F32(-1), pltpu.roll(last, 1, 1))
    full = last < bound
    row_sel = jnp.where((before < bound) & jnp.logical_not(full), F32(1), F32(0)).astype(BF16)
    keys = kref[...].reshape(512, 128)
    picked = None
    for piece in bf16_parts(keys):
        term = lax.dot_general(row_sel, piece, (((1,), (1,)), ((), ())), preferred_element_type=F32)
        picked = term if picked is None else picked + term
    inside = jnp.where(picked < bound, F32(1), F32(0)).astype(BF16)
    count = lax.dot_general(jnp.ones((8, 512), BF16), inside, (((1,), (1,)), ((), ())), preferred_element_type=F32)
    rows = lax.dot_general(jnp.ones((8, 128), BF16), jnp.where(full, F32(1), F32(0)).astype(BF16), (((1,), (1,)), ((), ())), preferred_element_type=F32)
    starts_ref[...] = (count + 512.0 * rows).astype(jnp.int32)

    nl = edges_ref.shape[0] // 32
    for k in range(4):
        kk = jnp.concatenate([kref[:, 2 * k, :], kref[:, 2 * k + 1, :]], axis=0)
        ww = jnp.concatenate([wref[:, 2 * k, :], wref[:, 2 * k + 1, :]], axis=0)
        ki = kk.astype(jnp.int32)
        bucket = ki >> 15
        block = jnp.floor((bucket.astype(F32) + 0.5) * F32(1.0 / nsb))
        edge_dst = block * DB + ((ki >> 8) & (DB - 1)).astype(F32)
        edge_src = (bucket.astype(F32) - block * nsb) * SB + (ki & (SB - 1)).astype(F32)
        for field, val in enumerate((edge_dst, edge_src, ww)):
            edges_ref[pl.ds(k * 8 + field, nl, stride=32), :] = val.T[:nl]

    for copy in z_copies:
        copy.wait_recv()
    tab_ref[...] = tab[...]
    for copy in x_copies + w1_copies + z_copies:
        copy.wait_send()


def run_pre(nfeat, ngraph, ndb, nsb, dst, src, valid, w, x, w1, hubs, send, keep):
    vert, part = x.shape[0], x.shape[0] // nfeat
    cols = w1.shape[1] // nfeat
    nrows = dst.shape[0]
    vm = lambda shape, dt: pltpu.VMEM(shape, dt)
    dma = pltpu.SemaphoreType.DMA((nfeat - 1,))
    vspec = pl.BlockSpec(memory_space=pltpu.VMEM)
    shape = jax.ShapeDtypeStruct
    return pl.pallas_call(
        functools.partial(pre_kernel, (nfeat, ngraph, ndb, nsb)),
        out_shape=[shape(((nrows + 8) * 8, 128), F32), shape((8, 384), jnp.int32), shape((vert, cols), BF16), shape((1, cols), F32),
                   shape((DB, DB), F32), shape((1, DB), jnp.int32), shape((ngraph, send.shape[1] + DB // ngraph, DB), jnp.int32)],
        in_specs=[vspec] * 9,
        out_specs=[vspec] * 7,
        scratch_shapes=[
            vm((64, 8, 128), F32), vm((64, 8, 128), F32), vm((nfeat, part, x.shape[1]), BF16), vm((nfeat, *w1.shape), BF16),
            vm((vert, cols), BF16), vm((nfeat, part, cols), BF16), dma, dma, dma, dma, dma, dma,
        ],
        compiler_params=pltpu.CompilerParams(collective_id=0, has_side_effects=True, vmem_limit_bytes=62 * 2**20),
        name="pre",
    )(dst, src, valid, w, x, w1, hubs, send, keep)


def layers_kernel(dims, tabown_ref, w2_ref, idx_ref, myhub_ref, b1_ref, inv_ref, a_hbm, o_ref,
                  a_v, acc, tot, w2in, tab1, tab2, zout, hsend, hin, halo, hubsend, hubrecv,
                  a_sem, w2s, w2r, z2s, z2r, hs, hr, ps, pr, us, ur, ns, nr):
    nfeat, ngraph, vert, nsend, per = dims
    part, rows_send = vert // nfeat, nsend + per
    nchunk = part // DB
    f, g = lax.axis_index("feat"), lax.axis_index("graph")
    halo_base, hub_base = vert, vert + ngraph * nsend
    nblock = vert // DB

    def fpeer(r):
        return lax.rem(f + r, nfeat)

    def gpeer(r):
        return lax.rem(g + r, ngraph)

    def frdma(src, dst, send, recv, r):
        return pltpu.make_async_remote_copy(src, dst, send, recv, device_id={"feat": fpeer(r)}, device_id_type=MESH)

    def grdma(src, dst, send, recv, r):
        return pltpu.make_async_remote_copy(src, dst, send, recv, device_id={"graph": gpeer(r)}, device_id_type=MESH)

    for i in range(a_hbm.shape[0] // DB):
        pltpu.make_async_copy(a_hbm.at[pl.ds(i * DB, DB)], a_v.at[pl.ds(i * DB, DB)], a_sem.at[i]).start()

    barrier = pltpu.get_barrier_semaphore()
    for r in range(1, nfeat):
        pl.semaphore_signal(barrier, inc=1, device_id={"feat": fpeer(r)}, device_id_type=MESH)
    for r in range(1, ngraph):
        pl.semaphore_signal(barrier, inc=1, device_id={"graph": gpeer(r)}, device_id_type=MESH)
    pl.semaphore_wait(barrier, nfeat + ngraph - 2)

    w2_copies = [frdma(w2_ref, w2in.at[f], w2s.at[r - 1], w2r.at[r - 1], r) for r in range(1, nfeat)]
    for copy in w2_copies:
        copy.start()
    w2in[f] = w2_ref[...]
    for tab in (tab1, tab2):
        tab[pl.ds(pl.multiple_of(halo_base + g * nsend, nsend), nsend)] = jnp.zeros((nsend, tab.shape[1]), BF16)

    cols = tab1.shape[1]
    tab1[:vert] = tabown_ref[...]

    lane = lax.broadcasted_iota(jnp.int32, (1, DB), 1)

    def select_rows(tab, idx):
        pieces = [jnp.where(idx == lane + DB * j, F32(1), F32(0)).astype(BF16) for j in range(vert // DB)]
        return jnp.dot(jnp.concatenate(pieces, axis=1), tab[:vert], preferred_element_type=F32).astype(BF16)

    def halo_copies(tab, layer, r):
        p = gpeer(r)
        return (
            grdma(halo.at[layer, p, pl.ds(0, nsend)], tab.at[pl.ds(pl.multiple_of(halo_base + g * nsend, nsend), nsend)],
                  hs.at[layer, r - 1], hr.at[layer, r - 1], r),
            grdma(halo.at[layer, p, pl.ds(nsend, per)], tab.at[pl.ds(pl.multiple_of(hub_base + g * per, per), per)],
                  ps.at[layer, r - 1], pr.at[layer, r - 1], r),
        )

    def start_halo(tab, layer):
        def one(r, carry):
            p = gpeer(r)
            halo[layer, p] = select_rows(tab, idx_ref[p])
            for copy in halo_copies(tab, layer, r):
                copy.start()
            return carry

        lax.fori_loop(1, ngraph, one, 0)
        tab[pl.ds(pl.multiple_of(hub_base + g * per, per), per)] = select_rows(tab, idx_ref[g, nsend:])

    def wait_halo(tab, layer):
        def arrive(r, carry):
            for copy in halo_copies(tab, layer, r):
                copy.wait_recv()
            return carry

        lax.fori_loop(1, ngraph, arrive, 0)

    inv = inv_ref[...]

    def chunk(i):
        return pl.ds(pl.multiple_of(i * DB, DB), DB)

    def product(a, tab):
        out = jnp.dot(jnp.concatenate(bf16_parts(a), axis=0), tab, preferred_element_type=F32)
        return out[:DB] + (out[DB:2 * DB] + out[2 * DB:])

    def a_copy(rb):
        return pltpu.make_async_copy(a_hbm.at[chunk(rb)], a_v.at[chunk(rb)], a_sem.at[rb])

    def own_part(tab, layer):
        def one(rb):
            acc[chunk(rb)] = product(a_v[chunk(rb), :vert], tab[:vert])

        def four(i, carry):
            if layer == 0:
                for u in range(4):
                    a_copy(4 * i + u).wait()
            for u in range(4):
                one(4 * i + u)
            return carry

        lax.fori_loop(0, nblock // 4, four, 0)
        if layer == 0:
            a_copy(nblock).wait()
        one(nblock)

    def far_part(tab, rb):
        return (acc[chunk(rb)] + product(a_v[chunk(rb), vert:], tab[vert:])) * inv

    def hub_copy(layer, r):
        p = gpeer(r)
        return grdma(hubsend.at[layer, pl.ds(pl.multiple_of(p * per, per), per)], hubrecv.at[layer, g], us.at[layer, r - 1], ur.at[layer, r - 1], r)

    def exchange_hubs(tab, layer):
        hubsend[layer] = far_part(tab, nblock)
        for r in range(1, ngraph):
            hub_copy(layer, r).start()
        hubrecv[layer, g] = hubsend[layer, pl.ds(pl.multiple_of(g * per, per), per)]

    def hub_totals(layer):
        for r in range(1, ngraph):
            hub_copy(layer, r).wait_recv()
        total = hubrecv[layer, 0]
        for p in range(1, ngraph):
            total = total + hubrecv[layer, p]
        fill = jnp.zeros((DB - 3 * per, total.shape[1]), BF16)
        tot[layer] = jnp.concatenate([*bf16_parts(total), fill], axis=0)

    def with_hubs(layer, rb):
        rows = lax.broadcasted_iota(jnp.int32, (DB, DB), 0) + rb * DB
        sel = jnp.where(rows == myhub_ref[...], F32(1), F32(0)).astype(BF16)
        return acc[chunk(rb)] + jnp.dot(sel, tot[layer], preferred_element_type=F32)

    start_halo(tab1, 0)
    own_part(tab1, 0)
    wait_halo(tab1, 0)
    exchange_hubs(tab1, 0)
    def h_copy(i, r):
        return frdma(hsend.at[fpeer(r), chunk(i)], hin.at[f, chunk(i)], ns.at[i, r - 1], nr.at[i, r - 1], r)

    def z2_copy(i, r):
        return frdma(zout.at[fpeer(r), chunk(i)], tab2.at[pl.ds(pl.multiple_of(f * part + i * DB, DB), DB)], z2s.at[i, r - 1], z2r.at[i, r - 1], r)

    def z2_chunk(i):
        for r in range(1, nfeat):
            h_copy(i, r).wait_recv()
        acc = None
        for s in range(nfeat):
            term = jnp.dot(hin[s, chunk(i)], w2in[s], preferred_element_type=F32)
            acc = term if acc is None else acc + term
        acc = acc.astype(BF16)
        for q in range(nfeat):
            zout[q, chunk(i)] = acc[:, q * cols:(q + 1) * cols]
        for r in range(1, nfeat):
            z2_copy(i, r).start()
        tab2[pl.ds(pl.multiple_of(f * part + i * DB, DB), DB)] = zout[f, chunk(i)]

    bias1 = b1_ref[...]

    def far1(i):
        for r in range(1, nfeat + 1):
            rb = fpeer(r) * nchunk + i
            acc[chunk(rb)] = far_part(tab1, rb)

    def finish1(i):
        for r in range(1, nfeat + 1):
            q = fpeer(r)
            h = jnp.maximum(with_hubs(0, q * nchunk + i) + bias1, 0.0).astype(BF16)
            if r < nfeat:
                hsend[q, chunk(i)] = h
                h_copy(i, r).start()
            else:
                hin[f, chunk(i)] = h

    far1(0)
    hub_totals(0)
    for copy in w2_copies:
        copy.wait_recv()

    def rows1(i, carry):
        finish1(i - 1)
        far1(i)
        z2_chunk(i - 1)
        return carry

    lax.fori_loop(1, nchunk, rows1, 0)
    finish1(nchunk - 1)
    z2_chunk(nchunk - 1)
    for i in range(nchunk):
        for r in range(1, nfeat):
            z2_copy(i, r).wait_recv()

    start_halo(tab2, 1)
    own_part(tab2, 1)
    wait_halo(tab2, 1)
    exchange_hubs(tab2, 1)
    def far2(i):
        for u in range(4):
            acc[chunk(4 * i + u)] = far_part(tab2, 4 * i + u)

    def finish2(i):
        for u in range(4):
            o_ref[chunk(4 * i + u), :] = with_hubs(1, 4 * i + u)

    far2(0)
    hub_totals(1)

    def rows2(i, carry):
        far2(i)
        finish2(i - 1)
        return carry

    lax.fori_loop(1, nblock // 4, rows2, 0)
    finish2(nblock // 4 - 1)

    for copy in w2_copies:
        copy.wait_send()
    for i in range(nchunk):
        for r in range(1, nfeat):
            h_copy(i, r).wait_send()
            z2_copy(i, r).wait_send()
    for layer, tab in enumerate((tab1, tab2)):
        for r in range(1, ngraph):
            for copy in halo_copies(tab, layer, r):
                copy.wait_send()
            hub_copy(layer, r).wait_send()


def run_layers(nfeat, ngraph, nsend, per, tab_own, w2, idx, myhub, b1, inv, adj):
    vert = tab_own.shape[0]
    part, cols = vert // nfeat, b1.shape[1]
    nchunk, nblk = part // DB, adj.shape[0] // DB
    vm = lambda shape, dt: pltpu.VMEM(shape, dt)
    dma = lambda *shape: pltpu.SemaphoreType.DMA(shape)
    vspec = pl.BlockSpec(memory_space=pltpu.VMEM)
    fr, gr = nfeat - 1, ngraph - 1
    return pl.pallas_call(
        functools.partial(layers_kernel, (nfeat, ngraph, vert, nsend, per)),
        out_shape=jax.ShapeDtypeStruct((vert, cols), F32),
        in_specs=[vspec] * 6 + [pl.BlockSpec(memory_space=pl.ANY)],
        out_specs=vspec,
        scratch_shapes=[
            vm(adj.shape, F32), vm((adj.shape[0], cols), F32), vm((2, DB, cols), BF16), vm((nfeat, *w2.shape), BF16),
            vm((adj.shape[1], cols), BF16), vm((adj.shape[1], cols), BF16), vm((nfeat, part, cols), BF16), vm((nfeat, part, cols), BF16),
            vm((nfeat, part, cols), BF16), vm((2, ngraph, nsend + per, cols), BF16), vm((2, ngraph * per, cols), F32), vm((2, ngraph, per, cols), F32),
            dma(nblk), dma(fr), dma(fr), dma(nchunk, fr), dma(nchunk, fr),
            dma(2, gr), dma(2, gr), dma(2, gr), dma(2, gr), dma(2, gr), dma(2, gr), dma(nchunk, fr), dma(nchunk, fr),
        ],
        compiler_params=pltpu.CompilerParams(collective_id=1, has_side_effects=True, vmem_limit_bytes=62 * 2**20),
        name="layers",
    )(tab_own, w2, idx, myhub, b1, inv, adj)


def solution(mesh):
    rows_axes = ("data", "graph")
    nfeat = mesh.shape["feat"]
    ngraph = mesh.shape["graph"]

    def device_program(x_loc, dst_loc, src_loc, valid_loc, w_loc, send_loc, keep_loc, hub_ids, w_first, w_second, b_first, b_second):
        vert = x_loc.shape[0]
        nhub = hub_ids.shape[0]
        per = nhub // ngraph
        nsend = send_loc.shape[1]
        ndb = (vert + nhub) // DB
        table_rows = vert + ngraph * nsend + nhub
        nsb = -(-table_rows // SB)
        grid = lambda v: v.reshape(-1, 128)
        edges, starts, tab_own, inv, hub_col, myhub, idx = run_pre(
            nfeat, ngraph, ndb, nsb, grid(dst_loc), grid(src_loc), grid(valid_loc), grid(w_loc), x_loc, w_first, hub_ids[None, :], send_loc, keep_loc)
        adj = build_adjacency(starts, edges, hub_col, ndb, nsb, table_rows)
        return run_layers(nfeat, ngraph, nsend, per, tab_own, w_second, idx, myhub, b_first[None, :], inv, adj) + b_second

    edge_spec = P(rows_axes)
    send_spec = P(rows_axes, None)
    in_specs = (P(rows_axes, "feat"), edge_spec, edge_spec, edge_spec, edge_spec, send_spec, send_spec, P("data"), P("feat", None), P("feat", None), P("feat"), P("feat"))
    return jax.shard_map(device_program, mesh=mesh, in_specs=in_specs, out_specs=P(rows_axes, "feat"), check_vma=False)
```

```python
import functools

import jax
import jax.numpy as jnp
from jax import lax
from jax.experimental import pallas as pl
from jax.experimental.pallas import tpu as pltpu
from jax.sharding import PartitionSpec as P

DB, SB, KW = 128, 256, 256
MESH = pl.DeviceIdType.MESH
F32, BF16 = jnp.float32, jnp.bfloat16


def bf16_parts(x):
    hi = x.astype(BF16)
    rest = x - hi.astype(F32)
    mid = rest.astype(BF16)
    low = (rest - mid.astype(F32)).astype(BF16)
    return hi, mid, low


def build_kernel(ndb, nsb, ncol, starts_ref, edges_ref, hubcol_ref, a_ref):
    db = pl.program_id(0)
    dbase = (db * DB).astype(F32)
    hub_col = hubcol_ref[...]
    row_id = jnp.where(db == ndb - 1, hub_col, lax.broadcasted_iota(jnp.int32, (DB, 128), 0).astype(F32)).astype(BF16)
    iota_s = lax.broadcasted_iota(jnp.int32, (SB, 128), 0).astype(BF16)
    zero = jnp.zeros((), BF16)

    def window(sb, start, slots):
        width = min(SB, ncol - sb * SB)
        chunk = start // 128
        shift = start - chunk * 128
        raw = edges_ref[pl.ds(pl.multiple_of(chunk * 8, 8), 8 * (slots // 128 + 1)), :]
        raw = jnp.concatenate([raw[8 * i:8 * i + 8] for i in range(slots // 128 + 1)], axis=1)
        rows = pltpu.roll(raw, slots + 128 - shift, 1)[:, :slots]
        dst = (rows[0:1] - dbase).astype(BF16)
        src = (rows[1:2] - F32(SB * sb)).astype(BF16)
        tiled = lambda v: jnp.concatenate([v] * (slots // 128), axis=1)
        hit = tiled(row_id) == dst
        d3 = jnp.concatenate([jnp.where(hit, part, zero) for part in bf16_parts(rows[2:3])], axis=0)
        col_id = hub_col.astype(BF16) if sb == nsb - 1 else iota_s
        sel = jnp.where(tiled(col_id) == src, jnp.ones((), BF16), zero)
        out = lax.dot_general(d3, sel, (((1,), (1,)), ((), ())), preferred_element_type=F32)
        return out[:DB] + (out[DB:2 * DB] + out[2 * DB:]), slice(sb * SB, sb * SB + width)

    slots = [KW] * (nsb - 1) + [2 * KW]
    over = None
    for sb in range(nsb):
        start = starts_ref[0, db * nsb + sb]
        more = starts_ref[0, db * nsb + sb + 1] - start - slots[sb]
        over = more if over is None else jnp.maximum(over, more)
        block, where = window(sb, start, slots[sb])
        a_ref[:, where] = block

    @pl.when(over > 0)
    def _():
        for sb in range(nsb):
            start = starts_ref[0, db * nsb + sb] + slots[sb]
            end = starts_ref[0, db * nsb + sb + 1]

            def step(i, carry):
                block, where = window(sb, start + i * KW, KW)
                a_ref[:, where] += block
                return carry

            lax.fori_loop(0, (jnp.maximum(end - start, 0) + KW - 1) // KW, step, 0)


def build_adjacency(starts, edges, hub_col, ndb, nsb, ncol):
    return pl.pallas_call(
        functools.partial(build_kernel, ndb, nsb, ncol),
        out_shape=jax.ShapeDtypeStruct((ndb * DB, ncol), F32),
        grid_spec=pltpu.PrefetchScalarGridSpec(
            num_scalar_prefetch=1,
            grid=(ndb,),
            in_specs=[pl.BlockSpec(edges.shape, lambda i, s: (0, 0)), pl.BlockSpec(hub_col.shape, lambda i, s: (0, 0))],
            out_specs=pl.BlockSpec((DB, ncol), lambda i, s: (i, 0)),
        ),
        compiler_params=pltpu.CompilerParams(vmem_limit_bytes=20 * 2**20),
        name="build",
    )(starts, edges, hub_col)


def iota2(axis):
    return lax.broadcasted_iota(jnp.int32, (8, 128), axis)


def sort_levels(kref, wref, first, last):
    sub, lane = iota2(0), iota2(1)

    def bit(b):
        return ((sub >> (b - 6)) & 1) == 1 if b < 9 else ((lane >> (b - 9)) & 1) == 1

    def within(level):
        steps = []
        for j in range(level - 1, 5, -1):
            high = bit(j)
            if level < 16:
                want_max = high != bit(level)
            else:
                want_max = high
            steps.append((j, high, want_max))

        def body(it, carry):
            pairs = [(kref[it * 16 + u], wref[it * 16 + u]) for u in range(16)]
            for j, high, want_max in steps:
                axis, m, size = (0, 1 << (j - 6), 8) if j < 9 else (1, 1 << (j - 9), 128)
                new = []
                index = (lane if axis else sub) ^ m
                for key, w in pairs:
                    if 2 * m == size:
                        pk, pw = pltpu.roll(key, m, axis), pltpu.roll(w, m, axis)
                    else:
                        pk = jnp.take_along_axis(key, index, axis=axis)
                        pw = jnp.take_along_axis(w, index, axis=axis)
                    nk = jnp.where(want_max, jnp.maximum(key, pk), jnp.minimum(key, pk))
                    new.append((nk, jnp.where(nk == key, w, pw)))
                pairs = new
            for u, (key, w) in enumerate(pairs):
                kref[it * 16 + u] = key
                wref[it * 16 + u] = w
            return carry

        lax.fori_loop(0, 4, body, 0)

    def across(level, top, low):
        base = 3 if low >= 3 else 0

        def body(it, carry):
            where_v = [(it + 8 * u) if base == 3 else (it * 8 + u) for u in range(8)]
            ks, ws = [kref[v] for v in where_v], [wref[v] for v in where_v]
            for j in range(top, low - 1, -1):
                m = 1 << (j - base)
                for u in range(8):
                    if u & m:
                        continue
                    a, b = u, u | m
                    down = None
                    if level < 6 and base <= level < base + 3:
                        flip = bool(u >> (level - base) & 1)
                        swap = (ks[a] < ks[b]) if flip else (ks[a] > ks[b])
                    elif level < 6:
                        down = jnp.full((8, 128), (it >> (level - 3 + base)) & 1, jnp.int32) == 1
                        swap = (ks[a] > ks[b]) != down
                    elif level < 16:
                        swap = (ks[a] > ks[b]) != bit(level)
                    else:
                        swap = ks[a] > ks[b]
                    ks[a], ks[b] = jnp.where(swap, ks[b], ks[a]), jnp.where(swap, ks[a], ks[b])
                    ws[a], ws[b] = jnp.where(swap, ws[b], ws[a]), jnp.where(swap, ws[a], ws[b])
            for u, v in enumerate(where_v):
                kref[v] = ks[u]
                wref[v] = ws[u]
            return carry

        lax.fori_loop(0, 8, body, 0)

    for level in range(first, last + 1):
        if level > 6:
            within(level)
        if level > 3:
            across(level, min(level - 1, 5), 3)
        across(level, min(level - 1, 2), 0)


def pre_kernel(dims, dst_ref, src_ref, valid_ref, w_ref, x_ref, w1_ref, hub_ref, send_ref, keep_ref,
               edges_ref, starts_ref, tab_ref, inv_ref, hubcol_ref, myhub_ref, idx_ref,
               kref, wref, xin, w1in, tab, zout, xs, xr, w1s, w1r, zs, zr):
    nfeat, ngraph, ndb, nsb = dims
    vert = x_ref.shape[1]
    part = vert // nfeat
    f = lax.axis_index("feat")

    def fpeer(r):
        return lax.rem(f + r, nfeat)

    def frdma(src, dst, send, recv, r):
        return pltpu.make_async_remote_copy(src, dst, send, recv, device_id={"feat": fpeer(r)}, device_id_type=MESH)

    def quarter(q):
        return pl.ds(pl.multiple_of(q * part, part), part)

    barrier = pltpu.get_barrier_semaphore()
    for r in range(1, nfeat):
        pl.semaphore_signal(barrier, inc=1, device_id={"feat": fpeer(r)}, device_id_type=MESH)
    pl.semaphore_wait(barrier, nfeat - 1)
    peers = range(1, nfeat)
    x_copies = [frdma(x_ref.at[:, quarter(fpeer(r))], xin.at[f], xs.at[r - 1], xr.at[r - 1], r) for r in peers]
    w1_copies = [frdma(w1_ref, w1in.at[f], w1s.at[r - 1], w1r.at[r - 1], r) for r in peers]
    z_copies = [frdma(zout.at[fpeer(r)], tab.at[quarter(f)], zs.at[r - 1], zr.at[r - 1], r) for r in peers]
    for copy in w1_copies + x_copies:
        copy.start()
    xin[f] = x_ref[:, quarter(f)]
    w1in[f] = w1_ref[...]

    dst, src = dst_ref[...], src_ref[...]
    key = (((dst // DB) * nsb + src // SB) << 15) | ((dst % DB) << 8) | (src % SB)
    nbucket = ndb * nsb
    key = jnp.where(valid_ref[...] > 0, key, nbucket << 15).astype(F32)
    coef = w_ref[...] * valid_ref[...].astype(F32)
    large = jnp.max(coef, keepdims=True) > 1e30
    coef = coef * jnp.where(large, F32(2.0**-40), F32(1))
    inv_ref[...] = jnp.broadcast_to(jnp.where(large, F32(2.0**40), F32(1)), inv_ref.shape)
    used = dst.shape[0] // 8
    kref[:used] = key.reshape(used, 8, 128)
    wref[:used] = coef.reshape(used, 8, 128)
    kref[used:] = jnp.full((64 - used, 8, 128), nbucket << 15, F32)
    wref[used:] = jnp.zeros((64 - used, 8, 128), F32)
    sort_levels(kref, wref, 1, 13)

    g, per = lax.axis_index("graph"), DB // ngraph
    lane_id = lax.broadcasted_iota(jnp.int32, (DB, DB), 1).astype(F32)
    row_id = lax.broadcasted_iota(jnp.int32, (DB, DB), 0).astype(F32)
    down = lambda row: jnp.broadcast_to(row, (DB, DB)).T
    ids = hub_ref[...].astype(F32)
    owner = (hub_ref[...] // vert).astype(F32)
    owner_down = down(owner)
    earlier = (owner == owner_down) & (lane_id < row_id)
    pos_down = owner_down * per + jnp.sum(jnp.where(earlier, F32(1), F32(0)), axis=1, keepdims=True)
    pos = pos_down.T
    base = (g * per).astype(F32)
    first = (g * vert).astype(F32)
    hubcol_ref[...] = jnp.broadcast_to(jnp.sum(jnp.where(pos == row_id, lane_id, F32(0)), axis=1, keepdims=True), (DB, DB))
    lane_row = lax.broadcasted_iota(jnp.int32, (1, DB), 1)
    target = (lane_row % per).astype(F32) + base
    mine = jnp.sum(jnp.where(pos_down == target, down(ids), F32(0)), axis=0, keepdims=True) - first
    myhub_ref[...] = jnp.where(lane_row < 3 * per, mine, F32(-1)).astype(jnp.int32)
    mine_down = jnp.sum(jnp.where(pos == row_id + base, ids, F32(0)), axis=1, keepdims=True) - first
    mine_down = jnp.broadcast_to(mine_down, (DB, DB))[:per].astype(jnp.int32)
    rows = jnp.where(keep_ref[...] > 0, send_ref[...], -1).astype(F32)
    nsend = rows.shape[1]
    for p in range(ngraph):
        for h in range(nsend // DB):
            idx_ref[p, h * DB:(h + 1) * DB] = down(rows[p:p + 1, h * DB:(h + 1) * DB]).astype(jnp.int32)
        idx_ref[p, nsend:] = mine_down

    for copy in w1_copies + x_copies:
        copy.wait_recv()
    cols = tab.shape[1]
    z = None
    for s in range(nfeat):
        term = lax.dot_general(xin[s], w1in[s], (((0,), (0,)), ((), ())), preferred_element_type=F32)
        z = term if z is None else z + term
    z = z.astype(BF16)
    for q in range(nfeat):
        zout[q] = z[:, q * cols:(q + 1) * cols]
    for copy in z_copies:
        copy.start()
    tab[quarter(f)] = zout[f]
    sort_levels(kref, wref, 14, 16)

    nb = starts_ref.shape[1]
    bound = (lax.broadcasted_iota(jnp.int32, (nb, 1), 0) << 15).astype(F32)
    last = kref[63, 7:8, :]
    lane = lax.broadcasted_iota(jnp.int32, (1, 128), 1)
    before = jnp.where(lane == 0, F32(-1), pltpu.roll(last, 1, 1))
    full = last < bound
    row_sel = jnp.where((before < bound) & jnp.logical_not(full), F32(1), F32(0)).astype(BF16)
    keys = kref[...].reshape(512, 128)
    picked = None
    for piece in bf16_parts(keys):
        term = lax.dot_general(row_sel, piece, (((1,), (1,)), ((), ())), preferred_element_type=F32)
        picked = term if picked is None else picked + term
    inside = jnp.where(picked < bound, F32(1), F32(0)).astype(BF16)
    count = lax.dot_general(jnp.ones((8, 512), BF16), inside, (((1,), (1,)), ((), ())), preferred_element_type=F32)
    rows = lax.dot_general(jnp.ones((8, 128), BF16), jnp.where(full, F32(1), F32(0)).astype(BF16), (((1,), (1,)), ((), ())), preferred_element_type=F32)
    starts_ref[...] = (count + 512.0 * rows).astype(jnp.int32)

    nl = edges_ref.shape[0] // 32
    for k in range(4):
        kk = jnp.concatenate([kref[:, 2 * k, :], kref[:, 2 * k + 1, :]], axis=0)
        ww = jnp.concatenate([wref[:, 2 * k, :], wref[:, 2 * k + 1, :]], axis=0)
        ki = kk.astype(jnp.int32)
        bucket = ki >> 15
        block = jnp.floor((bucket.astype(F32) + 0.5) * F32(1.0 / nsb))
        edge_dst = block * DB + ((ki >> 8) & (DB - 1)).astype(F32)
        edge_src = (bucket.astype(F32) - block * nsb) * SB + (ki & (SB - 1)).astype(F32)
        for field, val in enumerate((edge_dst, edge_src, ww)):
            edges_ref[pl.ds(k * 8 + field, nl, stride=32), :] = val.T[:nl]

    for copy in z_copies:
        copy.wait_recv()
    tab_ref[...] = tab[...]
    for copy in x_copies + w1_copies + z_copies:
        copy.wait_send()


def run_pre(nfeat, ngraph, ndb, nsb, dst, src, valid, w, x, w1, hubs, send, keep):
    vert, part = x.shape[1], x.shape[1] // nfeat
    cols = w1.shape[1] // nfeat
    nrows = dst.shape[0]
    vm = lambda shape, dt: pltpu.VMEM(shape, dt)
    dma = pltpu.SemaphoreType.DMA((nfeat - 1,))
    vspec = pl.BlockSpec(memory_space=pltpu.VMEM)
    shape = jax.ShapeDtypeStruct
    return pl.pallas_call(
        functools.partial(pre_kernel, (nfeat, ngraph, ndb, nsb)),
        out_shape=[shape(((nrows + 8) * 8, 128), F32), shape((8, 384), jnp.int32), shape((vert, cols), BF16), shape((1, cols), F32),
                   shape((DB, DB), F32), shape((1, DB), jnp.int32), shape((ngraph, send.shape[1] + DB // ngraph, DB), jnp.int32)],
        in_specs=[vspec] * 9,
        out_specs=[vspec] * 7,
        scratch_shapes=[
            vm((64, 8, 128), F32), vm((64, 8, 128), F32), vm((nfeat, x.shape[0], part), BF16), vm((nfeat, *w1.shape), BF16),
            vm((vert, cols), BF16), vm((nfeat, part, cols), BF16), dma, dma, dma, dma, dma, dma,
        ],
        compiler_params=pltpu.CompilerParams(collective_id=0, has_side_effects=True, vmem_limit_bytes=62 * 2**20),
        name="pre",
    )(dst, src, valid, w, x, w1, hubs, send, keep)


def layers_kernel(dims, tabown_ref, w2_ref, idx_ref, myhub_ref, b1_ref, inv_ref, a_hbm, o_ref,
                  a_v, acc, tot, w2in, tab1, tab2, zout, hsend, hin, halo, hubsend, hubrecv,
                  a_sem, w2s, w2r, z2s, z2r, hs, hr, ps, pr, us, ur, ns, nr):
    nfeat, ngraph, vert, nsend, per = dims
    part, rows_send = vert // nfeat, nsend + per
    nchunk = part // DB
    f, g = lax.axis_index("feat"), lax.axis_index("graph")
    halo_base, hub_base = vert, vert + ngraph * nsend
    nblock = vert // DB

    def fpeer(r):
        return lax.rem(f + r, nfeat)

    def gpeer(r):
        return lax.rem(g + r, ngraph)

    def frdma(src, dst, send, recv, r):
        return pltpu.make_async_remote_copy(src, dst, send, recv, device_id={"feat": fpeer(r)}, device_id_type=MESH)

    def grdma(src, dst, send, recv, r):
        return pltpu.make_async_remote_copy(src, dst, send, recv, device_id={"graph": gpeer(r)}, device_id_type=MESH)

    for i in [nblock] + [q * nchunk + c for c in range(nchunk) for q in range(nfeat)]:
        pltpu.make_async_copy(a_hbm.at[pl.ds(i * DB, DB)], a_v.at[pl.ds(i * DB, DB)], a_sem.at[i]).start()

    barrier = pltpu.get_barrier_semaphore()
    for r in range(1, nfeat):
        pl.semaphore_signal(barrier, inc=1, device_id={"feat": fpeer(r)}, device_id_type=MESH)
    for r in range(1, ngraph):
        pl.semaphore_signal(barrier, inc=1, device_id={"graph": gpeer(r)}, device_id_type=MESH)
    pl.semaphore_wait(barrier, nfeat + ngraph - 2)

    w2_copies = [frdma(w2_ref, w2in.at[f], w2s.at[r - 1], w2r.at[r - 1], r) for r in range(1, nfeat)]
    for copy in w2_copies:
        copy.start()
    w2in[f] = w2_ref[...]
    for tab in (tab1, tab2):
        tab[pl.ds(pl.multiple_of(halo_base + g * nsend, nsend), nsend)] = jnp.zeros((nsend, tab.shape[1]), BF16)

    cols = tab1.shape[1]
    tab1[:vert] = tabown_ref[...]

    lane = lax.broadcasted_iota(jnp.int32, (1, DB), 1)

    def select_rows(tab, idx):
        pieces = [jnp.where(idx == lane + DB * j, F32(1), F32(0)).astype(BF16) for j in range(vert // DB)]
        return jnp.dot(jnp.concatenate(pieces, axis=1), tab[:vert], preferred_element_type=F32).astype(BF16)

    def halo_copies(tab, layer, r):
        p = gpeer(r)
        return (
            grdma(halo.at[layer, p, pl.ds(0, nsend)], tab.at[pl.ds(pl.multiple_of(halo_base + g * nsend, nsend), nsend)],
                  hs.at[layer, r - 1], hr.at[layer, r - 1], r),
            grdma(halo.at[layer, p, pl.ds(nsend, per)], tab.at[pl.ds(pl.multiple_of(hub_base + g * per, per), per)],
                  ps.at[layer, r - 1], pr.at[layer, r - 1], r),
        )

    def start_halo(tab, layer):
        def one(r, carry):
            p = gpeer(r)
            halo[layer, p] = select_rows(tab, idx_ref[p])
            for copy in halo_copies(tab, layer, r):
                copy.start()
            return carry

        lax.fori_loop(1, ngraph, one, 0)
        tab[pl.ds(pl.multiple_of(hub_base + g * per, per), per)] = select_rows(tab, idx_ref[g, nsend:])

    def wait_halo(tab, layer):
        def arrive(r, carry):
            for copy in halo_copies(tab, layer, r):
                copy.wait_recv()
            return carry

        lax.fori_loop(1, ngraph, arrive, 0)

    inv = inv_ref[...]

    def chunk(i):
        return pl.ds(pl.multiple_of(i * DB, DB), DB)

    def product(a, tab):
        out = jnp.dot(jnp.concatenate(bf16_parts(a), axis=0), tab, preferred_element_type=F32)
        return out[:DB] + (out[DB:2 * DB] + out[2 * DB:])

    def a_copy(rb):
        return pltpu.make_async_copy(a_hbm.at[chunk(rb)], a_v.at[chunk(rb)], a_sem.at[rb])

    def own_blocks(tab, layer, blocks):
        if layer == 0:
            for rb in blocks:
                a_copy(rb).wait()
        for rb in blocks:
            acc[chunk(rb)] = product(a_v[chunk(rb), :vert], tab[:vert])

    def own_chunks(tab, layer, count):
        def one(i, carry):
            own_blocks(tab, layer, [q * nchunk + i for q in range(nfeat)])
            return carry

        lax.fori_loop(0, count, one, 0)

    def far_part(tab, rb):
        return (acc[chunk(rb)] + product(a_v[chunk(rb), vert:], tab[vert:])) * inv

    def hub_copy(layer, r):
        p = gpeer(r)
        return grdma(hubsend.at[layer, pl.ds(pl.multiple_of(p * per, per), per)], hubrecv.at[layer, g], us.at[layer, r - 1], ur.at[layer, r - 1], r)

    def exchange_hubs(tab, layer):
        hubsend[layer] = far_part(tab, nblock)
        for r in range(1, ngraph):
            hub_copy(layer, r).start()
        hubrecv[layer, g] = hubsend[layer, pl.ds(pl.multiple_of(g * per, per), per)]

    def hub_totals(layer):
        for r in range(1, ngraph):
            hub_copy(layer, r).wait_recv()
        total = hubrecv[layer, 0]
        for p in range(1, ngraph):
            total = total + hubrecv[layer, p]
        fill = jnp.zeros((DB - 3 * per, total.shape[1]), BF16)
        tot[layer] = jnp.concatenate([*bf16_parts(total), fill], axis=0)

    def with_hubs(layer, rb):
        rows = lax.broadcasted_iota(jnp.int32, (DB, DB), 0) + rb * DB
        sel = jnp.where(rows == myhub_ref[...], F32(1), F32(0)).astype(BF16)
        return acc[chunk(rb)] + jnp.dot(sel, tot[layer], preferred_element_type=F32)

    start_halo(tab1, 0)
    own_blocks(tab1, 0, [nblock])
    own_chunks(tab1, 0, nchunk - 1)
    wait_halo(tab1, 0)
    exchange_hubs(tab1, 0)
    def h_copy(i, r):
        return frdma(hsend.at[fpeer(r), chunk(i)], hin.at[f, chunk(i)], ns.at[i, r - 1], nr.at[i, r - 1], r)

    def z2_copy(i, r):
        return frdma(zout.at[fpeer(r), chunk(i)], tab2.at[pl.ds(pl.multiple_of(f * part + i * DB, DB), DB)], z2s.at[i, r - 1], z2r.at[i, r - 1], r)

    def z2_chunk(i):
        for r in range(1, nfeat):
            h_copy(i, r).wait_recv()
        acc = None
        for s in range(nfeat):
            term = jnp.dot(hin[s, chunk(i)], w2in[s], preferred_element_type=F32)
            acc = term if acc is None else acc + term
        acc = acc.astype(BF16)
        for q in range(nfeat):
            zout[q, chunk(i)] = acc[:, q * cols:(q + 1) * cols]
        for r in range(1, nfeat):
            z2_copy(i, r).start()
        tab2[pl.ds(pl.multiple_of(f * part + i * DB, DB), DB)] = zout[f, chunk(i)]

    bias1 = b1_ref[...]

    def far1(i):
        for r in range(1, nfeat + 1):
            rb = fpeer(r) * nchunk + i
            acc[chunk(rb)] = far_part(tab1, rb)

    def finish1(i):
        for r in range(1, nfeat + 1):
            q = fpeer(r)
            h = jnp.maximum(with_hubs(0, q * nchunk + i) + bias1, 0.0).astype(BF16)
            if r < nfeat:
                hsend[q, chunk(i)] = h
                h_copy(i, r).start()
            else:
                hin[f, chunk(i)] = h

    far1(0)
    hub_totals(0)
    for copy in w2_copies:
        copy.wait_recv()

    finish1(0)
    own_blocks(tab1, 0, [q * nchunk + nchunk - 1 for q in range(nfeat)])
    far1(1)

    def rows1(i, carry):
        finish1(i - 1)
        z2_chunk(i - 2)
        far1(i)
        return carry

    lax.fori_loop(2, nchunk, rows1, 0)
    finish1(nchunk - 1)
    z2_chunk(nchunk - 2)
    z2_chunk(nchunk - 1)
    for i in range(nchunk):
        for r in range(1, nfeat):
            z2_copy(i, r).wait_recv()

    start_halo(tab2, 1)
    own_blocks(tab2, 1, [nblock])
    own_chunks(tab2, 1, nchunk)
    wait_halo(tab2, 1)
    exchange_hubs(tab2, 1)
    def far2(i):
        for u in range(4):
            acc[chunk(4 * i + u)] = far_part(tab2, 4 * i + u)

    def finish2(i):
        for u in range(4):
            o_ref[chunk(4 * i + u), :] = with_hubs(1, 4 * i + u)

    lag = nblock // 4 - 1

    def far2_only(i, carry):
        far2(i)
        return carry

    lax.fori_loop(0, lag, far2_only, 0)
    hub_totals(1)
    far2(lag)
    for i in range(lag + 1):
        finish2(i)

    for copy in w2_copies:
        copy.wait_send()
    for i in range(nchunk):
        for r in range(1, nfeat):
            h_copy(i, r).wait_send()
            z2_copy(i, r).wait_send()
    for layer, tab in enumerate((tab1, tab2)):
        for r in range(1, ngraph):
            for copy in halo_copies(tab, layer, r):
                copy.wait_send()
            hub_copy(layer, r).wait_send()


def run_layers(nfeat, ngraph, nsend, per, tab_own, w2, idx, myhub, b1, inv, adj):
    vert = tab_own.shape[0]
    part, cols = vert // nfeat, b1.shape[1]
    nchunk, nblk = part // DB, adj.shape[0] // DB
    vm = lambda shape, dt: pltpu.VMEM(shape, dt)
    dma = lambda *shape: pltpu.SemaphoreType.DMA(shape)
    vspec = pl.BlockSpec(memory_space=pltpu.VMEM)
    fr, gr = nfeat - 1, ngraph - 1
    return pl.pallas_call(
        functools.partial(layers_kernel, (nfeat, ngraph, vert, nsend, per)),
        out_shape=jax.ShapeDtypeStruct((vert, cols), F32),
        in_specs=[vspec] * 6 + [pl.BlockSpec(memory_space=pl.ANY)],
        out_specs=vspec,
        scratch_shapes=[
            vm(adj.shape, F32), vm((adj.shape[0], cols), F32), vm((2, DB, cols), BF16), vm((nfeat, *w2.shape), BF16),
            vm((adj.shape[1], cols), BF16), vm((adj.shape[1], cols), BF16), vm((nfeat, part, cols), BF16), vm((nfeat, part, cols), BF16),
            vm((nfeat, part, cols), BF16), vm((2, ngraph, nsend + per, cols), BF16), vm((2, ngraph * per, cols), F32), vm((2, ngraph, per, cols), F32),
            dma(nblk), dma(fr), dma(fr), dma(nchunk, fr), dma(nchunk, fr),
            dma(2, gr), dma(2, gr), dma(2, gr), dma(2, gr), dma(2, gr), dma(2, gr), dma(nchunk, fr), dma(nchunk, fr),
        ],
        compiler_params=pltpu.CompilerParams(collective_id=1, has_side_effects=True, vmem_limit_bytes=52 * 2**20),
        name="layers",
    )(tab_own, w2, idx, myhub, b1, inv, adj)


def solution(mesh):
    rows_axes = ("data", "graph")
    nfeat = mesh.shape["feat"]
    ngraph = mesh.shape["graph"]

    def device_program(x_loc, dst_loc, src_loc, valid_loc, w_loc, send_loc, keep_loc, hub_ids, w_first, w_second, b_first, b_second):
        vert = x_loc.shape[0]
        nhub = hub_ids.shape[0]
        per = nhub // ngraph
        nsend = send_loc.shape[1]
        ndb = (vert + nhub) // DB
        table_rows = vert + ngraph * nsend + nhub
        nsb = -(-table_rows // SB)
        grid = lambda v: v.reshape(-1, 128)
        edges, starts, tab_own, inv, hub_col, myhub, idx = run_pre(
            nfeat, ngraph, ndb, nsb, grid(dst_loc), grid(src_loc), grid(valid_loc), grid(w_loc), x_loc.T, w_first, hub_ids[None, :], send_loc, keep_loc)
        adj = build_adjacency(starts, edges, hub_col, ndb, nsb, table_rows)
        return run_layers(nfeat, ngraph, nsend, per, tab_own, w_second, idx, myhub, b_first[None, :], inv, adj) + b_second

    edge_spec = P(rows_axes)
    send_spec = P(rows_axes, None)
    in_specs = (P(rows_axes, "feat"), edge_spec, edge_spec, edge_spec, edge_spec, send_spec, send_spec, P("data"), P("feat", None), P("feat", None), P("feat"), P("feat"))
    return jax.shard_map(device_program, mesh=mesh, in_specs=in_specs, out_specs=P(rows_axes, "feat"), check_vma=False)
```

```python
import functools

import jax
import jax.numpy as jnp
from jax import lax
from jax.experimental import pallas as pl
from jax.experimental.pallas import tpu as pltpu
from jax.sharding import PartitionSpec as P

DB, SB, KW = 128, 256, 256
MESH = pl.DeviceIdType.MESH
F32, BF16 = jnp.float32, jnp.bfloat16


def bf16_parts(x):
    hi = x.astype(BF16)
    rest = x - hi.astype(F32)
    mid = rest.astype(BF16)
    low = (rest - mid.astype(F32)).astype(BF16)
    return hi, mid, low


def build_kernel(ndb, nsb, ncol, starts_ref, edges_ref, hubcol_ref, a_ref):
    db = pl.program_id(0)
    dbase = (db * DB).astype(F32)
    hub_col = hubcol_ref[...]
    row_id = jnp.where(db == ndb - 1, hub_col, lax.broadcasted_iota(jnp.int32, (DB, 128), 0).astype(F32)).astype(BF16)
    iota_s = lax.broadcasted_iota(jnp.int32, (SB, 128), 0).astype(BF16)
    zero = jnp.zeros((), BF16)

    def window(sb, start, slots):
        width = min(SB, ncol - sb * SB)
        chunk = start // 128
        shift = start - chunk * 128
        raw = edges_ref[pl.ds(pl.multiple_of(chunk * 8, 8), 8 * (slots // 128 + 1)), :]
        raw = jnp.concatenate([raw[8 * i:8 * i + 8] for i in range(slots // 128 + 1)], axis=1)
        rows = pltpu.roll(raw, slots + 128 - shift, 1)[:, :slots]
        dst = (rows[0:1] - dbase).astype(BF16)
        src = (rows[1:2] - F32(SB * sb)).astype(BF16)
        tiled = lambda v: jnp.concatenate([v] * (slots // 128), axis=1)
        hit = tiled(row_id) == dst
        d3 = jnp.concatenate([jnp.where(hit, part, zero) for part in bf16_parts(rows[2:3])], axis=0)
        col_id = hub_col.astype(BF16) if sb == nsb - 1 else iota_s
        sel = jnp.where(tiled(col_id) == src, jnp.ones((), BF16), zero)
        out = lax.dot_general(d3, sel, (((1,), (1,)), ((), ())), preferred_element_type=F32)
        return out[:DB] + (out[DB:2 * DB] + out[2 * DB:]), slice(sb * SB, sb * SB + width)

    slots = [KW] * (nsb - 1) + [2 * KW]
    over = None
    for sb in range(nsb):
        start = starts_ref[0, db * nsb + sb]
        more = starts_ref[0, db * nsb + sb + 1] - start - slots[sb]
        over = more if over is None else jnp.maximum(over, more)
        block, where = window(sb, start, slots[sb])
        a_ref[:, where] = block

    @pl.when(over > 0)
    def _():
        for sb in range(nsb):
            start = starts_ref[0, db * nsb + sb] + slots[sb]
            end = starts_ref[0, db * nsb + sb + 1]

            def step(i, carry):
                block, where = window(sb, start + i * KW, KW)
                a_ref[:, where] += block
                return carry

            lax.fori_loop(0, (jnp.maximum(end - start, 0) + KW - 1) // KW, step, 0)


def build_adjacency(starts, edges, hub_col, ndb, nsb, ncol):
    return pl.pallas_call(
        functools.partial(build_kernel, ndb, nsb, ncol),
        out_shape=jax.ShapeDtypeStruct((ndb * DB, ncol), F32),
        grid_spec=pltpu.PrefetchScalarGridSpec(
            num_scalar_prefetch=1,
            grid=(ndb,),
            in_specs=[pl.BlockSpec(edges.shape, lambda i, s: (0, 0)), pl.BlockSpec(hub_col.shape, lambda i, s: (0, 0))],
            out_specs=pl.BlockSpec((DB, ncol), lambda i, s: (i, 0)),
        ),
        compiler_params=pltpu.CompilerParams(vmem_limit_bytes=62 * 2**20),
        name="build",
    )(starts, edges, hub_col)


def iota2(axis):
    return lax.broadcasted_iota(jnp.int32, (8, 128), axis)


def sort_levels(kref, wref, first, last):
    sub, lane = iota2(0), iota2(1)

    def bit(b):
        return ((sub >> (b - 6)) & 1) == 1 if b < 9 else ((lane >> (b - 9)) & 1) == 1

    def within(level):
        steps = []
        for j in range(level - 1, 5, -1):
            high = bit(j)
            if level < 16:
                want_max = high != bit(level)
            else:
                want_max = high
            steps.append((j, high, want_max))

        def body(it, carry):
            pairs = [(kref[it * 16 + u], wref[it * 16 + u]) for u in range(16)]
            for j, high, want_max in steps:
                axis, m, size = (0, 1 << (j - 6), 8) if j < 9 else (1, 1 << (j - 9), 128)
                new = []
                index = (lane if axis else sub) ^ m
                for key, w in pairs:
                    if 2 * m == size:
                        pk, pw = pltpu.roll(key, m, axis), pltpu.roll(w, m, axis)
                    else:
                        pk = jnp.take_along_axis(key, index, axis=axis)
                        pw = jnp.take_along_axis(w, index, axis=axis)
                    nk = jnp.where(want_max, jnp.maximum(key, pk), jnp.minimum(key, pk))
                    new.append((nk, jnp.where(nk == key, w, pw)))
                pairs = new
            for u, (key, w) in enumerate(pairs):
                kref[it * 16 + u] = key
                wref[it * 16 + u] = w
            return carry

        lax.fori_loop(0, 4, body, 0)

    def across(level, top, low):
        base = 3 if low >= 3 else 0

        def body(it, carry):
            where_v = [(it + 8 * u) if base == 3 else (it * 8 + u) for u in range(8)]
            ks, ws = [kref[v] for v in where_v], [wref[v] for v in where_v]
            for j in range(top, low - 1, -1):
                m = 1 << (j - base)
                for u in range(8):
                    if u & m:
                        continue
                    a, b = u, u | m
                    down = None
                    if level < 6 and base <= level < base + 3:
                        flip = bool(u >> (level - base) & 1)
                        swap = (ks[a] < ks[b]) if flip else (ks[a] > ks[b])
                    elif level < 6:
                        down = jnp.full((8, 128), (it >> (level - 3 + base)) & 1, jnp.int32) == 1
                        swap = (ks[a] > ks[b]) != down
                    elif level < 16:
                        swap = (ks[a] > ks[b]) != bit(level)
                    else:
                        swap = ks[a] > ks[b]
                    ks[a], ks[b] = jnp.where(swap, ks[b], ks[a]), jnp.where(swap, ks[a], ks[b])
                    ws[a], ws[b] = jnp.where(swap, ws[b], ws[a]), jnp.where(swap, ws[a], ws[b])
            for u, v in enumerate(where_v):
                kref[v] = ks[u]
                wref[v] = ws[u]
            return carry

        lax.fori_loop(0, 8, body, 0)

    for level in range(first, last + 1):
        if level > 6:
            within(level)
        if level > 3:
            across(level, min(level - 1, 5), 3)
        across(level, min(level - 1, 2), 0)


def pre_kernel(dims, dst_ref, src_ref, valid_ref, w_ref, x_ref, w1_ref, hub_ref, send_ref, keep_ref,
               edges_ref, starts_ref, tab_ref, inv_ref, hubcol_ref, myhub_ref, high_ref, low_ref,
               kref, wref, xin, w1in, tab, zout, xs, xr, w1s, w1r, zs, zr):
    nfeat, ngraph, ndb, nsb = dims
    vert = x_ref.shape[1]
    part = vert // nfeat
    f = lax.axis_index("feat")

    def fpeer(r):
        return lax.rem(f + r, nfeat)

    def frdma(src, dst, send, recv, r):
        return pltpu.make_async_remote_copy(src, dst, send, recv, device_id={"feat": fpeer(r)}, device_id_type=MESH)

    def quarter(q):
        return pl.ds(pl.multiple_of(q * part, part), part)

    barrier = pltpu.get_barrier_semaphore()
    for r in range(1, nfeat):
        pl.semaphore_signal(barrier, inc=1, device_id={"feat": fpeer(r)}, device_id_type=MESH)
    dst, src = dst_ref[...], src_ref[...]
    key = (((dst // DB) * nsb + src // SB) << 15) | ((dst % DB) << 8) | (src % SB)
    nbucket = ndb * nsb
    key = jnp.where(valid_ref[...] > 0, key, nbucket << 15).astype(F32)
    coef = w_ref[...] * valid_ref[...].astype(F32)
    large = jnp.max(coef, keepdims=True) > 1e30
    coef = coef * jnp.where(large, F32(2.0**-40), F32(1))
    inv_ref[...] = jnp.broadcast_to(jnp.where(large, F32(2.0**40), F32(1)), inv_ref.shape)
    used = dst.shape[0] // 8
    kref[:used] = key.reshape(used, 8, 128)
    wref[:used] = coef.reshape(used, 8, 128)
    kref[used:] = jnp.full((64 - used, 8, 128), nbucket << 15, F32)
    wref[used:] = jnp.zeros((64 - used, 8, 128), F32)
    pl.semaphore_wait(barrier, nfeat - 1)
    peers = range(1, nfeat)
    x_copies = [frdma(x_ref.at[:, quarter(fpeer(r))], xin.at[f], xs.at[r - 1], xr.at[r - 1], r) for r in peers]
    w1_copies = [frdma(w1_ref, w1in.at[f], w1s.at[r - 1], w1r.at[r - 1], r) for r in peers]
    z_copies = [frdma(zout.at[fpeer(r)], tab.at[quarter(f)], zs.at[r - 1], zr.at[r - 1], r) for r in peers]
    for copy in w1_copies + x_copies:
        copy.start()
    xin[f] = x_ref[:, quarter(f)]
    w1in[f] = w1_ref[...]

    sort_levels(kref, wref, 1, 13)

    g, per = lax.axis_index("graph"), DB // ngraph
    lane_id = lax.broadcasted_iota(jnp.int32, (DB, DB), 1).astype(F32)
    row_id = lax.broadcasted_iota(jnp.int32, (DB, DB), 0).astype(F32)
    down = lambda row: jnp.broadcast_to(row, (DB, DB)).T
    ids = hub_ref[...].astype(F32)
    owner = (hub_ref[...] // vert).astype(F32)
    owner_down = down(owner)
    earlier = (owner == owner_down) & (lane_id < row_id)
    pos_down = owner_down * per + jnp.sum(jnp.where(earlier, F32(1), F32(0)), axis=1, keepdims=True)
    pos = pos_down.T
    base = (g * per).astype(F32)
    first = (g * vert).astype(F32)
    hubcol_ref[...] = jnp.broadcast_to(jnp.sum(jnp.where(pos == row_id, lane_id, F32(0)), axis=1, keepdims=True), (DB, DB))
    lane_row = lax.broadcasted_iota(jnp.int32, (1, DB), 1)
    target = (lane_row % per).astype(F32) + base
    mine = jnp.sum(jnp.where(pos_down == target, down(ids), F32(0)), axis=0, keepdims=True) - first
    myhub_ref[...] = jnp.where(lane_row < 3 * per, mine, F32(-1)).astype(jnp.int32)
    mine_down = jnp.sum(jnp.where(pos == row_id + base, ids, F32(0)), axis=1, keepdims=True) - first
    mine_down = jnp.broadcast_to(mine_down, (DB, DB))[:per]
    rows = jnp.where(keep_ref[...] > 0, send_ref[...], -1).astype(F32)
    nsend = rows.shape[1]

    def put_index(p, where, val):
        high = jnp.floor(val * F32(1.0 / DB))
        high_ref[p, where] = high.astype(BF16)
        low_ref[p, where] = (val - high * DB).astype(BF16)

    for p in range(ngraph):
        for h in range(nsend // DB):
            put_index(p, slice(h * DB, (h + 1) * DB), down(rows[p:p + 1, h * DB:(h + 1) * DB]))
        put_index(p, slice(nsend, nsend + per), mine_down)

    for copy in w1_copies + x_copies:
        copy.wait_recv()
    cols = tab.shape[1]
    z = None
    for s in range(nfeat):
        term = lax.dot_general(xin[s], w1in[s], (((0,), (0,)), ((), ())), preferred_element_type=F32)
        z = term if z is None else z + term
    z = z.astype(BF16)
    for q in range(nfeat):
        zout[q] = z[:, q * cols:(q + 1) * cols]
    for copy in z_copies:
        copy.start()
    tab[quarter(f)] = zout[f]
    sort_levels(kref, wref, 14, 16)

    nb = starts_ref.shape[1]
    bound = (lax.broadcasted_iota(jnp.int32, (nb, 1), 0) << 15).astype(F32)
    last = kref[63, 7:8, :]
    lane = lax.broadcasted_iota(jnp.int32, (1, 128), 1)
    before = jnp.where(lane == 0, F32(-1), pltpu.roll(last, 1, 1))
    full = last < bound
    row_sel = jnp.where((before < bound) & jnp.logical_not(full), F32(1), F32(0)).astype(BF16)
    keys = kref[...].reshape(512, 128)
    picked = None
    for piece in bf16_parts(keys):
        term = lax.dot_general(row_sel, piece, (((1,), (1,)), ((), ())), preferred_element_type=F32)
        picked = term if picked is None else picked + term
    inside = jnp.where(picked < bound, F32(1), F32(0)).astype(BF16)
    count = lax.dot_general(jnp.ones((8, 512), BF16), inside, (((1,), (1,)), ((), ())), preferred_element_type=F32)
    rows = lax.dot_general(jnp.ones((8, 128), BF16), jnp.where(full, F32(1), F32(0)).astype(BF16), (((1,), (1,)), ((), ())), preferred_element_type=F32)
    starts_ref[...] = (count + 512.0 * rows).astype(jnp.int32)

    nl = edges_ref.shape[0] // 32
    for k in range(4):
        kk = jnp.concatenate([kref[:, 2 * k, :], kref[:, 2 * k + 1, :]], axis=0)
        ww = jnp.concatenate([wref[:, 2 * k, :], wref[:, 2 * k + 1, :]], axis=0)
        ki = kk.astype(jnp.int32)
        bucket = ki >> 15
        block = jnp.floor((bucket.astype(F32) + 0.5) * F32(1.0 / nsb))
        edge_dst = block * DB + ((ki >> 8) & (DB - 1)).astype(F32)
        edge_src = (bucket.astype(F32) - block * nsb) * SB + (ki & (SB - 1)).astype(F32)
        for field, val in enumerate((edge_dst, edge_src, ww)):
            edges_ref[pl.ds(k * 8 + field, nl, stride=32), :] = val.T[:nl]

    for copy in z_copies:
        copy.wait_recv()
    tab_ref[...] = tab[...]
    for copy in x_copies + w1_copies + z_copies:
        copy.wait_send()


def run_pre(nfeat, ngraph, ndb, nsb, dst, src, valid, w, x, w1, hubs, send, keep):
    vert, part = x.shape[1], x.shape[1] // nfeat
    cols = w1.shape[1] // nfeat
    nrows = dst.shape[0]
    vm = lambda shape, dt: pltpu.VMEM(shape, dt)
    dma = pltpu.SemaphoreType.DMA((nfeat - 1,))
    vspec = pl.BlockSpec(memory_space=pltpu.VMEM)
    shape = jax.ShapeDtypeStruct
    return pl.pallas_call(
        functools.partial(pre_kernel, (nfeat, ngraph, ndb, nsb)),
        out_shape=[shape(((nrows + 8) * 8, 128), F32), shape((8, 384), jnp.int32), shape((vert, cols), BF16), shape((1, cols), F32),
                   shape((DB, DB), F32), shape((1, DB), jnp.int32), *[shape((ngraph, send.shape[1] + DB // ngraph, DB), BF16)] * 2],
        in_specs=[vspec] * 9,
        out_specs=[vspec] * 8,
        scratch_shapes=[
            vm((64, 8, 128), F32), vm((64, 8, 128), F32), vm((nfeat, x.shape[0], part), BF16), vm((nfeat, *w1.shape), BF16),
            vm((vert, cols), BF16), vm((nfeat, part, cols), BF16), dma, dma, dma, dma, dma, dma,
        ],
        compiler_params=pltpu.CompilerParams(collective_id=0, has_side_effects=True, vmem_limit_bytes=62 * 2**20),
        name="pre",
    )(dst, src, valid, w, x, w1, hubs, send, keep)


def layers_kernel(dims, tabown_ref, w2_ref, high_ref, low_ref, myhub_ref, b1_ref, inv_ref, a_hbm, o_ref,
                  a_v, acc, tot, w2in, tab1, tab2, zout, hsend, hin, halo, hubsend, hubrecv,
                  a_sem, w2s, w2r, z2s, z2r, hs, hr, ps, pr, us, ur, ns, nr):
    nfeat, ngraph, vert, nsend, per = dims
    part, rows_send = vert // nfeat, nsend + per
    nchunk = part // DB
    f, g = lax.axis_index("feat"), lax.axis_index("graph")
    halo_base, hub_base = vert, vert + ngraph * nsend
    nblock = vert // DB

    def fpeer(r):
        return lax.rem(f + r, nfeat)

    def gpeer(r):
        return lax.rem(g + r, ngraph)

    def frdma(src, dst, send, recv, r):
        return pltpu.make_async_remote_copy(src, dst, send, recv, device_id={"feat": fpeer(r)}, device_id_type=MESH)

    def grdma(src, dst, send, recv, r):
        return pltpu.make_async_remote_copy(src, dst, send, recv, device_id={"graph": gpeer(r)}, device_id_type=MESH)

    for i in [nblock] + [q * nchunk + c for c in range(nchunk) for q in range(nfeat)]:
        pltpu.make_async_copy(a_hbm.at[pl.ds(i * DB, DB)], a_v.at[pl.ds(i * DB, DB)], a_sem.at[i]).start()

    barrier = pltpu.get_barrier_semaphore()
    for r in range(1, nfeat):
        pl.semaphore_signal(barrier, inc=1, device_id={"feat": fpeer(r)}, device_id_type=MESH)
    for r in range(1, ngraph):
        pl.semaphore_signal(barrier, inc=1, device_id={"graph": gpeer(r)}, device_id_type=MESH)
    pl.semaphore_wait(barrier, nfeat + ngraph - 2)

    w2_copies = [frdma(w2_ref, w2in.at[f], w2s.at[r - 1], w2r.at[r - 1], r) for r in range(1, nfeat)]
    for copy in w2_copies:
        copy.start()
    w2in[f] = w2_ref[...]
    for tab in (tab1, tab2):
        tab[pl.ds(pl.multiple_of(halo_base + g * nsend, nsend), nsend)] = jnp.zeros((nsend, tab.shape[1]), BF16)

    cols = tab1.shape[1]
    tab1[:vert] = tabown_ref[...]

    lane = lax.broadcasted_iota(jnp.int32, (1, DB), 1).astype(F32).astype(BF16)

    def select_rows(tab, high, low):
        zero = jnp.zeros((), BF16)
        hot = jnp.where(low == lane, jnp.ones((), BF16), zero)
        pieces = [jnp.where(high == jnp.full((), j, BF16), hot, zero) for j in range(vert // DB)]
        return jnp.dot(jnp.concatenate(pieces, axis=1), tab[:vert], preferred_element_type=F32).astype(BF16)

    def halo_copies(tab, layer, r):
        p = gpeer(r)
        return (
            grdma(halo.at[layer, p, pl.ds(0, nsend)], tab.at[pl.ds(pl.multiple_of(halo_base + g * nsend, nsend), nsend)],
                  hs.at[layer, r - 1], hr.at[layer, r - 1], r),
            grdma(halo.at[layer, p, pl.ds(nsend, per)], tab.at[pl.ds(pl.multiple_of(hub_base + g * per, per), per)],
                  ps.at[layer, r - 1], pr.at[layer, r - 1], r),
        )

    def start_halo(tab, layer):
        def one(r, carry):
            p = gpeer(r)
            halo[layer, p] = select_rows(tab, high_ref[p], low_ref[p])
            for copy in halo_copies(tab, layer, r):
                copy.start()
            return carry

        lax.fori_loop(1, ngraph, one, 0)
        tab[pl.ds(pl.multiple_of(hub_base + g * per, per), per)] = select_rows(tab, high_ref[g, nsend:], low_ref[g, nsend:])

    def wait_halo(tab, layer):
        def arrive(r, carry):
            for copy in halo_copies(tab, layer, r):
                copy.wait_recv()
            return carry

        lax.fori_loop(1, ngraph, arrive, 0)

    inv = inv_ref[...]

    def chunk(i):
        return pl.ds(pl.multiple_of(i * DB, DB), DB)

    def product(a, tab):
        out = jnp.dot(jnp.concatenate(bf16_parts(a), axis=0), tab, preferred_element_type=F32)
        return out[:DB] + (out[DB:2 * DB] + out[2 * DB:])

    def a_copy(rb):
        return pltpu.make_async_copy(a_hbm.at[chunk(rb)], a_v.at[chunk(rb)], a_sem.at[rb])

    def own_blocks(tab, layer, blocks):
        if layer == 0:
            for rb in blocks:
                a_copy(rb).wait()
        for rb in blocks:
            acc[chunk(rb)] = product(a_v[chunk(rb), :vert], tab[:vert])

    def own_chunks(tab, layer, count):
        def one(i, carry):
            own_blocks(tab, layer, [q * nchunk + i for q in range(nfeat)])
            return carry

        lax.fori_loop(0, count, one, 0)

    def far_part(tab, rb):
        return (acc[chunk(rb)] + product(a_v[chunk(rb), vert:], tab[vert:])) * inv

    def hub_copy(layer, r):
        p = gpeer(r)
        return grdma(hubsend.at[layer, pl.ds(pl.multiple_of(p * per, per), per)], hubrecv.at[layer, g], us.at[layer, r - 1], ur.at[layer, r - 1], r)

    def exchange_hubs(tab, layer):
        hubsend[layer] = far_part(tab, nblock)
        for r in range(1, ngraph):
            hub_copy(layer, r).start()
        hubrecv[layer, g] = hubsend[layer, pl.ds(pl.multiple_of(g * per, per), per)]

    def hub_totals(layer):
        for r in range(1, ngraph):
            hub_copy(layer, r).wait_recv()
        total = hubrecv[layer, 0]
        for p in range(1, ngraph):
            total = total + hubrecv[layer, p]
        fill = jnp.zeros((DB - 3 * per, total.shape[1]), BF16)
        tot[layer] = jnp.concatenate([*bf16_parts(total), fill], axis=0)

    def with_hubs(layer, rb):
        rows = lax.broadcasted_iota(jnp.int32, (DB, DB), 0) + rb * DB
        sel = jnp.where(rows == myhub_ref[...], F32(1), F32(0)).astype(BF16)
        return acc[chunk(rb)] + jnp.dot(sel, tot[layer], preferred_element_type=F32)

    start_halo(tab1, 0)
    own_blocks(tab1, 0, [nblock])
    own_chunks(tab1, 0, nchunk - 1)
    wait_halo(tab1, 0)
    exchange_hubs(tab1, 0)
    def h_copy(i, r):
        return frdma(hsend.at[fpeer(r), chunk(i)], hin.at[f, chunk(i)], ns.at[i, r - 1], nr.at[i, r - 1], r)

    def z2_copy(i, r):
        return frdma(zout.at[fpeer(r), chunk(i)], tab2.at[pl.ds(pl.multiple_of(f * part + i * DB, DB), DB)], z2s.at[i, r - 1], z2r.at[i, r - 1], r)

    def z2_chunk(i):
        for r in range(1, nfeat):
            h_copy(i, r).wait_recv()
        acc = None
        for s in range(nfeat):
            term = jnp.dot(hin[s, chunk(i)], w2in[s], preferred_element_type=F32)
            acc = term if acc is None else acc + term
        acc = acc.astype(BF16)
        for q in range(nfeat):
            zout[q, chunk(i)] = acc[:, q * cols:(q + 1) * cols]
        for r in range(1, nfeat):
            z2_copy(i, r).start()
        tab2[pl.ds(pl.multiple_of(f * part + i * DB, DB), DB)] = zout[f, chunk(i)]

    bias1 = b1_ref[...]

    def far1(i):
        for r in range(1, nfeat + 1):
            rb = fpeer(r) * nchunk + i
            acc[chunk(rb)] = far_part(tab1, rb)

    def finish1(i):
        for r in range(1, nfeat + 1):
            q = fpeer(r)
            h = jnp.maximum(with_hubs(0, q * nchunk + i) + bias1, 0.0).astype(BF16)
            if r < nfeat:
                hsend[q, chunk(i)] = h
                h_copy(i, r).start()
            else:
                hin[f, chunk(i)] = h

    far1(0)
    hub_totals(0)
    for copy in w2_copies:
        copy.wait_recv()

    finish1(0)
    own_blocks(tab1, 0, [q * nchunk + nchunk - 1 for q in range(nfeat)])
    far1(1)

    def rows1(i, carry):
        finish1(i - 1)
        z2_chunk(i - 2)
        far1(i)
        return carry

    lax.fori_loop(2, nchunk, rows1, 0)
    finish1(nchunk - 1)
    z2_chunk(nchunk - 2)

    def wait_z2(chunks):
        for i in chunks:
            for r in range(1, nfeat):
                z2_copy(i, r).wait_recv()

    half = nchunk // 2

    def own_half(rb, c):
        start = [q * part + c * DB for q in range(nfeat)]
        a = jnp.concatenate([a_v[chunk(rb), s:s + half * DB] for s in start], axis=1)
        return product(a, jnp.concatenate([tab2[s:s + half * DB] for s in start], axis=0))

    def first_half(i, carry):
        for u in range(4):
            acc[chunk(4 * i + u)] = own_half(4 * i + u, 0)
        return carry

    wait_z2(range(half))
    lax.fori_loop(0, nblock // 8, first_half, 0)
    z2_chunk(nchunk - 1)
    lax.fori_loop(nblock // 8, nblock // 4, first_half, 0)
    acc[chunk(nblock)] = own_half(nblock, 0)
    wait_z2(range(half, nchunk))

    start_halo(tab2, 1)

    def second_half(i, carry):
        for u in range(4):
            acc[chunk(4 * i + u)] += own_half(4 * i + u, half)
        return carry

    acc[chunk(nblock)] += own_half(nblock, half)
    lax.fori_loop(0, nblock // 4, second_half, 0)
    wait_halo(tab2, 1)
    exchange_hubs(tab2, 1)
    def far2(i):
        for u in range(4):
            acc[chunk(4 * i + u)] = far_part(tab2, 4 * i + u)

    def finish2(i):
        for u in range(4):
            o_ref[chunk(4 * i + u), :] = with_hubs(1, 4 * i + u)

    lag = nblock // 4 - 1

    def far2_only(i, carry):
        far2(i)
        return carry

    lax.fori_loop(0, lag, far2_only, 0)
    hub_totals(1)
    far2(lag)
    for i in range(lag + 1):
        finish2(i)

    for copy in w2_copies:
        copy.wait_send()
    for i in range(nchunk):
        for r in range(1, nfeat):
            h_copy(i, r).wait_send()
            z2_copy(i, r).wait_send()
    for layer, tab in enumerate((tab1, tab2)):
        for r in range(1, ngraph):
            for copy in halo_copies(tab, layer, r):
                copy.wait_send()
            hub_copy(layer, r).wait_send()


def run_layers(nfeat, ngraph, nsend, per, tab_own, w2, high, low, myhub, b1, inv, adj):
    vert = tab_own.shape[0]
    part, cols = vert // nfeat, b1.shape[1]
    nchunk, nblk = part // DB, adj.shape[0] // DB
    vm = lambda shape, dt: pltpu.VMEM(shape, dt)
    dma = lambda *shape: pltpu.SemaphoreType.DMA(shape)
    vspec = pl.BlockSpec(memory_space=pltpu.VMEM)
    fr, gr = nfeat - 1, ngraph - 1
    return pl.pallas_call(
        functools.partial(layers_kernel, (nfeat, ngraph, vert, nsend, per)),
        out_shape=jax.ShapeDtypeStruct((vert, cols), F32),
        in_specs=[vspec] * 7 + [pl.BlockSpec(memory_space=pl.ANY)],
        out_specs=vspec,
        scratch_shapes=[
            vm(adj.shape, F32), vm((adj.shape[0], cols), F32), vm((2, DB, cols), BF16), vm((nfeat, *w2.shape), BF16),
            vm((adj.shape[1], cols), BF16), vm((adj.shape[1], cols), BF16), vm((nfeat, part, cols), BF16), vm((nfeat, part, cols), BF16),
            vm((nfeat, part, cols), BF16), vm((2, ngraph, nsend + per, cols), BF16), vm((2, ngraph * per, cols), F32), vm((2, ngraph, per, cols), F32),
            dma(nblk), dma(fr), dma(fr), dma(nchunk, fr), dma(nchunk, fr),
            dma(2, gr), dma(2, gr), dma(2, gr), dma(2, gr), dma(2, gr), dma(2, gr), dma(nchunk, fr), dma(nchunk, fr),
        ],
        compiler_params=pltpu.CompilerParams(collective_id=1, has_side_effects=True, vmem_limit_bytes=52 * 2**20),
        name="layers",
    )(tab_own, w2, high, low, myhub, b1, inv, adj)


def solution(mesh):
    rows_axes = ("data", "graph")
    nfeat = mesh.shape["feat"]
    ngraph = mesh.shape["graph"]

    def device_program(x_loc, dst_loc, src_loc, valid_loc, w_loc, send_loc, keep_loc, hub_ids, w_first, w_second, b_first, b_second):
        vert = x_loc.shape[0]
        nhub = hub_ids.shape[0]
        per = nhub // ngraph
        nsend = send_loc.shape[1]
        ndb = (vert + nhub) // DB
        table_rows = vert + ngraph * nsend + nhub
        nsb = -(-table_rows // SB)
        grid = lambda v: v.reshape(-1, 128)
        edges, starts, tab_own, inv, hub_col, myhub, high, low = run_pre(
            nfeat, ngraph, ndb, nsb, grid(dst_loc), grid(src_loc), grid(valid_loc), grid(w_loc), x_loc.T, w_first, hub_ids[None, :], send_loc, keep_loc)
        adj = build_adjacency(starts, edges, hub_col, ndb, nsb, table_rows)
        return run_layers(nfeat, ngraph, nsend, per, tab_own, w_second, high, low, myhub, b_first[None, :], inv, adj) + b_second

    edge_spec = P(rows_axes)
    send_spec = P(rows_axes, None)
    in_specs = (P(rows_axes, "feat"), edge_spec, edge_spec, edge_spec, edge_spec, send_spec, send_spec, P("data"), P("feat", None), P("feat", None), P("feat"), P("feat"))
    return jax.shard_map(device_program, mesh=mesh, in_specs=in_specs, out_specs=P(rows_axes, "feat"), check_vma=False)
```

```python
import functools

import jax
import jax.numpy as jnp
from jax import lax
from jax.experimental import pallas as pl
from jax.experimental.pallas import tpu as pltpu
from jax.sharding import PartitionSpec as P

DB, SB, KW = 128, 256, 256
MESH = pl.DeviceIdType.MESH
F32, BF16 = jnp.float32, jnp.bfloat16


def bf16_parts(x):
    hi = x.astype(BF16)
    rest = x - hi.astype(F32)
    mid = rest.astype(BF16)
    low = (rest - mid.astype(F32)).astype(BF16)
    return hi, mid, low


def build_kernel(ndb, nsb, ncol, starts_ref, edges_ref, hubcol_ref, a_ref):
    db = pl.program_id(0)
    dbase = (db * DB).astype(F32)
    hub_col = hubcol_ref[...]
    row_id = jnp.where(db == ndb - 1, hub_col, lax.broadcasted_iota(jnp.int32, (DB, 128), 0).astype(F32)).astype(BF16)
    iota_s = lax.broadcasted_iota(jnp.int32, (SB, 128), 0).astype(BF16)
    zero = jnp.zeros((), BF16)

    def window(sb, start, slots):
        width = min(SB, ncol - sb * SB)
        chunk = start // 128
        shift = start - chunk * 128
        raw = edges_ref[pl.ds(pl.multiple_of(chunk * 8, 8), 8 * (slots // 128 + 1)), :]
        raw = jnp.concatenate([raw[8 * i:8 * i + 8] for i in range(slots // 128 + 1)], axis=1)
        rows = pltpu.roll(raw, slots + 128 - shift, 1)[:, :slots]
        dst = (rows[0:1] - dbase).astype(BF16)
        src = (rows[1:2] - F32(SB * sb)).astype(BF16)
        tiled = lambda v: jnp.concatenate([v] * (slots // 128), axis=1)
        hit = tiled(row_id) == dst
        d3 = jnp.concatenate([jnp.where(hit, part, zero) for part in bf16_parts(rows[2:3])], axis=0)
        col_id = hub_col.astype(BF16) if sb == nsb - 1 else iota_s
        sel = jnp.where(tiled(col_id) == src, jnp.ones((), BF16), zero)
        out = lax.dot_general(d3, sel, (((1,), (1,)), ((), ())), preferred_element_type=F32)
        return out[:DB] + (out[DB:2 * DB] + out[2 * DB:]), slice(sb * SB, sb * SB + width)

    slots = [KW] * (nsb - 1) + [2 * KW]
    over = None
    for sb in range(nsb):
        start = starts_ref[0, db * nsb + sb]
        more = starts_ref[0, db * nsb + sb + 1] - start - slots[sb]
        over = more if over is None else jnp.maximum(over, more)
        block, where = window(sb, start, slots[sb])
        a_ref[:, where] = block

    @pl.when(over > 0)
    def _():
        for sb in range(nsb):
            start = starts_ref[0, db * nsb + sb] + slots[sb]
            end = starts_ref[0, db * nsb + sb + 1]

            def step(i, carry):
                block, where = window(sb, start + i * KW, KW)
                a_ref[:, where] += block
                return carry

            lax.fori_loop(0, (jnp.maximum(end - start, 0) + KW - 1) // KW, step, 0)


def build_adjacency(starts, edges, hub_col, ndb, nsb, ncol):
    return pl.pallas_call(
        functools.partial(build_kernel, ndb, nsb, ncol),
        out_shape=jax.ShapeDtypeStruct((ndb * DB, ncol), F32),
        grid_spec=pltpu.PrefetchScalarGridSpec(
            num_scalar_prefetch=1,
            grid=(ndb,),
            in_specs=[pl.BlockSpec(edges.shape, lambda i, s: (0, 0)), pl.BlockSpec(hub_col.shape, lambda i, s: (0, 0))],
            out_specs=pl.BlockSpec((DB, ncol), lambda i, s: (i, 0)),
        ),
        compiler_params=pltpu.CompilerParams(vmem_limit_bytes=62 * 2**20),
        name="build",
    )(starts, edges, hub_col)


def iota2(axis):
    return lax.broadcasted_iota(jnp.int32, (8, 128), axis)


def sort_levels(kref, wref, first, last):
    sub, lane = iota2(0), iota2(1)

    def bit(b):
        return ((sub >> (b - 6)) & 1) == 1 if b < 9 else ((lane >> (b - 9)) & 1) == 1

    def within(level):
        steps = []
        for j in range(level - 1, 5, -1):
            high = bit(j)
            if level < 16:
                want_max = high != bit(level)
            else:
                want_max = high
            steps.append((j, high, want_max))

        def body(it, carry):
            pairs = [(kref[it * 16 + u], wref[it * 16 + u]) for u in range(16)]
            for j, high, want_max in steps:
                axis, m, size = (0, 1 << (j - 6), 8) if j < 9 else (1, 1 << (j - 9), 128)
                new = []
                index = (lane if axis else sub) ^ m
                for key, w in pairs:
                    if 2 * m == size:
                        pk, pw = pltpu.roll(key, m, axis), pltpu.roll(w, m, axis)
                    else:
                        pk = jnp.take_along_axis(key, index, axis=axis)
                        pw = jnp.take_along_axis(w, index, axis=axis)
                    nk = jnp.where(want_max, jnp.maximum(key, pk), jnp.minimum(key, pk))
                    new.append((nk, jnp.where(nk == key, w, pw)))
                pairs = new
            for u, (key, w) in enumerate(pairs):
                kref[it * 16 + u] = key
                wref[it * 16 + u] = w
            return carry

        lax.fori_loop(0, 4, body, 0)

    def across(level, top, low):
        base = 3 if low >= 3 else 0

        def body(it, carry):
            where_v = [(it + 8 * u) if base == 3 else (it * 8 + u) for u in range(8)]
            ks, ws = [kref[v] for v in where_v], [wref[v] for v in where_v]
            for j in range(top, low - 1, -1):
                m = 1 << (j - base)
                for u in range(8):
                    if u & m:
                        continue
                    a, b = u, u | m
                    down = None
                    if level < 6 and base <= level < base + 3:
                        flip = bool(u >> (level - base) & 1)
                        swap = (ks[a] < ks[b]) if flip else (ks[a] > ks[b])
                    elif level < 6:
                        down = jnp.full((8, 128), (it >> (level - 3 + base)) & 1, jnp.int32) == 1
                        swap = (ks[a] > ks[b]) != down
                    elif level < 16:
                        swap = (ks[a] > ks[b]) != bit(level)
                    else:
                        swap = ks[a] > ks[b]
                    ks[a], ks[b] = jnp.where(swap, ks[b], ks[a]), jnp.where(swap, ks[a], ks[b])
                    ws[a], ws[b] = jnp.where(swap, ws[b], ws[a]), jnp.where(swap, ws[a], ws[b])
            for u, v in enumerate(where_v):
                kref[v] = ks[u]
                wref[v] = ws[u]
            return carry

        lax.fori_loop(0, 8, body, 0)

    for level in range(first, last + 1):
        if level > 6:
            within(level)
        if level > 3:
            across(level, min(level - 1, 5), 3)
        across(level, min(level - 1, 2), 0)


def pre_kernel(dims, dst_ref, src_ref, valid_ref, w_ref, x_ref, w1_ref, hub_ref, send_ref, keep_ref,
               edges_ref, starts_ref, tab_ref, inv_ref, hubcol_ref, myhub_ref, high_ref, low_ref,
               kref, wref, xin, w1in, tab, zout, xs, xr, w1s, w1r, zs, zr):
    nfeat, ngraph, ndb, nsb = dims
    vert = x_ref.shape[1]
    part = vert // nfeat
    f = lax.axis_index("feat")

    def fpeer(r):
        return lax.rem(f + r, nfeat)

    def frdma(src, dst, send, recv, r):
        return pltpu.make_async_remote_copy(src, dst, send, recv, device_id={"feat": fpeer(r)}, device_id_type=MESH)

    def quarter(q):
        return pl.ds(pl.multiple_of(q * part, part), part)

    barrier = pltpu.get_barrier_semaphore()
    for r in range(1, nfeat):
        pl.semaphore_signal(barrier, inc=1, device_id={"feat": fpeer(r)}, device_id_type=MESH)
    dst, src = dst_ref[...], src_ref[...]
    key = (((dst // DB) * nsb + src // SB) << 15) | ((dst % DB) << 8) | (src % SB)
    nbucket = ndb * nsb
    key = jnp.where(valid_ref[...] > 0, key, nbucket << 15).astype(F32)
    coef = w_ref[...] * valid_ref[...].astype(F32)
    large = jnp.max(coef, keepdims=True) > 1e30
    coef = coef * jnp.where(large, F32(2.0**-40), F32(1))
    inv_ref[...] = jnp.broadcast_to(jnp.where(large, F32(2.0**40), F32(1)), inv_ref.shape)
    used = dst.shape[0] // 8
    kref[:used] = key.reshape(used, 8, 128)
    wref[:used] = coef.reshape(used, 8, 128)
    kref[used:] = jnp.full((64 - used, 8, 128), nbucket << 15, F32)
    wref[used:] = jnp.zeros((64 - used, 8, 128), F32)
    pl.semaphore_wait(barrier, nfeat - 1)
    peers = range(1, nfeat)
    x_copies = [frdma(x_ref.at[:, quarter(fpeer(r))], xin.at[f], xs.at[r - 1], xr.at[r - 1], r) for r in peers]
    w1_copies = [frdma(w1_ref, w1in.at[f], w1s.at[r - 1], w1r.at[r - 1], r) for r in peers]
    z_copies = [frdma(zout.at[fpeer(r)], tab.at[quarter(f)], zs.at[r - 1], zr.at[r - 1], r) for r in peers]
    for copy in w1_copies + x_copies:
        copy.start()
    xin[f] = x_ref[:, quarter(f)]
    w1in[f] = w1_ref[...]

    sort_levels(kref, wref, 1, 13)

    g, per = lax.axis_index("graph"), DB // ngraph
    lane_id = lax.broadcasted_iota(jnp.int32, (DB, DB), 1).astype(F32)
    row_id = lax.broadcasted_iota(jnp.int32, (DB, DB), 0).astype(F32)
    down = lambda row: jnp.broadcast_to(row, (DB, DB)).T
    ids = hub_ref[...].astype(F32)
    owner = (hub_ref[...] // vert).astype(F32)
    owner_down = down(owner)
    earlier = (owner == owner_down) & (lane_id < row_id)
    pos_down = owner_down * per + jnp.sum(jnp.where(earlier, F32(1), F32(0)), axis=1, keepdims=True)
    pos = pos_down.T
    base = (g * per).astype(F32)
    first = (g * vert).astype(F32)
    hubcol_ref[...] = jnp.broadcast_to(jnp.sum(jnp.where(pos == row_id, lane_id, F32(0)), axis=1, keepdims=True), (DB, DB))
    lane_row = lax.broadcasted_iota(jnp.int32, (1, DB), 1)
    target = (lane_row % per).astype(F32) + base
    mine = jnp.sum(jnp.where(pos_down == target, down(ids), F32(0)), axis=0, keepdims=True) - first
    myhub_ref[...] = jnp.where(lane_row < 3 * per, mine, F32(-1)).astype(jnp.int32)
    mine_down = jnp.sum(jnp.where(pos == row_id + base, ids, F32(0)), axis=1, keepdims=True) - first
    mine_down = jnp.broadcast_to(mine_down, (DB, DB))[:per]
    rows = jnp.where(keep_ref[...] > 0, send_ref[...], -1).astype(F32)
    nsend = rows.shape[1]

    def put_index(p, where, val):
        high = jnp.floor(val * F32(1.0 / DB))
        high_ref[p, where] = high.astype(BF16)
        low_ref[p, where] = (val - high * DB).astype(BF16)

    for p in range(ngraph):
        for h in range(nsend // DB):
            put_index(p, slice(h * DB, (h + 1) * DB), down(rows[p:p + 1, h * DB:(h + 1) * DB]))
        put_index(p, slice(nsend, nsend + per), mine_down)

    for copy in w1_copies + x_copies:
        copy.wait_recv()
    cols = tab.shape[1]
    z = None
    for s in range(nfeat):
        term = lax.dot_general(xin[s], w1in[s], (((0,), (0,)), ((), ())), preferred_element_type=F32)
        z = term if z is None else z + term
    z = z.astype(BF16)
    for q in range(nfeat):
        zout[q] = z[:, q * cols:(q + 1) * cols]
    for copy in z_copies:
        copy.start()
    tab[quarter(f)] = zout[f]
    sort_levels(kref, wref, 14, 16)

    nb = starts_ref.shape[1]
    bound = (lax.broadcasted_iota(jnp.int32, (nb, 1), 0) << 15).astype(F32)
    last = kref[63, 7:8, :]
    lane = lax.broadcasted_iota(jnp.int32, (1, 128), 1)
    before = jnp.where(lane == 0, F32(-1), pltpu.roll(last, 1, 1))
    full = last < bound
    row_sel = jnp.where((before < bound) & jnp.logical_not(full), F32(1), F32(0)).astype(BF16)
    keys = kref[...].reshape(512, 128)
    picked = None
    for piece in bf16_parts(keys):
        term = lax.dot_general(row_sel, piece, (((1,), (1,)), ((), ())), preferred_element_type=F32)
        picked = term if picked is None else picked + term
    inside = jnp.where(picked < bound, F32(1), F32(0)).astype(BF16)
    count = lax.dot_general(jnp.ones((8, 512), BF16), inside, (((1,), (1,)), ((), ())), preferred_element_type=F32)
    rows = lax.dot_general(jnp.ones((8, 128), BF16), jnp.where(full, F32(1), F32(0)).astype(BF16), (((1,), (1,)), ((), ())), preferred_element_type=F32)
    starts_ref[...] = (count + 512.0 * rows).astype(jnp.int32)

    nl = edges_ref.shape[0] // 32
    for k in range(4):
        kk = jnp.concatenate([kref[:, 2 * k, :], kref[:, 2 * k + 1, :]], axis=0)
        ww = jnp.concatenate([wref[:, 2 * k, :], wref[:, 2 * k + 1, :]], axis=0)
        ki = kk.astype(jnp.int32)
        bucket = ki >> 15
        block = jnp.floor((bucket.astype(F32) + 0.5) * F32(1.0 / nsb))
        edge_dst = block * DB + ((ki >> 8) & (DB - 1)).astype(F32)
        edge_src = (bucket.astype(F32) - block * nsb) * SB + (ki & (SB - 1)).astype(F32)
        for field, val in enumerate((edge_dst, edge_src, ww)):
            edges_ref[pl.ds(k * 8 + field, nl, stride=32), :] = val.T[:nl]

    for copy in z_copies:
        copy.wait_recv()
    tab_ref[...] = tab[...]
    for copy in x_copies + w1_copies + z_copies:
        copy.wait_send()


def run_pre(nfeat, ngraph, ndb, nsb, dst, src, valid, w, x, w1, hubs, send, keep):
    vert, part = x.shape[1], x.shape[1] // nfeat
    cols = w1.shape[1] // nfeat
    nrows = dst.shape[0]
    vm = lambda shape, dt: pltpu.VMEM(shape, dt)
    dma = pltpu.SemaphoreType.DMA((nfeat - 1,))
    vspec = pl.BlockSpec(memory_space=pltpu.VMEM)
    shape = jax.ShapeDtypeStruct
    return pl.pallas_call(
        functools.partial(pre_kernel, (nfeat, ngraph, ndb, nsb)),
        out_shape=[shape(((nrows + 8) * 8, 128), F32), shape((8, 384), jnp.int32), shape((vert, cols), BF16), shape((1, cols), F32),
                   shape((DB, DB), F32), shape((1, DB), jnp.int32), *[shape((ngraph, send.shape[1] + DB // ngraph, DB), BF16)] * 2],
        in_specs=[vspec] * 9,
        out_specs=[vspec] * 8,
        scratch_shapes=[
            vm((64, 8, 128), F32), vm((64, 8, 128), F32), vm((nfeat, x.shape[0], part), BF16), vm((nfeat, *w1.shape), BF16),
            vm((vert, cols), BF16), vm((nfeat, part, cols), BF16), dma, dma, dma, dma, dma, dma,
        ],
        compiler_params=pltpu.CompilerParams(collective_id=0, has_side_effects=True, vmem_limit_bytes=62 * 2**20),
        name="pre",
    )(dst, src, valid, w, x, w1, hubs, send, keep)


def layers_kernel(dims, tabown_ref, w2_ref, high_ref, low_ref, myhub_ref, b1_ref, inv_ref, a_hbm, o_ref,
                  a_v, acc, tot, w2in, tab1, tab2, zout, hsend, hin, halo, hubsend, hubrecv,
                  a_sem, w2s, w2r, z2s, z2r, hs, hr, ps, pr, us, ur, ns, nr):
    nfeat, ngraph, vert, nsend, per = dims
    part, rows_send = vert // nfeat, nsend + per
    nchunk = part // DB
    f, g = lax.axis_index("feat"), lax.axis_index("graph")
    halo_base, hub_base = vert, vert + ngraph * nsend
    nblock = vert // DB

    def fpeer(r):
        return lax.rem(f + r, nfeat)

    def gpeer(r):
        return lax.rem(g + r, ngraph)

    def frdma(src, dst, send, recv, r):
        return pltpu.make_async_remote_copy(src, dst, send, recv, device_id={"feat": fpeer(r)}, device_id_type=MESH)

    def grdma(src, dst, send, recv, r):
        return pltpu.make_async_remote_copy(src, dst, send, recv, device_id={"graph": gpeer(r)}, device_id_type=MESH)

    for i in [nblock] + [q * nchunk + c for c in range(nchunk) for q in range(nfeat)]:
        pltpu.make_async_copy(a_hbm.at[pl.ds(i * DB, DB)], a_v.at[pl.ds(i * DB, DB)], a_sem.at[i]).start()

    barrier = pltpu.get_barrier_semaphore()
    for r in range(1, nfeat):
        pl.semaphore_signal(barrier, inc=1, device_id={"feat": fpeer(r)}, device_id_type=MESH)
    for r in range(1, ngraph):
        pl.semaphore_signal(barrier, inc=1, device_id={"graph": gpeer(r)}, device_id_type=MESH)
    pl.semaphore_wait(barrier, nfeat + ngraph - 2)

    w2_copies = [frdma(w2_ref, w2in.at[f], w2s.at[r - 1], w2r.at[r - 1], r) for r in range(1, nfeat)]
    for copy in w2_copies:
        copy.start()
    w2in[f] = w2_ref[...]
    for tab in (tab1, tab2):
        tab[pl.ds(pl.multiple_of(halo_base + g * nsend, nsend), nsend)] = jnp.zeros((nsend, tab.shape[1]), BF16)

    cols = tab1.shape[1]
    tab1[:vert] = tabown_ref[...]

    lane = lax.broadcasted_iota(jnp.int32, (1, DB), 1).astype(F32).astype(BF16)

    def select_rows(tab, high, low):
        zero = jnp.zeros((), BF16)
        hot = jnp.where(low == lane, jnp.ones((), BF16), zero)
        pieces = [jnp.where(high == jnp.full((), j, BF16), hot, zero) for j in range(vert // DB)]
        return jnp.dot(jnp.concatenate(pieces, axis=1), tab[:vert], preferred_element_type=F32).astype(BF16)

    def halo_copies(tab, layer, r):
        p = gpeer(r)
        return (
            grdma(halo.at[layer, p, pl.ds(0, nsend)], tab.at[pl.ds(pl.multiple_of(halo_base + g * nsend, nsend), nsend)],
                  hs.at[layer, r - 1], hr.at[layer, r - 1], r),
            grdma(halo.at[layer, p, pl.ds(nsend, per)], tab.at[pl.ds(pl.multiple_of(hub_base + g * per, per), per)],
                  ps.at[layer, r - 1], pr.at[layer, r - 1], r),
        )

    def start_halo(tab, layer):
        for r in range(1, ngraph):
            p = gpeer(r)
            halo[layer, p] = select_rows(tab, high_ref[p], low_ref[p])
            for copy in halo_copies(tab, layer, r):
                copy.start()
        tab[pl.ds(pl.multiple_of(hub_base + g * per, per), per)] = select_rows(tab, high_ref[g, nsend:], low_ref[g, nsend:])

    def wait_halo(tab, layer):
        def arrive(r, carry):
            for copy in halo_copies(tab, layer, r):
                copy.wait_recv()
            return carry

        lax.fori_loop(1, ngraph, arrive, 0)

    inv = inv_ref[...]

    def chunk(i):
        return pl.ds(pl.multiple_of(i * DB, DB), DB)

    def product(a, tab):
        out = jnp.dot(jnp.concatenate(bf16_parts(a), axis=0), tab, preferred_element_type=F32)
        return out[:DB] + (out[DB:2 * DB] + out[2 * DB:])

    def a_copy(rb):
        return pltpu.make_async_copy(a_hbm.at[chunk(rb)], a_v.at[chunk(rb)], a_sem.at[rb])

    def own_blocks(tab, layer, blocks):
        if layer == 0:
            for rb in blocks:
                a_copy(rb).wait()
        for rb in blocks:
            acc[chunk(rb)] = product(a_v[chunk(rb), :vert], tab[:vert])

    def own_chunks(tab, layer, count):
        def one(i, carry):
            own_blocks(tab, layer, [q * nchunk + i for q in range(nfeat)])
            return carry

        lax.fori_loop(0, count, one, 0)

    def far_part(tab, rb):
        return (acc[chunk(rb)] + product(a_v[chunk(rb), vert:], tab[vert:])) * inv

    def hub_copy(layer, r):
        p = gpeer(r)
        return grdma(hubsend.at[layer, pl.ds(pl.multiple_of(p * per, per), per)], hubrecv.at[layer, g], us.at[layer, r - 1], ur.at[layer, r - 1], r)

    def exchange_hubs(tab, layer):
        hubsend[layer] = far_part(tab, nblock)
        for r in range(1, ngraph):
            hub_copy(layer, r).start()
        hubrecv[layer, g] = hubsend[layer, pl.ds(pl.multiple_of(g * per, per), per)]

    def hub_totals(layer):
        for r in range(1, ngraph):
            hub_copy(layer, r).wait_recv()
        total = hubrecv[layer, 0]
        for p in range(1, ngraph):
            total = total + hubrecv[layer, p]
        fill = jnp.zeros((DB - 3 * per, total.shape[1]), BF16)
        tot[layer] = jnp.concatenate([*bf16_parts(total), fill], axis=0)

    def with_hubs(layer, rb):
        rows = lax.broadcasted_iota(jnp.int32, (DB, DB), 0) + rb * DB
        sel = jnp.where(rows == myhub_ref[...], F32(1), F32(0)).astype(BF16)
        return acc[chunk(rb)] + jnp.dot(sel, tot[layer], preferred_element_type=F32)

    start_halo(tab1, 0)
    own_blocks(tab1, 0, [nblock])
    own_chunks(tab1, 0, nchunk - 1)
    wait_halo(tab1, 0)
    exchange_hubs(tab1, 0)
    def h_copy(i, r):
        return frdma(hsend.at[fpeer(r), chunk(i)], hin.at[f, chunk(i)], ns.at[i, r - 1], nr.at[i, r - 1], r)

    def z2_copy(i, r):
        return frdma(zout.at[fpeer(r), chunk(i)], tab2.at[pl.ds(pl.multiple_of(f * part + i * DB, DB), DB)], z2s.at[i, r - 1], z2r.at[i, r - 1], r)

    def z2_chunk(i):
        for r in range(1, nfeat):
            h_copy(i, r).wait_recv()
        acc = None
        for s in range(nfeat):
            term = jnp.dot(hin[s, chunk(i)], w2in[s], preferred_element_type=F32)
            acc = term if acc is None else acc + term
        acc = acc.astype(BF16)
        for q in range(nfeat):
            zout[q, chunk(i)] = acc[:, q * cols:(q + 1) * cols]
        for r in range(1, nfeat):
            z2_copy(i, r).start()
        tab2[pl.ds(pl.multiple_of(f * part + i * DB, DB), DB)] = zout[f, chunk(i)]

    bias1 = b1_ref[...]

    def far1(i):
        for r in range(1, nfeat + 1):
            rb = fpeer(r) * nchunk + i
            acc[chunk(rb)] = far_part(tab1, rb)

    def finish1(i):
        for r in range(1, nfeat + 1):
            q = fpeer(r)
            h = jnp.maximum(with_hubs(0, q * nchunk + i) + bias1, 0.0).astype(BF16)
            if r < nfeat:
                hsend[q, chunk(i)] = h
                h_copy(i, r).start()
            else:
                hin[f, chunk(i)] = h

    far1(0)
    own_blocks(tab1, 0, [q * nchunk + nchunk - 1 for q in range(nfeat)])
    hub_totals(0)
    for copy in w2_copies:
        copy.wait_recv()

    finish1(0)
    far1(1)

    def rows1(i, carry):
        finish1(i - 1)
        z2_chunk(i - 2)
        far1(i)
        return carry

    lax.fori_loop(2, nchunk, rows1, 0)
    finish1(nchunk - 1)
    z2_chunk(nchunk - 2)

    def wait_z2(chunks):
        for i in chunks:
            for r in range(1, nfeat):
                z2_copy(i, r).wait_recv()

    half = nchunk // 2

    def own_half(rb, c):
        start = [q * part + c * DB for q in range(nfeat)]
        a = jnp.concatenate([a_v[chunk(rb), s:s + half * DB] for s in start], axis=1)
        return product(a, jnp.concatenate([tab2[s:s + half * DB] for s in start], axis=0))

    def first_half(i, carry):
        for u in range(4):
            acc[chunk(4 * i + u)] = own_half(4 * i + u, 0)
        return carry

    wait_z2(range(half))
    lax.fori_loop(0, nblock // 8, first_half, 0)
    z2_chunk(nchunk - 1)
    lax.fori_loop(nblock // 8, nblock // 4, first_half, 0)
    acc[chunk(nblock)] = own_half(nblock, 0)
    wait_z2(range(half, nchunk))

    start_halo(tab2, 1)

    def second_half(i, carry):
        for u in range(4):
            acc[chunk(4 * i + u)] += own_half(4 * i + u, half)
        return carry

    acc[chunk(nblock)] += own_half(nblock, half)
    lax.fori_loop(0, nblock // 4, second_half, 0)
    wait_halo(tab2, 1)
    exchange_hubs(tab2, 1)
    def far2(i):
        for u in range(4):
            acc[chunk(4 * i + u)] = far_part(tab2, 4 * i + u)

    def finish2(i):
        for u in range(4):
            o_ref[chunk(4 * i + u), :] = with_hubs(1, 4 * i + u)

    lag = nblock // 4 - 1

    def far2_only(i, carry):
        far2(i)
        return carry

    lax.fori_loop(0, lag, far2_only, 0)
    hub_totals(1)
    far2(lag)
    for i in range(lag + 1):
        finish2(i)

    for copy in w2_copies:
        copy.wait_send()
    for i in range(nchunk):
        for r in range(1, nfeat):
            h_copy(i, r).wait_send()
            z2_copy(i, r).wait_send()
    for layer, tab in enumerate((tab1, tab2)):
        for r in range(1, ngraph):
            for copy in halo_copies(tab, layer, r):
                copy.wait_send()
            hub_copy(layer, r).wait_send()


def run_layers(nfeat, ngraph, nsend, per, tab_own, w2, high, low, myhub, b1, inv, adj):
    vert = tab_own.shape[0]
    part, cols = vert // nfeat, b1.shape[1]
    nchunk, nblk = part // DB, adj.shape[0] // DB
    vm = lambda shape, dt: pltpu.VMEM(shape, dt)
    dma = lambda *shape: pltpu.SemaphoreType.DMA(shape)
    vspec = pl.BlockSpec(memory_space=pltpu.VMEM)
    fr, gr = nfeat - 1, ngraph - 1
    return pl.pallas_call(
        functools.partial(layers_kernel, (nfeat, ngraph, vert, nsend, per)),
        out_shape=jax.ShapeDtypeStruct((vert, cols), F32),
        in_specs=[vspec] * 7 + [pl.BlockSpec(memory_space=pl.ANY)],
        out_specs=vspec,
        scratch_shapes=[
            vm(adj.shape, F32), vm((adj.shape[0], cols), F32), vm((2, DB, cols), BF16), vm((nfeat, *w2.shape), BF16),
            vm((adj.shape[1], cols), BF16), vm((adj.shape[1], cols), BF16), vm((nfeat, part, cols), BF16), vm((nfeat, part, cols), BF16),
            vm((nfeat, part, cols), BF16), vm((2, ngraph, nsend + per, cols), BF16), vm((2, ngraph * per, cols), F32), vm((2, ngraph, per, cols), F32),
            dma(nblk), dma(fr), dma(fr), dma(nchunk, fr), dma(nchunk, fr),
            dma(2, gr), dma(2, gr), dma(2, gr), dma(2, gr), dma(2, gr), dma(2, gr), dma(nchunk, fr), dma(nchunk, fr),
        ],
        compiler_params=pltpu.CompilerParams(collective_id=1, has_side_effects=True, vmem_limit_bytes=48 * 2**20),
        name="layers",
    )(tab_own, w2, high, low, myhub, b1, inv, adj)


def solution(mesh):
    rows_axes = ("data", "graph")
    nfeat = mesh.shape["feat"]
    ngraph = mesh.shape["graph"]

    def device_program(x_loc, dst_loc, src_loc, valid_loc, w_loc, send_loc, keep_loc, hub_ids, w_first, w_second, b_first, b_second):
        vert = x_loc.shape[0]
        nhub = hub_ids.shape[0]
        per = nhub // ngraph
        nsend = send_loc.shape[1]
        ndb = (vert + nhub) // DB
        table_rows = vert + ngraph * nsend + nhub
        nsb = -(-table_rows // SB)
        grid = lambda v: v.reshape(-1, 128)
        edges, starts, tab_own, inv, hub_col, myhub, high, low = run_pre(
            nfeat, ngraph, ndb, nsb, grid(dst_loc), grid(src_loc), grid(valid_loc), grid(w_loc), x_loc.T, w_first, hub_ids[None, :], send_loc, keep_loc)
        adj = build_adjacency(starts, edges, hub_col, ndb, nsb, table_rows)
        return run_layers(nfeat, ngraph, nsend, per, tab_own, w_second, high, low, myhub, b_first[None, :], inv, adj) + b_second

    edge_spec = P(rows_axes)
    send_spec = P(rows_axes, None)
    in_specs = (P(rows_axes, "feat"), edge_spec, edge_spec, edge_spec, edge_spec, send_spec, send_spec, P("data"), P("feat", None), P("feat", None), P("feat"), P("feat"))
    return jax.shard_map(device_program, mesh=mesh, in_specs=in_specs, out_specs=P(rows_axes, "feat"), check_vma=False)
```
